8 devices in a mesh: sweep: 1 (over z), data: 2 (over y), ent: 4 (over x, core).
Axes of the slice: x: 2, y: 2, z: 1, core: 2. Of those that a mesh axis runs over, the one named last changes fastest.
Arguments:
- ent_table: float32 [131072, 400], P(('sweep', 'ent'))
- ent_state: float32 [131072], P(('sweep', 'ent'))
- rel_table: float32 [14824, 400], P('sweep')
- head_idx: int32 [4, 4, 4096], P(('sweep', 'ent'), None, 'data')
- tail_idx: int32 [4, 4, 4096], P(('sweep', 'ent'), None, 'data')
- rel_idx: int32 [4, 4, 4096], P(('sweep', 'ent'), None, 'data')
- edge_mask: int32 [4, 4, 4096], P(('sweep', 'ent'), None, 'data')
- neg_idx: int32 [4, 4, 768], P(('sweep', 'ent'))
Outputs:
- output 1: float32 [131072, 400], P(('sweep', 'ent'))
- output 2: float32 [131072], P(('sweep', 'ent'))
- output 3: float32 [14824, 400], P('sweep')
- output 4: float32 [4, 4], P(('sweep', 'ent'))
All inputs are finite; a program needn't handle non-finite values.
Results may differ from the reference program's by a relative error of at most 0.001.
Values are sent between devices in bfloat16 or wider.
A program may use at most 1 GiB of HBM per device.

```python
import jax
import jax.numpy as jnp
from jax import lax

ENT_GROUP = 4
DATA_REPS = 2
ROWS_DEV = 32768
EDGES_DEV = 2048
NEG_COUNT = 768
EMBED_DIM = 400
REL_COUNT = 14824
HOT_IDS = 16

TOTAL_ROWS = ENT_GROUP * ROWS_DEV
BUCKET_EDGES = DATA_REPS * EDGES_DEV
LR_SCALE = 0.2
EPSILON = 1e-8


def draw_edges(edge_key):
    subkeys = jax.random.split(edge_key, 14)
    edge_shape = (ENT_GROUP, ENT_GROUP, BUCKET_EDGES)
    hot_ent = jax.random.randint(subkeys[0], (ENT_GROUP, HOT_IDS), 0, ROWS_DEV)
    hot_rel = jax.random.randint(subkeys[1], (HOT_IDS,), 0, REL_COUNT)
    group_ids = jnp.arange(ENT_GROUP)
    tail_group = (group_ids[:, None] + group_ids[None, :]) % ENT_GROUP
    head_hot = jnp.broadcast_to(hot_ent[:, None, :], (ENT_GROUP, ENT_GROUP, HOT_IDS))
    tail_hot = hot_ent[tail_group]

    def pick_rows(key_use, key_slot, key_uni, hot_rows):
        use_hot = jax.random.randint(key_use, edge_shape, 0, 4) == 0
        hot_slot = jax.random.randint(key_slot, edge_shape, 0, HOT_IDS)
        hot_pick = jnp.take_along_axis(hot_rows, hot_slot, axis=2)
        uni_pick = jax.random.randint(key_uni, edge_shape, 0, ROWS_DEV)
        return jnp.where(use_hot, hot_pick, uni_pick)

    head_idx = pick_rows(subkeys[2], subkeys[3], subkeys[4], head_hot)
    tail_idx = pick_rows(subkeys[5], subkeys[6], subkeys[7], tail_hot)
    rel_use = jax.random.randint(subkeys[8], edge_shape, 0, 2) == 0
    rel_slot = jax.random.randint(subkeys[9], edge_shape, 0, HOT_IDS)
    rel_uni = jax.random.randint(subkeys[10], edge_shape, 0, REL_COUNT)
    rel_idx = jnp.where(rel_use, hot_rel[rel_slot], rel_uni)
    keep_level = jax.random.randint(subkeys[11], (ENT_GROUP, ENT_GROUP, 1), 1, 17)
    edge_mask = (jax.random.randint(subkeys[12], edge_shape, 0, 16) < keep_level).astype(jnp.int32)
    neg_idx = jax.random.randint(subkeys[13], (ENT_GROUP, ENT_GROUP, NEG_COUNT), 0, ROWS_DEV)
    head_idx = head_idx.at[:, :, 0].set(ROWS_DEV - 1)
    tail_idx = tail_idx.at[:, :, 0].set(ROWS_DEV - 1)
    neg_idx = neg_idx.at[:, :, 0].set(ROWS_DEV - 1)
    rel_idx = rel_idx.at[:, :, 0].set(REL_COUNT - 1)
    return head_idx, tail_idx, rel_idx, edge_mask, neg_idx


def setup_inputs(seed: int = 0, part: int = 0) -> dict:
    part_key = jax.random.fold_in(jax.random.key(seed), part)
    subkeys = jax.random.split(part_key, 4)
    emb_scale = EMBED_DIM ** -0.25
    ent_table = jax.random.normal(subkeys[0], (TOTAL_ROWS, EMBED_DIM), jnp.float32) * emb_scale
    ent_state = jax.random.uniform(subkeys[1], (TOTAL_ROWS,), jnp.float32, 0.01, 0.1) * EMBED_DIM ** -0.5
    rel_table = jax.random.normal(subkeys[2], (REL_COUNT, EMBED_DIM), jnp.float32) * 0.7
    head_idx, tail_idx, rel_idx, edge_mask, neg_idx = draw_edges(subkeys[3])
    return {'ent_table': ent_table, 'ent_state': ent_state, 'rel_table': rel_table, 'head_idx': head_idx, 'tail_idx': tail_idx, 'rel_idx': rel_idx, 'edge_mask': edge_mask, 'neg_idx': neg_idx}


def adagrad(param_rows, accum_rows, grad_rows, learn_rate):
    accum_new = accum_rows + jnp.mean(grad_rows * grad_rows, axis=-1)
    step_rows = grad_rows / jnp.sqrt(accum_new + EPSILON)[..., None]
    return param_rows - learn_rate * step_rows, accum_new


def bucket_terms(head_rows, rel_rows, tail_bf, neg_bf, weight):
    half_dim = head_rows.shape[1] // 2
    re_h = head_rows[:, :half_dim]
    im_h = head_rows[:, half_dim:]
    re_r = rel_rows[:, :half_dim]
    im_r = rel_rows[:, half_dim:]
    query_vec = jnp.concatenate([re_h * re_r - im_h * im_r, re_h * im_r + im_h * re_r], axis=1)
    query_bf = query_vec.astype(jnp.bfloat16)
    query_wide = query_bf.astype(jnp.float32)
    tail_wide = tail_bf.astype(jnp.float32)
    pos_score = jnp.sum(query_wide * tail_wide, axis=1)
    neg_score = jnp.dot(query_bf, neg_bf.T, preferred_element_type=jnp.float32)
    top_score = jnp.maximum(jnp.max(neg_score, axis=1), pos_score)
    pos_exp = jnp.exp(pos_score - top_score)
    neg_exp = jnp.exp(neg_score - top_score[:, None])
    exp_total = pos_exp + jnp.sum(neg_exp, axis=1)
    log_total = top_score + jnp.log(exp_total)
    loss_sum = jnp.sum(weight * (log_total - pos_score))
    d_pos = weight * (pos_exp / exp_total - 1.0)
    d_neg = ((weight / exp_total)[:, None] * neg_exp).astype(jnp.bfloat16)
    grad_query = d_pos[:, None] * tail_wide + jnp.dot(d_neg, neg_bf, preferred_element_type=jnp.float32)
    grad_tail = d_pos[:, None] * query_wide
    grad_neg = jnp.dot(d_neg.T, query_bf, preferred_element_type=jnp.float32)
    re_g = grad_query[:, :half_dim]
    im_g = grad_query[:, half_dim:]
    grad_head = jnp.concatenate([re_g * re_r + im_g * im_r, im_g * re_r - re_g * im_r], axis=1)
    grad_rel = jnp.concatenate([re_g * re_h + im_g * im_h, im_g * re_h - re_g * im_h], axis=1)
    return loss_sum, grad_head, grad_rel, grad_tail, grad_neg


def reference(ent_table, ent_state, rel_table, head_idx, tail_idx, rel_idx, edge_mask, neg_idx):
    groups = head_idx.shape[0]
    part_rows = ent_table.shape[0] // groups
    emb_width = ent_table.shape[1]
    rel_rows = rel_table.shape[0]
    bucket_edges = head_idx.shape[2]
    share_edges = bucket_edges // DATA_REPS
    learn_rate = LR_SCALE * emb_width ** -0.25
    pair_ids = jnp.arange(groups * DATA_REPS)

    def one_pass(pass_carry, step_idx):
        table_now, state_now, rel_now, rel_state = pass_carry
        table_bf = table_now.astype(jnp.bfloat16)

        def one_share(grad_acc, pair_id):
            ent_grad, rel_grad = grad_acc
            group_id = pair_id // DATA_REPS
            edge_start = (pair_id % DATA_REPS) * share_edges
            tail_base = ((group_id + step_idx) % groups) * part_rows
            h_ids = lax.dynamic_slice_in_dim(head_idx[group_id, step_idx], edge_start, share_edges) + group_id * part_rows
            t_ids = lax.dynamic_slice_in_dim(tail_idx[group_id, step_idx], edge_start, share_edges) + tail_base
            r_ids = lax.dynamic_slice_in_dim(rel_idx[group_id, step_idx], edge_start, share_edges)
            weight = lax.dynamic_slice_in_dim(edge_mask[group_id, step_idx], edge_start, share_edges).astype(jnp.float32)
            n_ids = neg_idx[group_id, step_idx] + tail_base
            loss_sum, g_head, g_rel, g_tail, g_neg = bucket_terms(table_now[h_ids], rel_now[r_ids], table_bf[t_ids], table_bf[n_ids], weight)
            ent_grad = ent_grad.at[h_ids].add(g_head).at[t_ids].add(g_tail).at[n_ids].add(g_neg)
            rel_grad = rel_grad.at[r_ids].add(g_rel)
            return (ent_grad, rel_grad), loss_sum

        share_init = (jnp.zeros_like(table_now), jnp.zeros_like(rel_now))
        grads_end, share_loss = lax.scan(one_share, share_init, pair_ids)
        ent_grad, rel_grad = grads_end
        table_now, state_now = adagrad(table_now, state_now, ent_grad, learn_rate)
        rel_now, rel_state = adagrad(rel_now, rel_state, rel_grad, learn_rate)
        bucket_loss = share_loss.reshape(groups, DATA_REPS).sum(axis=1) / bucket_edges
        return (table_now, state_now, rel_now, rel_state), bucket_loss

    pass_init = (ent_table, ent_state, rel_table, jnp.zeros((rel_rows,), jnp.float32))
    pass_end, losses = lax.scan(one_pass, pass_init, jnp.arange(groups))
    return pass_end[0], pass_end[1], pass_end[2], losses.T
```

```python
import functools

import jax
import jax.numpy as jnp
from jax import lax
from jax.experimental import pallas as pl
from jax.experimental.pallas import tpu as pltpu
from jax.sharding import PartitionSpec as P

LR_SCALE = 0.2
EPSILON = 1e-8

LANES = 128
WORDS = 4
SHIFT = 14
POS_MASK = (1 << SHIFT) - 1
NO_KEY = 2**31 - 1
BLOCK = 1024
SUB = 128
SLOTS = 4
ROW_SLOT = 16
QUERY_SLOT = 32
WIDE = WORDS * LANES
TILE = 512
CHUNK = 256
VMEM_LIMIT = 63 * 2**20
F32 = jnp.float32
BF16 = jnp.bfloat16
ANY = pl.BlockSpec(memory_space=pl.ANY)


def words_of(start):
    return pl.ds(pl.multiple_of(start * WORDS, WORDS), WORDS)


def word(start):
    return pl.ds(pl.multiple_of(start, WORDS), WORDS)


def unrolled_loop(lo, hi, unroll, body, carry):
    full = (hi - lo) // unroll

    def several(t, c):
        for j in range(unroll):
            c = body(lo + t * unroll + j, c)
        return c

    carry = lax.fori_loop(0, full, several, carry)
    return lax.fori_loop(lo + full * unroll, hi, body, carry)


def packed_rows(n, slot):
    return 3 * n + n * slot // LANES


def pack(v, pad, slot):
    n = v[0].shape[0]
    gap = LANES - pad
    lane = lax.broadcasted_iota(jnp.int32, (n, LANES), 1)
    mixed = jnp.where(lane < pad, v[1], pltpu.roll(v[3], pad, 1))
    groups = LANES // slot
    size = n // groups
    thin = lane[:size]
    rest = jnp.zeros((size, LANES), F32)
    for a in range(groups):
        moved = pltpu.roll(v[3][a * size:(a + 1) * size], (slot * a - gap) % LANES, 1)
        rest = jnp.where((thin >= slot * a) & (thin < slot * (a + 1)), moved, rest)
    return v[0], v[2], mixed, rest


def unpack(first, third, mixed, rest, pad, slot):
    n = first.shape[0]
    gap = LANES - pad
    lane = lax.broadcasted_iota(jnp.int32, (n, LANES), 1)
    tail = jnp.concatenate([pltpu.roll(rest, (gap - slot * a) % LANES, 1) for a in range(LANES // slot)], axis=0)
    last = jnp.where(lane < gap, pltpu.roll(mixed, LANES - pad, 1), tail)
    return [first, jnp.where(lane < pad, mixed, 0.0), third, jnp.where(lane < pad, last, 0.0)], last


def put_packed(ref, base, v, pad, slot):
    n = v[0].shape[0]
    for c, part in enumerate(pack(v, pad, slot)):
        ref[pl.ds(pl.multiple_of(base + c * n, 16), part.shape[0]), :] = part.astype(ref.dtype)


def get_packed(ref, base, n, pad, slot):
    at = [pl.ds(pl.multiple_of(base + c * n, 16), n if c < 3 else n * slot // LANES) for c in range(4)]
    return unpack(*[ref[i, :].astype(F32) for i in at], pad, slot)


def params(**kw):
    return pltpu.CompilerParams(dimension_semantics=("arbitrary",), vmem_limit_bytes=VMEM_LIMIT, **kw)


def whole(shape):
    return pl.BlockSpec(shape, lambda *_: (0,) * len(shape), pipeline_mode=pl.Buffered(1))


def convert_kernel(half, has_state, *refs):
    src = refs[0]
    state = refs[1] if has_state else None
    dst = refs[-1]
    pad = half - LANES
    sub8 = lax.broadcasted_iota(jnp.int32, (8, LANES), 0)
    for r0 in range(0, BLOCK, SUB):
        cols = slice(r0, r0 + SUB)
        if has_state:
            low = jnp.where(sub8 == 7, jnp.broadcast_to(state[:, cols], (8, LANES)), 0.0)
        else:
            low = jnp.zeros((8, LANES), F32)
        gap = jnp.zeros((LANES - pad - 8, LANES), F32)
        none = jnp.zeros((8, LANES), F32)
        w = [
            src[:LANES, cols],
            jnp.concatenate([src[LANES:half, cols], gap, none], axis=0),
            src[half:half + LANES, cols],
            jnp.concatenate([src[half + LANES:, cols], gap, low], axis=0),
        ]
        for c in range(WORDS):
            dst[pl.ds(r0 * WORDS + c, SUB, stride=WORDS), :] = w[c].T


def to_words(table_t, state):
    dim, rows = table_t.shape
    blocks = pl.cdiv(rows, BLOCK)
    ins = [pl.BlockSpec((dim, BLOCK), lambda b: (0, b))]
    args = [table_t]
    if state is not None:
        ins.append(pl.BlockSpec((None, 1, BLOCK), lambda b: (b, 0, 0)))
        args.append(state.reshape(blocks, 1, BLOCK))
    return pl.pallas_call(
        functools.partial(convert_kernel, dim // 2, state is not None),
        grid=(blocks,),
        in_specs=ins,
        out_specs=pl.BlockSpec((BLOCK * WORDS, LANES), lambda b: (b, 0)),
        out_shape=jax.ShapeDtypeStruct((blocks * BLOCK * WORDS, LANES), F32),
        compiler_params=params(),
        name="to_words",
    )(*args)


def sweep(table, ring, load_sems, store, blocks, body):
    def load(b):
        slot = lax.rem(b, SLOTS)
        at = pl.ds(pl.multiple_of(b * BLOCK * WORDS, BLOCK * WORDS), BLOCK * WORDS)
        return pltpu.make_async_copy(table.at[at], ring.at[slot], load_sems.at[slot])

    load(0).start()
    load(1).start()

    def turn(b, carry):
        load(b).wait()

        @pl.when(b >= 2)
        def _():
            store(b - 2).wait()

        @pl.when(b + 2 < blocks)
        def _():
            load(b + 2).start()

        body(b, ring.at[lax.rem(b, SLOTS)])
        store(b).start()
        return carry

    lax.fori_loop(0, blocks, turn, 0)
    store(blocks - 2).wait()
    store(blocks - 1).wait()


def apply_step(w, g, dim, lr):
    total = (g[0] * g[0] + g[1] * g[1]) + (g[2] * g[2] + g[3] * g[3])
    state = w[3][:, LANES - 1:] + jnp.sum(total, axis=1, keepdims=True) * (1.0 / dim)
    scale = lr * lax.rsqrt(state + EPSILON)
    return [w[c] - g[c] * scale for c in range(WORDS)], state


def sum_terms(src, dst, lo, hi, terms, acc):
    acc[...] = jnp.zeros_like(acc)

    def body(k, carry):
        prev, total = carry
        at = dst[k]
        total = jnp.where(at == prev, total, 0.0) + terms[word(src[k]), :]
        acc[word(at), :] = total
        return at, total

    unrolled_loop(lo, hi, 8, body, (jnp.int32(-1), jnp.zeros((WORDS, LANES), F32)))


def update_words(ref, acc, dim, lr):
    lane = lax.broadcasted_iota(jnp.int32, (SUB, LANES), 1)
    for r0 in range(0, BLOCK, SUB):
        at = [pl.ds(r0 * WORDS + c, SUB, stride=WORDS) for c in range(WORDS)]
        w, state = apply_step([ref[i, :] for i in at], [acc[i, :] for i in at], dim, lr)
        w[3] = jnp.where(lane == LANES - 1, state, w[3])
        for c in range(WORDS):
            ref[at[c], :] = w[c]


def update_columns(ref, acc, dst, state_out, dim, lr):
    half = dim // 2
    pad = half - LANES
    lane = lax.broadcasted_iota(jnp.int32, (SUB, LANES), 1)
    for r0 in range(0, BLOCK, SUB):
        at = [pl.ds(r0 * WORDS + c, SUB, stride=WORDS) for c in range(WORDS)]
        w, state = apply_step([ref[i, :] for i in at], [acc[i, :] for i in at], dim, lr)
        cols = slice(r0, r0 + SUB)
        dst[:LANES, cols] = w[0].T
        dst[LANES:half, cols] = w[1].T[:pad]
        dst[half:half + LANES, cols] = w[2].T
        w3 = jnp.where(lane == LANES - 1, state, w[3]).T
        dst[half + LANES:, cols] = w3[:pad]
        if state_out is not None:
            state_out[:, cols] = w3[LANES - 1:]


def load_entity_terms(sizes, half, gh, qb, gn, terms, queries, neg_terms, sems):
    heads, tails, negs = sizes
    pad = half - LANES
    copies = [
        pltpu.make_async_copy(qb, queries, sems.at[0]),
        pltpu.make_async_copy(gn, neg_terms, sems.at[1]),
        pltpu.make_async_copy(gh, terms.at[pl.ds(0, heads * WORDS)], sems.at[2]),
    ]
    for c in copies:
        c.start()
    copies[0].wait()

    def body(t, carry):
        q, last = get_packed(queries, t * packed_rows(TILE, QUERY_SLOT), TILE, pad, QUERY_SLOT)
        dp = (last[:, pad:pad + 1] + last[:, pad + 1:pad + 2]) + last[:, pad + 2:pad + 3]
        for c in range(WORDS):
            terms[pl.ds((heads + t * TILE) * WORDS + c, TILE, stride=WORDS), :] = dp * q[c]
        return carry

    lax.fori_loop(0, tails // TILE, body, 0)
    copies[1].wait()
    for c, v in enumerate(get_packed(neg_terms, 0, negs, pad, ROW_SLOT)[0]):
        terms[pl.ds((heads + tails) * WORDS + c, negs, stride=WORDS), :] = v
    copies[2].wait()


def store_entity_rows(sizes, half, rows, xh, xt, sem):
    heads, tails, negs = sizes
    pad = half - LANES
    copy = pltpu.make_async_copy(rows.at[pl.ds(0, heads * WORDS)], xh, sem)
    copy.start()

    def move(r0, n, base):
        v = [rows[pl.ds((heads + r0) * WORDS + c, n, stride=WORDS), :] for c in range(WORDS)]
        put_packed(xt, base, v, pad, ROW_SLOT)

    def body(t, carry):
        move(t * TILE, TILE, t * packed_rows(TILE, ROW_SLOT))
        return carry

    lax.fori_loop(0, tails // TILE, body, 0)
    move(tails, negs, tails // TILE * packed_rows(TILE, ROW_SLOT))
    copy.wait()


def near_rows(tails, negs):
    return tails // TILE * packed_rows(TILE, ROW_SLOT) + packed_rows(negs, ROW_SLOT)


def fetch_rows(row, spot, count, table, rows, sem):
    def body(k, carry):
        pltpu.make_async_copy(table.at[word(row[k])], rows.at[word(spot(k))], sem).start()
        return carry

    unrolled_loop(0, count, 8, body, 0)
    size = pl.multiple_of(count * WORDS, WORDS)
    pltpu.make_async_copy(table.at[pl.ds(0, size)], rows.at[pl.ds(0, size)], sem).wait()


def entity_fetch_kernel(sizes, half, row, spot, count, table, xh, xt, rows, sems):
    fetch_rows(row, lambda k: spot[k], count[0], table, rows, sems.at[0])
    store_entity_rows(sizes, half, rows, xh, xt, sems.at[1])


def relation_fetch_kernel(row, count, table, xr, rows, sems):
    fetch_rows(row, lambda k: k * WORDS, count[0], table, rows, sems.at[0])
    copy = pltpu.make_async_copy(rows, xr, sems.at[1])
    copy.start()
    copy.wait()


def entity_kernel(cfg, *refs):
    sizes, dim, lr, final = cfg
    it = iter(refs)
    usrc, udst, uoff = next(it), next(it), next(it)
    xsrc, xdst, xoff = (None, None, None) if final else (next(it), next(it), next(it))
    table, gh, qb, gn = next(it), next(it), next(it), next(it)
    out = next(it)
    if final:
        state_out = next(it)
    else:
        xh, xt = next(it), next(it)
    terms, queries, neg_terms, acc, ring = next(it), next(it), next(it), next(it), next(it)
    rows = None if final else next(it)
    cols = next(it) if final else None
    sems, load_sems, store_sems = next(it), next(it), next(it)
    blocks = table.shape[0] // (BLOCK * WORDS)
    load_entity_terms(sizes, dim // 2, gh, qb, gn, terms, queries, neg_terms, sems)

    def store(b):
        if final:
            slot = lax.rem(b, 2)
            at = pl.ds(pl.multiple_of(b * BLOCK, BLOCK), BLOCK)
            return pltpu.make_async_copy(cols.at[slot], out.at[:, at], store_sems.at[slot])
        slot = lax.rem(b, SLOTS)
        at = pl.ds(pl.multiple_of(b * BLOCK * WORDS, BLOCK * WORDS), BLOCK * WORDS)
        return pltpu.make_async_copy(ring.at[slot], out.at[at], store_sems.at[slot])

    def body(b, ref):
        sum_terms(usrc, udst, uoff[b], uoff[b + 1], terms, acc)
        if final:
            update_columns(ref, acc, cols.at[lax.rem(b, 2)], state_out.at[b], dim, lr)
        else:
            update_words(ref, acc, dim, lr)
            copy_rows(xsrc, lambda k: xdst[k], xoff[b], xoff[b + 1], ref, rows)

    sweep(table, ring, load_sems, store, blocks, body)
    if not final:
        store_entity_rows(sizes, dim // 2, rows, xh, xt, sems.at[0])


def copy_rows(src, dst, lo, hi, ref, rows):
    def body(k, carry):
        rows[word(dst(k)), :] = ref[word(src[k]), :]
        return carry

    unrolled_loop(lo, hi, 8, body, 0)


def entity_fetch(table, sizes, half, row, spot, count):
    heads, tails, negs = sizes
    return pl.pallas_call(
        functools.partial(entity_fetch_kernel, sizes, half),
        grid_spec=pltpu.PrefetchScalarGridSpec(
            num_scalar_prefetch=3, grid=(1,), in_specs=[ANY], out_specs=[ANY, whole((near_rows(tails, negs), LANES))],
            scratch_shapes=[pltpu.VMEM((sum(sizes) * WORDS, LANES), F32), pltpu.SemaphoreType.DMA((2,))]),
        out_shape=[jax.ShapeDtypeStruct((heads * WORDS, LANES), F32), jax.ShapeDtypeStruct((near_rows(tails, negs), LANES), BF16)],
        compiler_params=params(),
        name="entity_fetch",
    )(row, spot, count, table)


def relation_fetch(table, edges, row, count):
    return pl.pallas_call(
        relation_fetch_kernel,
        grid_spec=pltpu.PrefetchScalarGridSpec(
            num_scalar_prefetch=2, grid=(1,), in_specs=[ANY], out_specs=ANY,
            scratch_shapes=[pltpu.VMEM((edges * WORDS, LANES), F32), pltpu.SemaphoreType.DMA((2,))]),
        out_shape=jax.ShapeDtypeStruct((edges * WORDS, LANES), F32),
        compiler_params=params(),
        name="relation_fetch",
    )(row, count, table)


def entity_pass(table, sizes, dim, lr, upd, parts, ext=None):
    heads, tails, negs = sizes
    final = ext is None
    blocks = table.shape[0] // (BLOCK * WORDS)
    total = sum(sizes) * WORDS
    scalars = [*upd, *(() if final else ext)]
    scratch = [
        pltpu.VMEM((total, LANES), F32),
        pltpu.VMEM(parts[1].shape, BF16),
        pltpu.VMEM(parts[2].shape, F32),
        pltpu.VMEM((BLOCK * WORDS, LANES), F32),
        pltpu.VMEM((SLOTS, BLOCK * WORDS, LANES), F32),
    ]
    if final:
        outs = [ANY, whole((blocks, 1, BLOCK))]
        shapes = [jax.ShapeDtypeStruct((dim, blocks * BLOCK), F32), jax.ShapeDtypeStruct((blocks, 1, BLOCK), F32)]
        scratch.append(pltpu.VMEM((2, dim, BLOCK), F32))
    else:
        outs = [ANY, ANY, whole((near_rows(tails, negs), LANES))]
        shapes = [jax.ShapeDtypeStruct(table.shape, F32), jax.ShapeDtypeStruct((heads * WORDS, LANES), F32),
                  jax.ShapeDtypeStruct((near_rows(tails, negs), LANES), BF16)]
        scratch.append(pltpu.VMEM((total, LANES), F32))
    scratch += [pltpu.SemaphoreType.DMA((3,)), pltpu.SemaphoreType.DMA((SLOTS,)), pltpu.SemaphoreType.DMA((SLOTS,))]
    return pl.pallas_call(
        functools.partial(entity_kernel, (sizes, dim, lr, final)),
        grid_spec=pltpu.PrefetchScalarGridSpec(
            num_scalar_prefetch=len(scalars), grid=(1,), in_specs=[ANY] * 4, out_specs=outs, scratch_shapes=scratch),
        out_shape=shapes,
        input_output_aliases={} if final else {len(scalars): 0},
        compiler_params=params(),
        name="entity_last" if final else "entity_pass",
    )(*scalars, table, *parts)


def load_relation_terms(parts, terms, sems):
    at = 0
    copies = []
    for n, part in enumerate(parts):
        copies.append(pltpu.make_async_copy(part, terms.at[pl.ds(at, part.shape[0])], sems.at[n]))
        at += part.shape[0]
    for c in copies:
        c.start()
    for c in copies:
        c.wait()


def relation_kernel(cfg, *refs):
    dim, lr, n_parts = cfg
    usrc, udst, uoff, xsrc, xoff, table = refs[:6]
    parts = refs[6:6 + n_parts]
    out, xr, terms, acc, ring, rows, sems, load_sems, store_sems = refs[6 + n_parts:]
    blocks = table.shape[0] // (BLOCK * WORDS)
    load_relation_terms(parts, terms, sems)

    def store(b):
        slot = lax.rem(b, SLOTS)
        at = pl.ds(pl.multiple_of(b * BLOCK * WORDS, BLOCK * WORDS), BLOCK * WORDS)
        return pltpu.make_async_copy(ring.at[slot], out.at[at], store_sems.at[slot])

    def body(b, ref):
        sum_terms(usrc, udst, uoff[b], uoff[b + 1], terms, acc)
        update_words(ref, acc, dim, lr)
        copy_rows(xsrc, lambda k: k * WORDS, xoff[b], xoff[b + 1], ref, rows)

    sweep(table, ring, load_sems, store, blocks, body)
    copy = pltpu.make_async_copy(rows, xr, sems.at[0])
    copy.start()
    copy.wait()


def relation_last_kernel(cfg, *refs):
    dim, lr, n_parts = cfg
    usrc, udst, uoff, src = refs[:4]
    parts = refs[4:4 + n_parts]
    dst, terms, acc, sems = refs[4 + n_parts:]
    step = pl.program_id(0)

    @pl.when(step == 0)
    def _():
        load_relation_terms(parts, terms, sems)

    sum_terms(usrc, udst, uoff[step], uoff[step + 1], terms, acc)
    update_columns(src, acc, dst, None, dim, lr)


def relation_pass(table, edges, dim, lr, upd, parts, ext):
    scalars = [*upd, *ext]
    return pl.pallas_call(
        functools.partial(relation_kernel, (dim, lr, len(parts))),
        grid_spec=pltpu.PrefetchScalarGridSpec(
            num_scalar_prefetch=len(scalars), grid=(1,), in_specs=[ANY] * (1 + len(parts)), out_specs=[ANY, ANY],
            scratch_shapes=[
                pltpu.VMEM((sum(p.shape[0] for p in parts), LANES), F32),
                pltpu.VMEM((BLOCK * WORDS, LANES), F32),
                pltpu.VMEM((SLOTS, BLOCK * WORDS, LANES), F32),
                pltpu.VMEM((edges * WORDS, LANES), F32),
                pltpu.SemaphoreType.DMA((len(parts),)),
                pltpu.SemaphoreType.DMA((SLOTS,)),
                pltpu.SemaphoreType.DMA((SLOTS,)),
            ]),
        out_shape=[jax.ShapeDtypeStruct(table.shape, F32), jax.ShapeDtypeStruct((edges * WORDS, LANES), F32)],
        input_output_aliases={len(scalars): 0},
        compiler_params=params(),
        name="relation_pass",
    )(*scalars, table, *parts)


def relation_last(table, n_rel, dim, lr, upd, parts):
    return pl.pallas_call(
        functools.partial(relation_last_kernel, (dim, lr, len(parts))),
        grid_spec=pltpu.PrefetchScalarGridSpec(
            num_scalar_prefetch=len(upd), grid=(table.shape[0] // (BLOCK * WORDS),),
            in_specs=[pl.BlockSpec((BLOCK * WORDS, LANES), lambda b, *_: (b, 0))] + [ANY] * len(parts),
            out_specs=pl.BlockSpec((dim, BLOCK), lambda b, *_: (0, b)),
            scratch_shapes=[
                pltpu.VMEM((sum(p.shape[0] for p in parts), LANES), F32),
                pltpu.VMEM((BLOCK * WORDS, LANES), F32),
                pltpu.SemaphoreType.DMA((len(parts),)),
            ]),
        out_shape=jax.ShapeDtypeStruct((dim, n_rel), F32),
        compiler_params=params(),
        name="relation_last",
    )(*upd, table, *parts)


def bucket_kernel(cfg, spot, info, xh, xr, tb, near, gh, qb_out, ua, ub, gn, loss, neg_in, nb, gr, uniq, gacc, held, sems):
    cap, edges, half = cfg
    step = pl.program_id(0)
    last = pl.num_programs(0) - 1
    pad = half - LANES
    n = info[0]
    start = step * TILE

    @pl.when(step == 0)
    def _():
        gacc[...] = jnp.zeros_like(gacc)
        loss[0, 0] = 0.0
        copy = pltpu.make_async_copy(near.at[pl.ds(near.shape[0] - neg_in.shape[0], neg_in.shape[0])], neg_in, sems.at[0])
        copy.start()
        copy.wait()
        for c, v in enumerate(get_packed(neg_in, 0, nb.shape[0], pad, ROW_SLOT)[0]):
            nb[:, LANES * c:LANES * (c + 1)] = v.astype(BF16)

    @pl.when(start < n)
    def _():
        row = lax.broadcasted_iota(jnp.int32, (TILE, LANES), 0) + start
        lane = lax.broadcasted_iota(jnp.int32, (TILE, LANES), 1)
        keep = row < n
        keep_data = keep & (lane < pad)

        def load(ref):
            v = [ref[pl.ds(c, TILE, stride=WORDS), :] for c in range(WORDS)]
            return [jnp.where(keep_data if c % 2 else keep, v[c], 0.0) for c in range(WORDS)]

        h = load(xh)
        r = load(xr)
        q = [h[0] * r[0] - h[2] * r[2], h[1] * r[1] - h[3] * r[3], h[0] * r[2] + h[2] * r[0], h[1] * r[3] + h[3] * r[1]]
        qc = [v.astype(BF16) for v in q]
        query = jnp.concatenate(qc, axis=1)
        tail = [jnp.where(keep, v, 0.0) for v in get_packed(tb, 0, TILE, pad, ROW_SLOT)[0]]
        prod = [qc[c].astype(F32) * tail[c] for c in range(WORDS)]
        pos = jnp.sum((prod[0] + prod[1]) + (prod[2] + prod[3]), axis=1, keepdims=True)
        neg = nb[...]
        score = lax.dot_general(query, neg, (((1,), (1,)), ((), ())), preferred_element_type=F32)
        top = jnp.maximum(jnp.max(score, axis=1, keepdims=True), pos)
        pos_exp = jnp.exp(pos - top)
        neg_exp = jnp.exp(score - top)
        total = pos_exp + jnp.sum(neg_exp, axis=1, keepdims=True)
        weight = jnp.where(keep[:, :1], 1.0, 0.0)
        loss[0, 0] += jnp.sum(weight * ((top + jnp.log(total)) - pos))
        inverse = 1.0 / total
        dp = weight * (pos_exp * inverse - 1.0)
        ds = ((weight * inverse) * neg_exp).astype(BF16)
        gq = lax.dot_general(ds, neg, (((1,), (0,)), ((), ())), preferred_element_type=F32)
        gacc[...] += lax.dot_general(ds, query, (((0,), (0,)), ((), ())), preferred_element_type=F32)
        g = [dp * tail[c] + gq[:, LANES * c:LANES * (c + 1)] for c in range(WORDS)]
        out = [g[0] * r[0] + g[2] * r[2], g[1] * r[1] + g[3] * r[3], g[2] * r[0] - g[0] * r[2], g[3] * r[1] - g[1] * r[3]]
        rel_g = [g[0] * h[0] + g[2] * h[2], g[1] * h[1] + g[3] * h[3], g[2] * h[0] - g[0] * h[2], g[3] * h[1] - g[1] * h[3]]
        for c in range(WORDS):
            gh[pl.ds(c, TILE, stride=WORDS), :] = out[c]
            gr[pl.ds(c, TILE, stride=WORDS), :] = rel_g[c]
        hi = dp.astype(BF16).astype(F32)
        mid = (dp - hi).astype(BF16).astype(F32)
        low = (dp - hi) - mid
        q3 = jnp.where(lane == pad, hi, jnp.where(lane == pad + 1, mid, jnp.where(lane == pad + 2, low, qc[3].astype(F32))))
        put_packed(qb_out, 0, [*[v.astype(F32) for v in qc[:3]], q3], pad, QUERY_SLOT)

        def body(k, carry):
            prev, acc = carry
            at = spot[k]
            acc = jnp.where(at == prev, acc, 0.0) + gr[words_of(k - start), :]
            uniq[word(at), :] = acc
            return at, acc

        prev = jnp.where(step > 0, spot[jnp.maximum(start - 1, 0)], -1)
        _, acc = unrolled_loop(start, jnp.minimum(start + TILE, n), 8, body, (prev, held[:WORDS, :]))
        held[:WORDS, :] = acc

    @pl.when(step == last)
    def _():
        size = cap // 2 * WORDS
        mine = pl.ds(pl.multiple_of(info[1] * size, size), size)
        copy = pltpu.make_async_copy(uniq.at[mine], ua, sems.at[0])
        more = pltpu.make_async_copy(uniq.at[pl.ds(cap * WORDS, (edges - cap) * WORDS)], ub, sems.at[1])
        copy.start()
        more.start()
        put_packed(gn, 0, [gacc[:, LANES * c:LANES * (c + 1)] for c in range(WORDS)], pad, ROW_SLOT)
        copy.wait()
        more.wait()


def bucket(spot, info, xh, xr, tail, negs, cap, half):
    edges = spot.shape[0]
    word_spec = pl.BlockSpec((TILE * WORDS, LANES), lambda t, *_: (t, 0))
    tail_spec = pl.BlockSpec((packed_rows(TILE, ROW_SLOT), LANES), lambda t, *_: (t, 0))
    query_spec = pl.BlockSpec((packed_rows(TILE, QUERY_SLOT), LANES), lambda t, *_: (t, 0))
    neg_rows = packed_rows(negs, ROW_SLOT)
    return pl.pallas_call(
        functools.partial(bucket_kernel, (cap, edges, half)),
        grid_spec=pltpu.PrefetchScalarGridSpec(
            num_scalar_prefetch=2,
            grid=(edges // TILE,),
            in_specs=[word_spec, word_spec, tail_spec, ANY],
            out_specs=[word_spec, query_spec, ANY, ANY, whole((neg_rows, LANES)),
                       pl.BlockSpec((1, 1), lambda *_: (0, 0), memory_space=pltpu.SMEM)],
            scratch_shapes=[
                pltpu.VMEM((neg_rows, LANES), BF16),
                pltpu.VMEM((negs, WIDE), BF16),
                pltpu.VMEM((TILE * WORDS, LANES), F32),
                pltpu.VMEM((edges * WORDS, LANES), F32),
                pltpu.VMEM((negs, WIDE), F32),
                pltpu.VMEM((8, LANES), F32),
                pltpu.SemaphoreType.DMA((2,)),
            ]),
        out_shape=[
            jax.ShapeDtypeStruct((edges * WORDS, LANES), F32),
            jax.ShapeDtypeStruct((edges // TILE * packed_rows(TILE, QUERY_SLOT), LANES), BF16),
            jax.ShapeDtypeStruct((cap // 2 * WORDS, LANES), F32),
            jax.ShapeDtypeStruct(((edges - cap) * WORDS, LANES), F32),
            jax.ShapeDtypeStruct((neg_rows, LANES), F32),
            jax.ShapeDtypeStruct((1, 1), F32),
        ],
        compiler_params=params(),
        name="bucket",
    )(spot, info, xh, xr, tail, tail)


def running_count(flags):
    lead = flags.shape[:-1]
    n = flags.shape[-1] // LANES
    x = flags.reshape(*lead, n, LANES).astype(F32)
    tri = jnp.triu(jnp.ones((LANES, LANES), F32))
    inner = jnp.einsum('...k,kl->...l', x, tri, precision=lax.Precision.HIGHEST)
    before = jnp.einsum('...k,kl->...l', inner[..., -1], jnp.triu(jnp.ones((n, n), F32), 1), precision=lax.Precision.HIGHEST)
    return (inner + before[..., None]).astype(jnp.int32).reshape(flags.shape)


def offsets(keys, bounds):
    return jnp.sum(keys[:, None, :] < bounds[None, :, None], axis=2, dtype=jnp.int32)


def solution(mesh):
    groups = mesh.shape['ent']
    data_reps = mesh.shape['data']
    row_spec = P(('sweep', 'ent'), None)
    edge_spec = P(('sweep', 'ent'), None, 'data')

    def device_fn(ent_table, ent_state, rel_table, head_idx, tail_idx, rel_idx, edge_mask, neg_idx):
        part_rows, dim = ent_table.shape
        half = dim // 2
        n_rel = rel_table.shape[0]
        rounds = head_idx.shape[1]
        edges = head_idx.shape[2] * data_reps
        negs = neg_idx.shape[2]
        sizes = (edges, edges, negs)
        cap = edges // 2
        lr = LR_SCALE * dim ** -0.25
        me = lax.axis_index('ent')
        rep = lax.axis_index('data')

        ent_words = to_words(ent_table.T, ent_state)
        rel_words = to_words(rel_table.T, None)

        big = (NO_KEY >> 13) - 1
        order = jnp.where(edge_mask[0] > 0, rel_idx[0], big)
        packed = head_idx[0] * part_rows + tail_idx[0]
        both = lax.all_gather(jnp.stack([order, packed]), 'data', axis=2, tiled=True)
        spot = jnp.arange(edges, dtype=jnp.int32)
        order, packed = lax.sort((both[0] * edges + spot, both[1]), dimension=1, num_keys=1)
        rel_s = order // edges
        head_s = packed // part_rows
        tail_s = packed % part_rows
        live = rel_s < n_rel
        kept = jnp.sum(live, axis=1, dtype=jnp.int32)
        info = jnp.concatenate([jnp.where(live, rel_s, n_rel), jnp.where(live, tail_s, part_rows), neg_idx[0]], axis=1)
        every = lax.all_gather(info, 'ent', axis=0)

        far = jnp.stack([lax.dynamic_index_in_dim(every, (me - s) % groups, 0, False)[s, edges:] for s in range(rounds)])
        ids = jnp.concatenate([jnp.where(live, head_s, part_rows), far], axis=1)
        keys = jnp.where(ids < part_rows, (ids << SHIFT) + jnp.arange(sum(sizes), dtype=jnp.int32), NO_KEY)
        ent_key = lax.sort(keys, dimension=1, is_stable=False)
        ent_off = offsets(ent_key, jnp.arange(part_rows // BLOCK + 1, dtype=jnp.int32) * (BLOCK << SHIFT))
        ent_src = (ent_key & POS_MASK) * WORDS
        ent_dst = ((ent_key >> SHIFT) % BLOCK) * WORDS

        rels = every[:, :, :edges]
        prev = jnp.concatenate([jnp.full((groups, rounds, 1), -1, jnp.int32), rels[:, :, :-1]], axis=2)
        fresh = (rels != prev) & (rels < n_rel)
        slot = running_count(fresh) - 1
        over = jnp.max(slot[:, :, -1], axis=0) >= cap
        own_spot = lax.dynamic_index_in_dim(slot, me, 0, False) * WORDS
        source = jnp.arange(groups, dtype=jnp.int32)[:, None, None]
        part = cap // data_reps
        first = (slot // part * groups + source) * part + slot % part
        slot = jnp.where(slot < cap, first, groups * cap + source * (edges - cap) + slot - cap)
        keys = jnp.where(fresh, (rels << SHIFT) + slot, NO_KEY).transpose(1, 0, 2).reshape(rounds, groups * edges)
        rel_key = lax.sort(keys, dimension=1, is_stable=False)
        bounds = jnp.arange(pl.cdiv(n_rel, BLOCK) + 1, dtype=jnp.int32) * BLOCK
        rel_off = offsets(rel_key, bounds << SHIFT)
        rel_src = (rel_key & POS_MASK) * WORDS
        rel_dst = ((rel_key >> SHIFT) % BLOCK) * WORDS
        own_off = offsets(jnp.where(live, rel_s, NO_KEY), bounds)
        own_src = (rel_s % BLOCK) * WORDS
        info = jnp.stack([kept, jnp.full((rounds,), rep, jnp.int32)], axis=1)

        ent_args = (sizes, dim, lr)
        rel_args = (dim, lr)
        xh, xt = entity_fetch(ent_words, sizes, half, (ent_key[0] >> SHIFT) * WORDS, ent_src[0], ent_off[0, -1:])
        xr = relation_fetch(rel_words, edges, rel_s[0] * WORDS, kept[:1])
        losses = []
        for s in range(rounds):
            tn = xt if s == 0 else lax.ppermute(xt, 'ent', [(i, (i - s) % groups) for i in range(groups)])
            gh, qb, ua, ub, gn, loss = bucket(own_spot[s], info[s], xh, xr, tn, negs, cap, half)
            losses.append(loss[0, 0] / edges)
            if s > 0:
                back = [(i, (i + s) % groups) for i in range(groups)]
                qb = lax.ppermute(qb, 'ent', back)
                gn = lax.ppermute(gn, 'ent', back)
                qb, gn, ua = lax.optimization_barrier((qb, gn, ua))
            shared = lax.all_gather(ua, ('data', 'ent'), axis=0, tiled=True)

            final = s == rounds - 1
            ent_upd = (ent_src[s], ent_dst[s], ent_off[s])
            rel_upd = (rel_src[s], rel_dst[s], rel_off[s])

            def relations(table, *parts, s=s, final=final, rel_upd=rel_upd):
                if final:
                    return (relation_last(table, n_rel, *rel_args, rel_upd, parts),)
                return relation_pass(table, edges, *rel_args, rel_upd, parts, (own_src[s + 1], own_off[s + 1]))

            def small(table, shared, ub, relations=relations):
                return relations(table, shared)

            def large(table, shared, ub, relations=relations):
                return relations(table, shared, lax.all_gather(ub, 'ent', axis=0, tiled=True))

            if final:
                ent_cols, state = entity_pass(ent_words, *ent_args, ent_upd, (gh, qb, gn))
                (rel_cols,) = lax.cond(over[s], large, small, rel_words, shared, ub)
            else:
                ent_words, xh, xt = entity_pass(ent_words, *ent_args, ent_upd, (gh, qb, gn), (ent_dst[s + 1], ent_src[s + 1], ent_off[s + 1]))
                rel_words, xr = lax.cond(over[s], large, small, rel_words, shared, ub)
        return ent_cols.T, state.reshape(part_rows), rel_cols.T, jnp.stack(losses)[None, :]

    return jax.shard_map(device_fn, mesh=mesh, in_specs=(row_spec, P(('sweep', 'ent')), P('sweep', None), edge_spec, edge_spec, edge_spec, edge_spec, P(('sweep', 'ent'), None, None)), out_specs=(row_spec, P(('sweep', 'ent')), P('sweep', None), row_spec), check_vma=False)
```

```python
import functools

import jax
import jax.numpy as jnp
from jax import lax
from jax.experimental import pallas as pl
from jax.experimental.pallas import tpu as pltpu
from jax.sharding import PartitionSpec as P

LR_SCALE = 0.2
EPSILON = 1e-8

LANES = 128
WORDS = 4
SHIFT = 14
POS_MASK = (1 << SHIFT) - 1
NO_KEY = 2**31 - 1
BLOCK = 1024
SUB = 128
SLOTS = 4
UNROLL = (16, 4)
ROW_SLOT = 16
QUERY_SLOT = 32
WIDE = WORDS * LANES
TILE = 512
CHUNK = 256
VMEM_LIMIT = 63 * 2**20
F32 = jnp.float32
BF16 = jnp.bfloat16
ANY = pl.BlockSpec(memory_space=pl.ANY)


def words_of(start):
    return pl.ds(pl.multiple_of(start * WORDS, WORDS), WORDS)


def word(start):
    return pl.ds(pl.multiple_of(start, WORDS), WORDS)


def block_rows(slot):
    return pl.ds(pl.multiple_of(slot * BLOCK * WORDS, BLOCK * WORDS), BLOCK * WORDS)


def unrolled_loop(lo, hi, unroll, body, carry):
    for width in (*unroll, 1):
        full = (hi - lo) // width

        def several(t, c, lo=lo, width=width):
            for j in range(width):
                c = body(lo + t * width + j, c)
            return c

        carry = lax.fori_loop(0, full, several, carry)
        lo = lo + full * width
    return carry


def packed_rows(n, slot):
    return 3 * n + n * slot // LANES


def pack(v, pad, slot):
    n = v[0].shape[0]
    gap = LANES - pad
    lane = lax.broadcasted_iota(jnp.int32, (n, LANES), 1)
    mixed = jnp.where(lane < pad, v[1], pltpu.roll(v[3], pad, 1))
    groups = LANES // slot
    size = n // groups
    thin = lane[:size]
    rest = jnp.zeros((size, LANES), F32)
    for a in range(groups):
        moved = pltpu.roll(v[3][a * size:(a + 1) * size], (slot * a - gap) % LANES, 1)
        rest = jnp.where((thin >= slot * a) & (thin < slot * (a + 1)), moved, rest)
    return v[0], v[2], mixed, rest


def unpack(first, third, mixed, rest, pad, slot):
    n = first.shape[0]
    gap = LANES - pad
    lane = lax.broadcasted_iota(jnp.int32, (n, LANES), 1)
    tail = jnp.concatenate([pltpu.roll(rest, (gap - slot * a) % LANES, 1) for a in range(LANES // slot)], axis=0)
    last = jnp.where(lane < gap, pltpu.roll(mixed, LANES - pad, 1), tail)
    return [first, jnp.where(lane < pad, mixed, 0.0), third, jnp.where(lane < pad, last, 0.0)], last


def put_packed(ref, base, v, pad, slot):
    n = v[0].shape[0]
    for c, part in enumerate(pack(v, pad, slot)):
        ref[pl.ds(pl.multiple_of(base + c * n, 16), part.shape[0]), :] = part.astype(ref.dtype)


def get_packed(ref, base, n, pad, slot):
    at = [pl.ds(pl.multiple_of(base + c * n, 16), n if c < 3 else n * slot // LANES) for c in range(4)]
    return unpack(*[ref[i, :].astype(F32) for i in at], pad, slot)


def params(**kw):
    return pltpu.CompilerParams(dimension_semantics=("arbitrary",), vmem_limit_bytes=VMEM_LIMIT, **kw)


def whole(shape):
    return pl.BlockSpec(shape, lambda *_: (0,) * len(shape), pipeline_mode=pl.Buffered(1))


def convert_block(src, state, dst, half):
    pad = half - LANES
    sub8 = lax.broadcasted_iota(jnp.int32, (8, LANES), 0)
    for r0 in range(0, BLOCK, SUB):
        cols = slice(r0, r0 + SUB)
        if state is not None:
            low = jnp.where(sub8 == 7, jnp.broadcast_to(state[:, cols], (8, LANES)), 0.0)
        else:
            low = jnp.zeros((8, LANES), F32)
        gap = jnp.zeros((LANES - pad - 8, LANES), F32)
        none = jnp.zeros((8, LANES), F32)
        w = [
            src[:LANES, cols],
            jnp.concatenate([src[LANES:half, cols], gap, none], axis=0),
            src[half:half + LANES, cols],
            jnp.concatenate([src[half + LANES:, cols], gap, low], axis=0),
        ]
        for c in range(WORDS):
            dst[pl.ds(r0 * WORDS + c, SUB, stride=WORDS), :] = w[c].T


def relation_words_kernel(half, src, dst):
    convert_block(src, None, dst, half)


def entity_first_kernel(sizes, half, xsrc, xdst, xoff, src, state, dst, xh, xt, rows, sems):
    step = pl.program_id(0)
    convert_block(src, state, dst, half)
    copy_rows(xsrc, lambda k: xdst[k], xoff[step], xoff[step + 1], dst, rows)

    @pl.when(step == pl.num_programs(0) - 1)
    def _():
        store_entity_rows(sizes, half, rows, xh, xt, sems.at[0])


def relation_words(table_t):
    dim, rows = table_t.shape
    blocks = pl.cdiv(rows, BLOCK)
    return pl.pallas_call(
        functools.partial(relation_words_kernel, dim // 2),
        grid=(blocks,),
        in_specs=[pl.BlockSpec((dim, BLOCK), lambda b: (0, b))],
        out_specs=pl.BlockSpec((BLOCK * WORDS, LANES), lambda b: (b, 0)),
        out_shape=jax.ShapeDtypeStruct((blocks * BLOCK * WORDS, LANES), F32),
        compiler_params=params(),
        name="relation_words",
    )(table_t)


def entity_first(table_t, state, sizes, ext):
    dim, rows = table_t.shape
    heads, tails, negs = sizes
    blocks = rows // BLOCK
    near = near_rows(tails, negs)
    return pl.pallas_call(
        functools.partial(entity_first_kernel, sizes, dim // 2),
        grid_spec=pltpu.PrefetchScalarGridSpec(
            num_scalar_prefetch=3, grid=(blocks,),
            in_specs=[pl.BlockSpec((dim, BLOCK), lambda b, *_: (0, b)), pl.BlockSpec((None, 1, BLOCK), lambda b, *_: (b, 0, 0))],
            out_specs=[pl.BlockSpec((BLOCK * WORDS, LANES), lambda b, *_: (b, 0)), ANY, whole((near, LANES))],
            scratch_shapes=[pltpu.VMEM((sum(sizes) * WORDS, LANES), F32), pltpu.SemaphoreType.DMA((1,))]),
        out_shape=[jax.ShapeDtypeStruct((rows * WORDS, LANES), F32), jax.ShapeDtypeStruct((heads * WORDS, LANES), F32),
                   jax.ShapeDtypeStruct((near, LANES), BF16)],
        compiler_params=params(),
        name="entity_first",
    )(*ext, table_t, state.reshape(blocks, 1, BLOCK))


def sweep(table, ring, load_sems, store, blocks, body):
    def load(b):
        slot = lax.rem(b, SLOTS)
        at = block_rows(b)
        return pltpu.make_async_copy(table.at[at], ring.at[block_rows(slot)], load_sems.at[slot])

    load(0).start()
    load(1).start()

    def turn(b, carry):
        load(b).wait()

        @pl.when(b >= 2)
        def _():
            store(b - 2).wait()

        @pl.when(b + 2 < blocks)
        def _():
            load(b + 2).start()

        body(b, ring.at[block_rows(lax.rem(b, SLOTS))])
        store(b).start()
        return carry

    lax.fori_loop(0, blocks, turn, 0)
    store(blocks - 2).wait()
    store(blocks - 1).wait()


def apply_step(w, g, lane, dim, lr):
    total = (g[0] * g[0] + g[1] * g[1]) + (g[2] * g[2] + g[3] * g[3])
    last = lane == LANES - 1
    state = jnp.sum(total * (1.0 / dim) + jnp.where(last, w[3], 0.0), axis=1, keepdims=True)
    scale = lr * lax.rsqrt(state + EPSILON)
    new = [w[c] - g[c] * scale for c in range(WORDS)]
    return [*new[:3], jnp.where(last, state, new[3])]


def sum_terms(src, dst, lo, hi, terms, acc):
    def body(k, carry):
        prev, total = carry
        at = dst[k]
        total = jnp.where(at == prev, total, 0.0) + terms[word(src[k]), :]
        acc[word(at), :] = total
        return at, total

    unrolled_loop(lo, hi, UNROLL, body, (jnp.int32(-1), jnp.zeros((WORDS, LANES), F32)))


def take_sums(acc, at):
    sums = [acc[i, :] for i in at]
    for i in at:
        acc[i, :] = jnp.zeros((SUB, LANES), F32)
    return sums


def update_words(ref, acc, dim, lr):
    lane = lax.broadcasted_iota(jnp.int32, (SUB, LANES), 1)
    for r0 in range(0, BLOCK, SUB):
        at = [pl.ds(r0 * WORDS + c, SUB, stride=WORDS) for c in range(WORDS)]
        w = apply_step([ref[i, :] for i in at], take_sums(acc, at), lane, dim, lr)
        for c in range(WORDS):
            ref[at[c], :] = w[c]


def update_columns(ref, acc, dst, state_out, dim, lr):
    half = dim // 2
    pad = half - LANES
    lane = lax.broadcasted_iota(jnp.int32, (SUB, LANES), 1)
    for r0 in range(0, BLOCK, SUB):
        at = [pl.ds(r0 * WORDS + c, SUB, stride=WORDS) for c in range(WORDS)]
        w = apply_step([ref[i, :] for i in at], take_sums(acc, at), lane, dim, lr)
        cols = slice(r0, r0 + SUB)
        dst[:LANES, cols] = w[0].T
        dst[LANES:half, cols] = w[1].T[:pad]
        dst[half:half + LANES, cols] = w[2].T
        w3 = w[3].T
        dst[half + LANES:, cols] = w3[:pad]
        if state_out is not None:
            state_out[:, cols] = w3[LANES - 1:]


def place_parts(rep, parts, dst, sems, first):
    size = parts[0].shape[0]
    side = len(parts) // 2
    copies = []
    for n, part in enumerate(parts):
        at = 0 if side == 0 else (rep * side + n if n < side else (1 - rep) * side + n - side) * size
        copies.append(pltpu.make_async_copy(part, dst.at[pl.ds(pl.multiple_of(at, 16) if side else 0, size)], sems.at[first + n]))
    return copies


def load_entity_terms(sizes, half, rep, gh, qb, gn, terms, queries, neg_terms, sems):
    heads, tails, negs = sizes
    pad = half - LANES
    head_copy = pltpu.make_async_copy(gh, terms.at[pl.ds(0, heads * WORDS)], sems.at[0])
    query_copies = place_parts(rep, qb, queries, sems, 1)
    neg_copies = place_parts(rep, gn, neg_terms, sems, 1 + len(qb))
    for c in (*query_copies, *neg_copies, head_copy):
        c.start()
    for c in query_copies:
        c.wait()

    def body(t, carry):
        q, last = get_packed(queries, t * packed_rows(TILE, QUERY_SLOT), TILE, pad, QUERY_SLOT)
        dp = dp_of(last, pad)
        for c in range(WORDS):
            terms[pl.ds((heads + t * TILE) * WORDS + c, TILE, stride=WORDS), :] = dp * q[c]
        return carry

    lax.fori_loop(0, tails // TILE, body, 0)
    for c in neg_copies:
        c.wait()
    for c, v in enumerate(get_packed(neg_terms, 0, negs, pad, ROW_SLOT)[0]):
        terms[pl.ds((heads + tails) * WORDS + c, negs, stride=WORDS), :] = v
    head_copy.wait()


def store_entity_rows(sizes, half, rows, xh, xt, sem):
    heads, tails, negs = sizes
    pad = half - LANES
    copy = pltpu.make_async_copy(rows.at[pl.ds(0, heads * WORDS)], xh, sem)
    copy.start()

    def move(r0, n, base):
        v = [rows[pl.ds((heads + r0) * WORDS + c, n, stride=WORDS), :] for c in range(WORDS)]
        put_packed(xt, base, v, pad, ROW_SLOT)

    def body(t, carry):
        move(t * TILE, TILE, t * packed_rows(TILE, ROW_SLOT))
        return carry

    lax.fori_loop(0, tails // TILE, body, 0)
    move(tails, negs, tails // TILE * packed_rows(TILE, ROW_SLOT))
    copy.wait()


def near_rows(tails, negs):
    return tails // TILE * packed_rows(TILE, ROW_SLOT) + packed_rows(negs, ROW_SLOT)


def fetch_rows(row, spot, count, table, rows, sem):
    def body(k, carry):
        pltpu.make_async_copy(table.at[word(row[k])], rows.at[word(spot(k))], sem).start()
        return carry

    unrolled_loop(0, count, UNROLL, body, 0)
    size = pl.multiple_of(count * WORDS, WORDS)
    pltpu.make_async_copy(table.at[pl.ds(0, size)], rows.at[pl.ds(0, size)], sem).wait()


def relation_fetch_kernel(row, count, table, xr, rows, sems):
    fetch_rows(row, lambda k: k * WORDS, count[0], table, rows, sems.at[0])
    copy = pltpu.make_async_copy(rows, xr, sems.at[1])
    copy.start()
    copy.wait()


def entity_kernel(cfg, *refs):
    sizes, dim, lr, final, n_qb, n_gn = cfg
    it = iter(refs)
    place, usrc, udst, uoff = next(it), next(it), next(it), next(it)
    xsrc, xdst, xoff = (None, None, None) if final else (next(it), next(it), next(it))
    table, gh = next(it), next(it)
    qb = [next(it) for _ in range(n_qb)]
    gn = [next(it) for _ in range(n_gn)]
    out = next(it)
    if final:
        state_out = next(it)
    else:
        xh, xt = next(it), next(it)
    terms, queries, neg_terms, acc, ring = next(it), next(it), next(it), next(it), next(it)
    rows = None if final else next(it)
    cols = next(it) if final else None
    sems, load_sems, store_sems = next(it), next(it), next(it)
    blocks = table.shape[0] // (BLOCK * WORDS)
    acc[...] = jnp.zeros_like(acc)
    load_entity_terms(sizes, dim // 2, place[0], gh, qb, gn, terms, queries, neg_terms, sems)

    def store(b):
        if final:
            slot = lax.rem(b, 2)
            at = pl.ds(pl.multiple_of(b * BLOCK, BLOCK), BLOCK)
            return pltpu.make_async_copy(cols.at[slot], out.at[:, at], store_sems.at[slot])
        slot = lax.rem(b, SLOTS)
        at = block_rows(b)
        return pltpu.make_async_copy(ring.at[block_rows(slot)], out.at[at], store_sems.at[slot])

    def body(b, ref):
        sum_terms(usrc, udst, uoff[b], uoff[b + 1], terms, acc)
        if final:
            update_columns(ref, acc, cols.at[lax.rem(b, 2)], state_out.at[b], dim, lr)
        else:
            update_words(ref, acc, dim, lr)
            copy_rows(xsrc, lambda k: xdst[k], xoff[b], xoff[b + 1], ref, rows)

    sweep(table, ring, load_sems, store, blocks, body)
    if not final:
        store_entity_rows(sizes, dim // 2, rows, xh, xt, sems.at[0])


def copy_rows(src, dst, lo, hi, ref, rows):
    def body(k, carry):
        rows[word(dst(k)), :] = ref[word(src[k]), :]
        return carry

    unrolled_loop(lo, hi, UNROLL, body, 0)


def relation_fetch(table, edges, row, count):
    return pl.pallas_call(
        relation_fetch_kernel,
        grid_spec=pltpu.PrefetchScalarGridSpec(
            num_scalar_prefetch=2, grid=(1,), in_specs=[ANY], out_specs=ANY,
            scratch_shapes=[pltpu.VMEM((edges * WORDS, LANES), F32), pltpu.SemaphoreType.DMA((2,))]),
        out_shape=jax.ShapeDtypeStruct((edges * WORDS, LANES), F32),
        compiler_params=params(),
        name="relation_fetch",
    )(row, count, table)


def entity_pass(table, sizes, dim, lr, place, upd, gh, qb, gn, ext=None):
    heads, tails, negs = sizes
    final = ext is None
    blocks = table.shape[0] // (BLOCK * WORDS)
    total = sum(sizes) * WORDS
    scalars = [place, *upd, *(() if final else ext)]
    parts = (gh, *qb, *gn)
    scratch = [
        pltpu.VMEM((total, LANES), F32),
        pltpu.VMEM((sum(p.shape[0] for p in qb), LANES), BF16),
        pltpu.VMEM((sum(p.shape[0] for p in gn), LANES), F32),
        pltpu.VMEM((BLOCK * WORDS, LANES), F32),
        pltpu.VMEM((SLOTS * BLOCK * WORDS, LANES), F32),
    ]
    if final:
        outs = [ANY, whole((blocks, 1, BLOCK))]
        shapes = [jax.ShapeDtypeStruct((dim, blocks * BLOCK), F32), jax.ShapeDtypeStruct((blocks, 1, BLOCK), F32)]
        scratch.append(pltpu.VMEM((2, dim, BLOCK), F32))
    else:
        outs = [ANY, ANY, whole((near_rows(tails, negs), LANES))]
        shapes = [jax.ShapeDtypeStruct(table.shape, F32), jax.ShapeDtypeStruct((heads * WORDS, LANES), F32),
                  jax.ShapeDtypeStruct((near_rows(tails, negs), LANES), BF16)]
        scratch.append(pltpu.VMEM((total, LANES), F32))
    scratch += [pltpu.SemaphoreType.DMA((len(parts),)), pltpu.SemaphoreType.DMA((SLOTS,)), pltpu.SemaphoreType.DMA((SLOTS,))]
    return pl.pallas_call(
        functools.partial(entity_kernel, (sizes, dim, lr, final, len(qb), len(gn))),
        grid_spec=pltpu.PrefetchScalarGridSpec(
            num_scalar_prefetch=len(scalars), grid=(1,), in_specs=[ANY] * (1 + len(parts)), out_specs=outs, scratch_shapes=scratch),
        out_shape=shapes,
        input_output_aliases={} if final else {len(scalars): 0},
        compiler_params=params(),
        name="entity_last" if final else "entity_pass",
    )(*scalars, table, *parts)


def load_relation_terms(part, pad, counts, parts, terms, stages, sems):
    shared = parts[0]
    size = part // TILE * packed_rows(TILE, ROW_SLOT)
    copies = []
    for j in range(8):
        copies.append(pltpu.make_async_copy(shared.at[pl.ds(j * size, size)], stages[j // 4].at[pl.ds(j % 4 * BLOCK * WORDS, size)], sems.at[j]))
    if len(parts) > 1:
        copies.append(pltpu.make_async_copy(parts[1], terms.at[pl.ds(8 * part * WORDS, parts[1].shape[0])], sems.at[8]))
    for c in copies:
        c.start()
    for c in copies:
        c.wait()
    tiles = part // TILE
    for side in range(2):
        def body(i, carry, side=side):
            slot = i // tiles
            t = lax.rem(i, tiles)

            @pl.when(side * part + t * TILE < counts[slot])
            def _():
                v, _ = get_packed(stages[side], slot * BLOCK * WORDS + t * packed_rows(TILE, ROW_SLOT), TILE, pad, ROW_SLOT)
                for c in range(WORDS):
                    terms[pl.ds(((side * 4 + slot) * part + t * TILE) * WORDS + c, TILE, stride=WORDS), :] = v[c]

            return carry

        lax.fori_loop(0, 4 * tiles, body, 0)


def relation_kernel(cfg, *refs):
    dim, lr, part, n_parts = cfg
    usrc, udst, uoff, counts, xsrc, xoff, table = refs[:7]
    parts = refs[7:7 + n_parts]
    out, xr, terms, acc, ring, rows, sems, load_sems, store_sems = refs[7 + n_parts:]
    blocks = table.shape[0] // (BLOCK * WORDS)
    acc[...] = jnp.zeros_like(acc)
    load_relation_terms(part, dim // 2 - LANES, counts, parts, terms, (ring, rows), sems)

    def store(b):
        slot = lax.rem(b, SLOTS)
        at = block_rows(b)
        return pltpu.make_async_copy(ring.at[block_rows(slot)], out.at[at], store_sems.at[slot])

    def body(b, ref):
        sum_terms(usrc, udst, uoff[b], uoff[b + 1], terms, acc)
        update_words(ref, acc, dim, lr)
        copy_rows(xsrc, lambda k: k * WORDS, xoff[b], xoff[b + 1], ref, rows)

    sweep(table, ring, load_sems, store, blocks, body)
    copy = pltpu.make_async_copy(rows, xr, sems.at[0])
    copy.start()
    copy.wait()


def relation_last_kernel(cfg, *refs):
    dim, lr, part, n_parts = cfg
    usrc, udst, uoff, counts, src = refs[:5]
    parts = refs[5:5 + n_parts]
    dst, terms, acc, stage_a, stage_b, sems = refs[5 + n_parts:]
    step = pl.program_id(0)

    @pl.when(step == 0)
    def _():
        acc[...] = jnp.zeros_like(acc)
        load_relation_terms(part, dim // 2 - LANES, counts, parts, terms, (stage_a, stage_b), sems)

    sum_terms(usrc, udst, uoff[step], uoff[step + 1], terms, acc)
    update_columns(src, acc, dst, None, dim, lr)


def relation_pass(table, edges, part, dim, lr, upd, parts, ext):
    count = 8 * part * WORDS + sum(p.shape[0] for p in parts[1:])
    scalars = [*upd, *ext]
    return pl.pallas_call(
        functools.partial(relation_kernel, (dim, lr, part, len(parts))),
        grid_spec=pltpu.PrefetchScalarGridSpec(
            num_scalar_prefetch=len(scalars), grid=(1,), in_specs=[ANY] * (1 + len(parts)), out_specs=[ANY, ANY],
            scratch_shapes=[
                pltpu.VMEM((count, LANES), F32),
                pltpu.VMEM((BLOCK * WORDS, LANES), F32),
                pltpu.VMEM((SLOTS * BLOCK * WORDS, LANES), F32),
                pltpu.VMEM((4 * BLOCK * WORDS, LANES), F32),
                pltpu.SemaphoreType.DMA((9,)),
                pltpu.SemaphoreType.DMA((SLOTS,)),
                pltpu.SemaphoreType.DMA((SLOTS,)),
            ]),
        out_shape=[jax.ShapeDtypeStruct(table.shape, F32), jax.ShapeDtypeStruct((edges * WORDS, LANES), F32)],
        input_output_aliases={len(scalars): 0},
        compiler_params=params(),
        name="relation_pass",
    )(*scalars, table, *parts)


def relation_last(table, n_rel, part, dim, lr, upd, parts):
    count = 8 * part * WORDS + sum(p.shape[0] for p in parts[1:])
    return pl.pallas_call(
        functools.partial(relation_last_kernel, (dim, lr, part, len(parts))),
        grid_spec=pltpu.PrefetchScalarGridSpec(
            num_scalar_prefetch=len(upd), grid=(table.shape[0] // (BLOCK * WORDS),),
            in_specs=[pl.BlockSpec((BLOCK * WORDS, LANES), lambda b, *_: (b, 0))] + [ANY] * len(parts),
            out_specs=pl.BlockSpec((dim, BLOCK), lambda b, *_: (0, b)),
            scratch_shapes=[
                pltpu.VMEM((count, LANES), F32),
                pltpu.VMEM((BLOCK * WORDS, LANES), F32),
                pltpu.VMEM((4 * BLOCK * WORDS, LANES), F32),
                pltpu.VMEM((4 * BLOCK * WORDS, LANES), F32),
                pltpu.SemaphoreType.DMA((9,)),
            ]),
        out_shape=jax.ShapeDtypeStruct((dim, n_rel), F32),
        compiler_params=params(),
        name="relation_last",
    )(*upd, table, *parts)


def edge_rows(ref, keep, keep_data):
    v = [ref[pl.ds(c, TILE, stride=WORDS), :] for c in range(WORDS)]
    return [jnp.where(keep_data if c % 2 else keep, v[c], 0.0) for c in range(WORDS)]


def edge_masks(start, n, pad):
    row = lax.broadcasted_iota(jnp.int32, (TILE, LANES), 0) + start
    lane = lax.broadcasted_iota(jnp.int32, (TILE, LANES), 1)
    keep = row < n
    return lane, keep, keep & (lane < pad)


def fetch_negatives(near, neg_in, nb, pad, sem):
    copy = pltpu.make_async_copy(near.at[pl.ds(near.shape[0] - neg_in.shape[0], neg_in.shape[0])], neg_in, sem)
    copy.start()
    copy.wait()
    for c, v in enumerate(get_packed(neg_in, 0, nb.shape[0], pad, ROW_SLOT)[0]):
        nb[:, LANES * c:LANES * (c + 1)] = v.astype(BF16)


def score_kernel(half, info, xh, xr, tb, near, qb_out, ds_out, gn, loss, neg_in, nb, gacc, sem):
    step = pl.program_id(0)
    pad = half - LANES
    n = info[0]
    start = step * TILE

    @pl.when(step == 0)
    def _():
        gacc[...] = jnp.zeros_like(gacc)
        loss[0, 0] = 0.0
        fetch_negatives(near, neg_in, nb, pad, sem)

    @pl.when(start < n)
    def _():
        lane, keep, keep_data = edge_masks(start, n, pad)
        h = edge_rows(xh, keep, keep_data)
        r = edge_rows(xr, keep, keep_data)
        q = [h[0] * r[0] - h[2] * r[2], h[1] * r[1] - h[3] * r[3], h[0] * r[2] + h[2] * r[0], h[1] * r[3] + h[3] * r[1]]
        qc = [v.astype(BF16) for v in q]
        query = jnp.concatenate(qc, axis=1)
        wide = [v.astype(F32) for v in qc]
        tail = [jnp.where(keep, v, 0.0) for v in get_packed(tb, 0, TILE, pad, ROW_SLOT)[0]]
        prod = [wide[c] * tail[c] for c in range(WORDS)]
        pos = jnp.sum((prod[0] + prod[1]) + (prod[2] + prod[3]), axis=1, keepdims=True)
        score = lax.dot_general(query, nb[...], (((1,), (1,)), ((), ())), preferred_element_type=F32)
        top = jnp.maximum(jnp.max(score, axis=1, keepdims=True), pos)
        pos_exp = jnp.exp(pos - top)
        neg_exp = jnp.exp(score - top)
        total = pos_exp + jnp.sum(neg_exp, axis=1, keepdims=True)
        weight = jnp.where(keep[:, :1], 1.0, 0.0)
        loss[0, 0] += jnp.sum(weight * ((top + jnp.log(total)) - pos))
        inverse = 1.0 / total
        dp = weight * (pos_exp * inverse - 1.0)
        ds = ((weight * inverse) * neg_exp).astype(BF16)
        ds_out[...] = ds
        gacc[...] += lax.dot_general(ds, query, (((0,), (0,)), ((), ())), preferred_element_type=F32)
        hi = dp.astype(BF16).astype(F32)
        mid = (dp - hi).astype(BF16).astype(F32)
        low = (dp - hi) - mid
        q3 = jnp.where(lane == pad, hi, jnp.where(lane == pad + 1, mid, jnp.where(lane == pad + 2, low, wide[3])))
        put_packed(qb_out, 0, [*wide[:3], q3], pad, QUERY_SLOT)

    @pl.when(step == pl.num_programs(0) - 1)
    def _():
        put_packed(gn, 0, [gacc[:, LANES * c:LANES * (c + 1)] for c in range(WORDS)], pad, ROW_SLOT)


def dp_of(last, pad):
    return (last[:, pad:pad + 1] + last[:, pad + 1:pad + 2]) + last[:, pad + 2:pad + 3]


def gradient_kernel(cfg, spot, info, xh, xr, tb, near, qb, ds, gh, ua, ub, neg_in, nb, gr, uniq, held, sem):
    cap, edges, half = cfg
    step = pl.program_id(0)
    pad = half - LANES
    n = info[0]
    start = step * TILE

    @pl.when(step == 0)
    def _():
        fetch_negatives(near, neg_in, nb, pad, sem)

    @pl.when(start < n)
    def _():
        _, keep, keep_data = edge_masks(start, n, pad)
        h = edge_rows(xh, keep, keep_data)
        r = edge_rows(xr, keep, keep_data)
        tail = [jnp.where(keep, v, 0.0) for v in get_packed(tb, 0, TILE, pad, ROW_SLOT)[0]]
        dp = dp_of(get_packed(qb, 0, TILE, pad, QUERY_SLOT)[1], pad)
        gq = lax.dot_general(ds[...], nb[...], (((1,), (0,)), ((), ())), preferred_element_type=F32)
        g = [dp * tail[c] + gq[:, LANES * c:LANES * (c + 1)] for c in range(WORDS)]
        out = [g[0] * r[0] + g[2] * r[2], g[1] * r[1] + g[3] * r[3], g[2] * r[0] - g[0] * r[2], g[3] * r[1] - g[1] * r[3]]
        rel_g = [g[0] * h[0] + g[2] * h[2], g[1] * h[1] + g[3] * h[3], g[2] * h[0] - g[0] * h[2], g[3] * h[1] - g[1] * h[3]]
        for c in range(WORDS):
            gh[pl.ds(c, TILE, stride=WORDS), :] = out[c]
            gr[pl.ds(c, TILE, stride=WORDS), :] = rel_g[c]

        def body(k, carry):
            prev, acc = carry
            at = spot[k]
            acc = jnp.where(at == prev, acc, 0.0) + gr[words_of(k - start), :]
            uniq[word(at), :] = acc
            return at, acc

        prev = jnp.where(step > 0, spot[jnp.maximum(start - 1, 0)], -1)
        _, acc = unrolled_loop(start, jnp.minimum(start + TILE, n), UNROLL, body, (prev, held[:WORDS, :]))
        held[:WORDS, :] = acc

    @pl.when(step == pl.num_programs(0) - 1)
    def _():
        more = pltpu.make_async_copy(uniq.at[pl.ds(cap * WORDS, (edges - cap) * WORDS)], ub, sem)
        more.start()
        part = cap // 2

        def body(t, carry):
            r0 = info[1] * part + t * TILE
            v = [uniq[pl.ds(r0 * WORDS + c, TILE, stride=WORDS), :] for c in range(WORDS)]
            put_packed(ua, t * packed_rows(TILE, ROW_SLOT), v, pad, ROW_SLOT)
            return carry

        lax.fori_loop(0, part // TILE, body, 0)
        more.wait()


def bucket_specs(negs):
    word_spec = pl.BlockSpec((TILE * WORDS, LANES), lambda t, *_: (t, 0))
    tail_spec = pl.BlockSpec((packed_rows(TILE, ROW_SLOT), LANES), lambda t, *_: (t, 0))
    query_spec = pl.BlockSpec((packed_rows(TILE, QUERY_SLOT), LANES), lambda t, *_: (t, 0))
    return word_spec, tail_spec, query_spec, pl.BlockSpec((TILE, negs), lambda t, *_: (t, 0))


def scores(info, xh, xr, near, edges, negs, half):
    word_spec, tail_spec, query_spec, prob_spec = bucket_specs(negs)
    neg_rows = packed_rows(negs, ROW_SLOT)
    return pl.pallas_call(
        functools.partial(score_kernel, half),
        grid_spec=pltpu.PrefetchScalarGridSpec(
            num_scalar_prefetch=1,
            grid=(edges // TILE,),
            in_specs=[word_spec, word_spec, tail_spec, ANY],
            out_specs=[query_spec, prob_spec, whole((neg_rows, LANES)),
                       pl.BlockSpec((1, 1), lambda *_: (0, 0), memory_space=pltpu.SMEM)],
            scratch_shapes=[
                pltpu.VMEM((neg_rows, LANES), BF16),
                pltpu.VMEM((negs, WIDE), BF16),
                pltpu.VMEM((negs, WIDE), F32),
                pltpu.SemaphoreType.DMA(()),
            ]),
        out_shape=[
            jax.ShapeDtypeStruct((edges // TILE * packed_rows(TILE, QUERY_SLOT), LANES), BF16),
            jax.ShapeDtypeStruct((edges, negs), BF16),
            jax.ShapeDtypeStruct((neg_rows, LANES), F32),
            jax.ShapeDtypeStruct((1, 1), F32),
        ],
        compiler_params=params(),
        name="scores",
    )(info, xh, xr, near, near)


def gradients(spot, info, xh, xr, near, qb, ds, negs, cap, half):
    edges = spot.shape[0]
    word_spec, tail_spec, query_spec, prob_spec = bucket_specs(negs)
    shared_rows = cap // 2 // TILE * packed_rows(TILE, ROW_SLOT)
    return pl.pallas_call(
        functools.partial(gradient_kernel, (cap, edges, half)),
        grid_spec=pltpu.PrefetchScalarGridSpec(
            num_scalar_prefetch=2,
            grid=(edges // TILE,),
            in_specs=[word_spec, word_spec, tail_spec, ANY, query_spec, prob_spec],
            out_specs=[word_spec, whole((shared_rows, LANES)), ANY],
            scratch_shapes=[
                pltpu.VMEM((packed_rows(negs, ROW_SLOT), LANES), BF16),
                pltpu.VMEM((negs, WIDE), BF16),
                pltpu.VMEM((TILE * WORDS, LANES), F32),
                pltpu.VMEM((edges * WORDS, LANES), F32),
                pltpu.VMEM((8, LANES), F32),
                pltpu.SemaphoreType.DMA(()),
            ]),
        out_shape=[
            jax.ShapeDtypeStruct((edges * WORDS, LANES), F32),
            jax.ShapeDtypeStruct((shared_rows, LANES), F32),
            jax.ShapeDtypeStruct(((edges - cap) * WORDS, LANES), F32),
        ],
        compiler_params=params(),
        name="gradients",
    )(spot, info, xh, xr, near, near, qb, ds)


def running_count(flags):
    lead = flags.shape[:-1]
    n = flags.shape[-1] // LANES
    x = flags.reshape(*lead, n, LANES).astype(F32)
    tri = jnp.triu(jnp.ones((LANES, LANES), F32))
    inner = jnp.einsum('...k,kl->...l', x, tri, precision=lax.Precision.HIGHEST)
    before = jnp.einsum('...k,kl->...l', inner[..., -1], jnp.triu(jnp.ones((n, n), F32), 1), precision=lax.Precision.HIGHEST)
    return (inner + before[..., None]).astype(jnp.int32).reshape(flags.shape)


def halves(x, rep, count):
    size = x.shape[0] // 2 // count
    return [lax.dynamic_slice_in_dim(x, (rep * count + j) * size, size) for j in range(count)]


def offsets(keys, bounds):
    return jnp.sum(keys[:, None, :] < bounds[None, :, None], axis=2, dtype=jnp.int32)


def solution(mesh):
    groups = mesh.shape['ent']
    data_reps = mesh.shape['data']
    row_spec = P(('sweep', 'ent'), None)
    edge_spec = P(('sweep', 'ent'), None, 'data')

    def device_fn(ent_table, ent_state, rel_table, head_idx, tail_idx, rel_idx, edge_mask, neg_idx):
        part_rows, dim = ent_table.shape
        half = dim // 2
        n_rel = rel_table.shape[0]
        rounds = head_idx.shape[1]
        edges = head_idx.shape[2] * data_reps
        negs = neg_idx.shape[2]
        sizes = (edges, edges, negs)
        cap = edges // 2
        lr = LR_SCALE * dim ** -0.25
        me = lax.axis_index('ent')
        rep = lax.axis_index('data')

        rel_words = relation_words(rel_table.T)

        big = (NO_KEY >> 13) - 1
        order = jnp.where(edge_mask[0] > 0, rel_idx[0], big)
        packed = head_idx[0] * part_rows + tail_idx[0]
        both = lax.all_gather(jnp.stack([order, packed]), 'data', axis=2, tiled=True)
        spot = jnp.arange(edges, dtype=jnp.int32)
        order, packed = lax.sort((both[0] * edges + spot, both[1]), dimension=1, num_keys=1)
        rel_s = order // edges
        head_s = packed // part_rows
        tail_s = packed % part_rows
        live = rel_s < n_rel
        kept = jnp.sum(live, axis=1, dtype=jnp.int32)
        info = jnp.concatenate([jnp.where(live, rel_s, n_rel), jnp.where(live, tail_s, part_rows), neg_idx[0]], axis=1)
        every = lax.all_gather(info, 'ent', axis=0)
        every, fetch_from = lax.optimization_barrier((every, rel_words))
        xr = relation_fetch(fetch_from, edges, rel_s[0] * WORDS, kept[:1])

        far = jnp.stack([lax.dynamic_index_in_dim(every, (me - s) % groups, 0, False)[s, edges:] for s in range(rounds)])
        ids = jnp.concatenate([jnp.where(live, head_s, part_rows), far], axis=1)
        keys = jnp.where(ids < part_rows, (ids << SHIFT) + jnp.arange(sum(sizes), dtype=jnp.int32), NO_KEY)
        ent_key = lax.sort(keys, dimension=1, is_stable=False)
        ent_off = offsets(ent_key, jnp.arange(part_rows // BLOCK + 1, dtype=jnp.int32) * (BLOCK << SHIFT))
        ent_src = (ent_key & POS_MASK) * WORDS
        ent_dst = ((ent_key >> SHIFT) % BLOCK) * WORDS

        rels = every[:, :, :edges]
        prev = jnp.concatenate([jnp.full((groups, rounds, 1), -1, jnp.int32), rels[:, :, :-1]], axis=2)
        fresh = (rels != prev) & (rels < n_rel)
        slot = running_count(fresh) - 1
        over = jnp.max(slot[:, :, -1], axis=0) >= cap
        counts = (slot[:, :, -1] + 1).T
        own_spot = lax.dynamic_index_in_dim(slot, me, 0, False) * WORDS
        source = jnp.arange(groups, dtype=jnp.int32)[:, None, None]
        part = cap // data_reps
        first = (slot // part * groups + source) * part + slot % part
        slot = jnp.where(slot < cap, first, groups * cap + source * (edges - cap) + slot - cap)
        keys = jnp.where(fresh, (rels << SHIFT) + slot, NO_KEY).transpose(1, 0, 2).reshape(rounds, groups * edges)
        keys, ent_key = lax.optimization_barrier((keys, ent_key))
        rel_key = lax.sort(keys, dimension=1, is_stable=False)
        bounds = jnp.arange(pl.cdiv(n_rel, BLOCK) + 1, dtype=jnp.int32) * BLOCK
        rel_off = offsets(rel_key, bounds << SHIFT)
        rel_src = (rel_key & POS_MASK) * WORDS
        rel_dst = ((rel_key >> SHIFT) % BLOCK) * WORDS
        own_off = offsets(jnp.where(live, rel_s, NO_KEY), bounds)
        own_src = (rel_s % BLOCK) * WORDS
        info = jnp.stack([kept, jnp.full((rounds,), rep, jnp.int32)], axis=1)

        ent_args = (sizes, dim, lr)
        rel_args = (part, dim, lr)
        ent_words, xh, xt = entity_first(ent_table.T, ent_state, sizes, (ent_dst[0], ent_src[0], ent_off[0]))
        place = rep[None].astype(jnp.int32)
        swap = [(i, 1 - i) for i in range(data_reps)]
        losses = []
        for s in range(rounds):
            tn = xt if s == 0 else lax.ppermute(xt, 'ent', [(i, (i - s) % groups) for i in range(groups)])
            own_qb, ds, gn, loss = scores(info[s], xh, xr, tn, edges, negs, half)
            losses.append(loss[0, 0] / edges)
            gh, ua, ub = gradients(own_spot[s], info[s], xh, xr, tn, own_qb, ds, negs, cap, half)
            qb, gn = (own_qb,), (gn,)
            if s > 0:
                back = [(i, (i + s) % groups) for i in range(groups)]
                if s == groups // 2:
                    qb = [lax.ppermute(v, 'ent', back) for v in halves(qb[0], rep, 4)]
                    gn = [lax.ppermute(v, 'ent', back) for v in halves(gn[0], rep, 1)]
                    qb = (*qb, *[lax.ppermute(v, 'data', swap) for v in qb])
                    gn = (*gn, *[lax.ppermute(v, 'data', swap) for v in gn])
                else:
                    qb = (lax.ppermute(qb[0], 'ent', back),)
                    gn = (lax.ppermute(gn[0], 'ent', back),)
                qb, gn, ua = lax.optimization_barrier((qb, gn, ua))
            shared = lax.all_gather(ua, ('data', 'ent'), axis=0, tiled=True)

            final = s == rounds - 1
            ent_upd = (ent_src[s], ent_dst[s], ent_off[s])
            rel_upd = (rel_src[s], rel_dst[s], rel_off[s], counts[s])

            def relations(table, *parts, s=s, final=final, rel_upd=rel_upd):
                if final:
                    return (relation_last(table, n_rel, *rel_args, rel_upd, parts),)
                return relation_pass(table, edges, *rel_args, rel_upd, parts, (own_src[s + 1], own_off[s + 1]))

            def small(table, shared, ub, relations=relations):
                return relations(table, shared)

            def large(table, shared, ub, relations=relations):
                return relations(table, shared, lax.all_gather(ub, 'ent', axis=0, tiled=True))

            if final:
                ent_cols, state = entity_pass(ent_words, *ent_args, place, ent_upd, gh, qb, gn)
                (rel_cols,) = lax.cond(over[s], large, small, rel_words, shared, ub)
            else:
                ent_words, xh, xt = entity_pass(ent_words, *ent_args, place, ent_upd, gh, qb, gn, (ent_dst[s + 1], ent_src[s + 1], ent_off[s + 1]))
                rel_words, xr = lax.cond(over[s], large, small, rel_words, shared, ub)
        return ent_cols.T, state.reshape(part_rows), rel_cols.T, jnp.stack(losses)[None, :]

    return jax.shard_map(device_fn, mesh=mesh, in_specs=(row_spec, P(('sweep', 'ent')), P('sweep', None), edge_spec, edge_spec, edge_spec, edge_spec, P(('sweep', 'ent'), None, None)), out_specs=(row_spec, P(('sweep', 'ent')), P('sweep', None), row_spec), check_vma=False)
```

```python
import functools

import jax
import jax.numpy as jnp
from jax import lax
from jax.experimental import pallas as pl
from jax.experimental.pallas import tpu as pltpu
from jax.sharding import PartitionSpec as P

LR_SCALE = 0.2
EPSILON = 1e-8

LANES = 128
WORDS = 4
SHIFT = 14
POS_MASK = (1 << SHIFT) - 1
NO_KEY = 2**31 - 1
BLOCK = 1024
SUB = 128
SLOTS = 4
FIRST = 2
UNROLL = (16, 4)
ROW_SLOT = 16
QUERY_SLOT = 32
WIDE = WORDS * LANES
TILE = 512
CHUNK = 256
VMEM_LIMIT = 63 * 2**20
F32 = jnp.float32
BF16 = jnp.bfloat16
ANY = pl.BlockSpec(memory_space=pl.ANY)


def words_of(start):
    return pl.ds(pl.multiple_of(start * WORDS, WORDS), WORDS)


def word(start):
    return pl.ds(pl.multiple_of(start, WORDS), WORDS)


def block_rows(slot):
    return pl.ds(pl.multiple_of(slot * BLOCK * WORDS, BLOCK * WORDS), BLOCK * WORDS)


def unrolled_loop(lo, hi, unroll, body, carry):
    for width in (*unroll, 1):
        full = (hi - lo) // width

        def several(t, c, lo=lo, width=width):
            for j in range(width):
                c = body(lo + t * width + j, c)
            return c

        carry = lax.fori_loop(0, full, several, carry)
        lo = lo + full * width
    return carry


def packed_rows(n, slot):
    return 3 * n + n * slot // LANES


def pack(v, pad, slot):
    n = v[0].shape[0]
    gap = LANES - pad
    lane = lax.broadcasted_iota(jnp.int32, (n, LANES), 1)
    mixed = jnp.where(lane < pad, v[1], pltpu.roll(v[3], pad, 1))
    groups = LANES // slot
    size = n // groups
    thin = lane[:size]
    rest = jnp.zeros((size, LANES), F32)
    for a in range(groups):
        moved = pltpu.roll(v[3][a * size:(a + 1) * size], (slot * a - gap) % LANES, 1)
        rest = jnp.where((thin >= slot * a) & (thin < slot * (a + 1)), moved, rest)
    return v[0], v[2], mixed, rest


def unpack(first, third, mixed, rest, pad, slot):
    n = first.shape[0]
    gap = LANES - pad
    lane = lax.broadcasted_iota(jnp.int32, (n, LANES), 1)
    tail = jnp.concatenate([pltpu.roll(rest, (gap - slot * a) % LANES, 1) for a in range(LANES // slot)], axis=0)
    last = jnp.where(lane < gap, pltpu.roll(mixed, LANES - pad, 1), tail)
    return [first, jnp.where(lane < pad, mixed, 0.0), third, jnp.where(lane < pad, last, 0.0)], last


def put_packed(ref, base, v, pad, slot):
    n = v[0].shape[0]
    for c, part in enumerate(pack(v, pad, slot)):
        ref[pl.ds(pl.multiple_of(base + c * n, 16), part.shape[0]), :] = part.astype(ref.dtype)


def get_packed(ref, base, n, pad, slot):
    at = [pl.ds(pl.multiple_of(base + c * n, 16), n if c < 3 else n * slot // LANES) for c in range(4)]
    return unpack(*[ref[i, :].astype(F32) for i in at], pad, slot)


def params(**kw):
    return pltpu.CompilerParams(dimension_semantics=("arbitrary",), vmem_limit_bytes=VMEM_LIMIT, **kw)


def whole(shape):
    return pl.BlockSpec(shape, lambda *_: (0,) * len(shape), pipeline_mode=pl.Buffered(1))


def convert_block(src, state, dst, half, first=0):
    pad = half - LANES
    sub8 = lax.broadcasted_iota(jnp.int32, (8, LANES), 0)
    for r0 in range(0, BLOCK, SUB):
        cols = slice(first + r0, first + r0 + SUB)
        if state is not None:
            low = jnp.where(sub8 == 7, jnp.broadcast_to(state[:, cols], (8, LANES)), 0.0)
        else:
            low = jnp.zeros((8, LANES), F32)
        gap = jnp.zeros((LANES - pad - 8, LANES), F32)
        none = jnp.zeros((8, LANES), F32)
        w = [
            src[:LANES, cols],
            jnp.concatenate([src[LANES:half, cols], gap, none], axis=0),
            src[half:half + LANES, cols],
            jnp.concatenate([src[half + LANES:, cols], gap, low], axis=0),
        ]
        for c in range(WORDS):
            dst[pl.ds(r0 * WORDS + c, SUB, stride=WORDS), :] = w[c].T


def relation_words_kernel(half, src, dst):
    for j in range(dst.shape[0] // (BLOCK * WORDS)):
        convert_block(src, None, dst.at[block_rows(j)], half, j * BLOCK)


def entity_first_kernel(sizes, half, xsrc, xdst, xoff, src, state, dst, xh, xt, rows, sems):
    step = pl.program_id(0)
    for j in range(FIRST):
        part = dst.at[block_rows(j)]
        convert_block(src, state, part, half, j * BLOCK)
        b = step * FIRST + j
        copy_rows(xsrc, lambda k: xdst[k], xoff[b], xoff[b + 1], part, rows)

    @pl.when(step == pl.num_programs(0) - 1)
    def _():
        store_entity_rows(sizes, half, rows, xh, xt, sems.at[0])


def relation_words(table_t):
    dim, rows = table_t.shape
    blocks = pl.cdiv(rows, BLOCK)
    group = 3 if blocks % 3 == 0 else 1
    return pl.pallas_call(
        functools.partial(relation_words_kernel, dim // 2),
        grid=(blocks // group,),
        in_specs=[pl.BlockSpec((dim, BLOCK * group), lambda b: (0, b))],
        out_specs=pl.BlockSpec((BLOCK * group * WORDS, LANES), lambda b: (b, 0)),
        out_shape=jax.ShapeDtypeStruct((blocks * BLOCK * WORDS, LANES), F32),
        compiler_params=params(),
        name="relation_words",
    )(table_t)


def entity_first(table_t, state, sizes, ext):
    dim, rows = table_t.shape
    heads, tails, negs = sizes
    steps = rows // (BLOCK * FIRST)
    near = near_rows(tails, negs)
    return pl.pallas_call(
        functools.partial(entity_first_kernel, sizes, dim // 2),
        grid_spec=pltpu.PrefetchScalarGridSpec(
            num_scalar_prefetch=3, grid=(steps,),
            in_specs=[pl.BlockSpec((dim, BLOCK * FIRST), lambda b, *_: (0, b)),
                      pl.BlockSpec((None, 1, BLOCK * FIRST), lambda b, *_: (b, 0, 0))],
            out_specs=[pl.BlockSpec((BLOCK * FIRST * WORDS, LANES), lambda b, *_: (b, 0)), ANY, whole((near, LANES))],
            scratch_shapes=[pltpu.VMEM((sum(sizes) * WORDS, LANES), F32), pltpu.SemaphoreType.DMA((1,))]),
        out_shape=[jax.ShapeDtypeStruct((rows * WORDS, LANES), F32), jax.ShapeDtypeStruct((heads * WORDS, LANES), F32),
                   jax.ShapeDtypeStruct((near, LANES), BF16)],
        compiler_params=params(),
        name="entity_first",
    )(*ext, table_t, state.reshape(steps, 1, BLOCK * FIRST))


def block_load(table, ring, load_sems, b):
    slot = lax.rem(b, SLOTS)
    return pltpu.make_async_copy(table.at[block_rows(b)], ring.at[block_rows(slot)], load_sems.at[slot])


def start_sweep(table, ring, load_sems):
    for b in range(2):
        block_load(table, ring, load_sems, b).start()


def sweep(table, ring, load_sems, store, blocks, body):
    load = functools.partial(block_load, table, ring, load_sems)

    def turn(b, carry):
        load(b).wait()

        @pl.when(b >= 2)
        def _():
            store(b - 2).wait()

        @pl.when(b + 2 < blocks)
        def _():
            load(b + 2).start()

        body(b, ring.at[block_rows(lax.rem(b, SLOTS))])
        store(b).start()
        return carry

    lax.fori_loop(0, blocks, turn, 0)
    store(blocks - 2).wait()
    store(blocks - 1).wait()


def apply_step(w, g, lane, dim, lr):
    total = (g[0] * g[0] + g[1] * g[1]) + (g[2] * g[2] + g[3] * g[3])
    last = lane == LANES - 1
    state = jnp.sum(total * (1.0 / dim) + jnp.where(last, w[3], 0.0), axis=1, keepdims=True)
    scale = lr * lax.rsqrt(state + EPSILON)
    new = [w[c] - g[c] * scale for c in range(WORDS)]
    return [*new[:3], jnp.where(last, state, new[3])]


def sum_terms(src, dst, lo, hi, terms, acc):
    def body(k, carry):
        prev, total = carry
        at = dst[k]
        total = jnp.where(at == prev, total, 0.0) + terms[word(src[k]), :]
        acc[word(at), :] = total
        return at, total

    unrolled_loop(lo, hi, UNROLL, body, (jnp.int32(-1), jnp.zeros((WORDS, LANES), F32)))


def take_sums(acc, at):
    sums = [acc[i, :] for i in at]
    for i in at:
        acc[i, :] = jnp.zeros((SUB, LANES), F32)
    return sums


def update_words(ref, acc, dim, lr):
    lane = lax.broadcasted_iota(jnp.int32, (SUB, LANES), 1)
    for r0 in range(0, BLOCK, SUB):
        at = [pl.ds(r0 * WORDS + c, SUB, stride=WORDS) for c in range(WORDS)]
        w = apply_step([ref[i, :] for i in at], take_sums(acc, at), lane, dim, lr)
        for c in range(WORDS):
            ref[at[c], :] = w[c]


def update_columns(ref, acc, dst, state_out, dim, lr, first=0):
    half = dim // 2
    pad = half - LANES
    lane = lax.broadcasted_iota(jnp.int32, (SUB, LANES), 1)
    for r0 in range(0, BLOCK, SUB):
        at = [pl.ds(r0 * WORDS + c, SUB, stride=WORDS) for c in range(WORDS)]
        w = apply_step([ref[i, :] for i in at], take_sums(acc, at), lane, dim, lr)
        cols = slice(first + r0, first + r0 + SUB)
        dst[:LANES, cols] = w[0].T
        dst[LANES:half, cols] = w[1].T[:pad]
        dst[half:half + LANES, cols] = w[2].T
        w3 = w[3].T
        dst[half + LANES:, cols] = w3[:pad]
        if state_out is not None:
            state_out[:, cols] = w3[LANES - 1:]


def place_parts(rep, parts, dst, sems, first):
    size = parts[0].shape[0]
    side = len(parts) // 2
    copies = []
    for n, part in enumerate(parts):
        at = 0 if side == 0 else (rep * side + n if n < side else (1 - rep) * side + n - side) * size
        copies.append(pltpu.make_async_copy(part, dst.at[pl.ds(pl.multiple_of(at, 16) if side else 0, size)], sems.at[first + n]))
    return copies


def load_entity_terms(sizes, half, rep, gh, qb, gn, terms, queries, neg_terms, sems, then):
    heads, tails, negs = sizes
    pad = half - LANES
    head_copy = pltpu.make_async_copy(gh, terms.at[pl.ds(0, heads * WORDS)], sems.at[0])
    query_copies = place_parts(rep, qb, queries, sems, 1)
    neg_copies = place_parts(rep, gn, neg_terms, sems, 1 + len(qb))
    for c in (*query_copies, *neg_copies, head_copy):
        c.start()
    then()
    for c in query_copies:
        c.wait()

    def body(t, carry):
        q, last = get_packed(queries, t * packed_rows(TILE, QUERY_SLOT), TILE, pad, QUERY_SLOT)
        dp = dp_of(last, pad)
        for c in range(WORDS):
            terms[pl.ds((heads + t * TILE) * WORDS + c, TILE, stride=WORDS), :] = dp * q[c]
        return carry

    lax.fori_loop(0, tails // TILE, body, 0)
    for c in neg_copies:
        c.wait()
    for c, v in enumerate(get_packed(neg_terms, 0, negs, pad, ROW_SLOT)[0]):
        terms[pl.ds((heads + tails) * WORDS + c, negs, stride=WORDS), :] = v
    head_copy.wait()


def store_entity_rows(sizes, half, rows, xh, xt, sem):
    heads, tails, negs = sizes
    pad = half - LANES
    copy = pltpu.make_async_copy(rows.at[pl.ds(0, heads * WORDS)], xh, sem)
    copy.start()

    def move(r0, n, base):
        v = [rows[pl.ds((heads + r0) * WORDS + c, n, stride=WORDS), :] for c in range(WORDS)]
        put_packed(xt, base, v, pad, ROW_SLOT)

    def body(t, carry):
        move(t * TILE, TILE, t * packed_rows(TILE, ROW_SLOT))
        return carry

    lax.fori_loop(0, tails // TILE, body, 0)
    move(tails, negs, tails // TILE * packed_rows(TILE, ROW_SLOT))
    copy.wait()


def near_rows(tails, negs):
    return tails // TILE * packed_rows(TILE, ROW_SLOT) + packed_rows(negs, ROW_SLOT)


def fetch_rows(row, spot, count, table, rows, sem):
    def body(k, carry):
        pltpu.make_async_copy(table.at[word(row[k])], rows.at[word(spot(k))], sem).start()
        return carry

    unrolled_loop(0, count, UNROLL, body, 0)
    size = pl.multiple_of(count * WORDS, WORDS)
    pltpu.make_async_copy(table.at[pl.ds(0, size)], rows.at[pl.ds(0, size)], sem).wait()


def relation_fetch_kernel(row, count, table, xr, rows, sems):
    fetch_rows(row, lambda k: k * WORDS, count[0], table, rows, sems.at[0])
    copy = pltpu.make_async_copy(rows, xr, sems.at[1])
    copy.start()
    copy.wait()


def entity_kernel(cfg, *refs):
    sizes, dim, lr, final, n_qb, n_gn = cfg
    it = iter(refs)
    place, usrc, udst, uoff = next(it), next(it), next(it), next(it)
    xsrc, xdst, xoff = (None, None, None) if final else (next(it), next(it), next(it))
    table, gh = next(it), next(it)
    qb = [next(it) for _ in range(n_qb)]
    gn = [next(it) for _ in range(n_gn)]
    out = next(it)
    if final:
        state_out = next(it)
    else:
        xh, xt = next(it), next(it)
    terms, queries, neg_terms, acc, ring = next(it), next(it), next(it), next(it), next(it)
    rows = None if final else next(it)
    cols = next(it) if final else None
    sems, load_sems, store_sems = next(it), next(it), next(it)
    blocks = table.shape[0] // (BLOCK * WORDS)
    acc[...] = jnp.zeros_like(acc)
    load_entity_terms(sizes, dim // 2, place[0], gh, qb, gn, terms, queries, neg_terms, sems, lambda: start_sweep(table, ring, load_sems))

    def store(b):
        if final:
            slot = lax.rem(b, 2)
            at = pl.ds(pl.multiple_of(b * BLOCK, BLOCK), BLOCK)
            return pltpu.make_async_copy(cols.at[slot], out.at[:, at], store_sems.at[slot])
        slot = lax.rem(b, SLOTS)
        at = block_rows(b)
        return pltpu.make_async_copy(ring.at[block_rows(slot)], out.at[at], store_sems.at[slot])

    def body(b, ref):
        sum_terms(usrc, udst, uoff[b], uoff[b + 1], terms, acc)
        if final:
            update_columns(ref, acc, cols.at[lax.rem(b, 2)], state_out.at[b], dim, lr)
        else:
            update_words(ref, acc, dim, lr)
            copy_rows(xsrc, lambda k: xdst[k], xoff[b], xoff[b + 1], ref, rows)

    sweep(table, ring, load_sems, store, blocks, body)
    if not final:
        store_entity_rows(sizes, dim // 2, rows, xh, xt, sems.at[0])


def copy_rows(src, dst, lo, hi, ref, rows):
    def body(k, carry):
        rows[word(dst(k)), :] = ref[word(src[k]), :]
        return carry

    unrolled_loop(lo, hi, UNROLL, body, 0)


def relation_fetch(table, edges, row, count):
    return pl.pallas_call(
        relation_fetch_kernel,
        grid_spec=pltpu.PrefetchScalarGridSpec(
            num_scalar_prefetch=2, grid=(1,), in_specs=[ANY], out_specs=ANY,
            scratch_shapes=[pltpu.VMEM((edges * WORDS, LANES), F32), pltpu.SemaphoreType.DMA((2,))]),
        out_shape=jax.ShapeDtypeStruct((edges * WORDS, LANES), F32),
        compiler_params=params(),
        name="relation_fetch",
    )(row, count, table)


def entity_pass(table, sizes, dim, lr, place, upd, gh, qb, gn, ext=None):
    heads, tails, negs = sizes
    final = ext is None
    blocks = table.shape[0] // (BLOCK * WORDS)
    total = sum(sizes) * WORDS
    scalars = [place, *upd, *(() if final else ext)]
    parts = (gh, *qb, *gn)
    scratch = [
        pltpu.VMEM((total, LANES), F32),
        pltpu.VMEM((sum(p.shape[0] for p in qb), LANES), BF16),
        pltpu.VMEM((sum(p.shape[0] for p in gn), LANES), F32),
        pltpu.VMEM((BLOCK * WORDS, LANES), F32),
        pltpu.VMEM((SLOTS * BLOCK * WORDS, LANES), F32),
    ]
    if final:
        outs = [ANY, whole((blocks, 1, BLOCK))]
        shapes = [jax.ShapeDtypeStruct((dim, blocks * BLOCK), F32), jax.ShapeDtypeStruct((blocks, 1, BLOCK), F32)]
        scratch.append(pltpu.VMEM((2, dim, BLOCK), F32))
    else:
        outs = [ANY, ANY, whole((near_rows(tails, negs), LANES))]
        shapes = [jax.ShapeDtypeStruct(table.shape, F32), jax.ShapeDtypeStruct((heads * WORDS, LANES), F32),
                  jax.ShapeDtypeStruct((near_rows(tails, negs), LANES), BF16)]
        scratch.append(pltpu.VMEM((total, LANES), F32))
    scratch += [pltpu.SemaphoreType.DMA((len(parts),)), pltpu.SemaphoreType.DMA((SLOTS,)), pltpu.SemaphoreType.DMA((SLOTS,))]
    return pl.pallas_call(
        functools.partial(entity_kernel, (sizes, dim, lr, final, len(qb), len(gn))),
        grid_spec=pltpu.PrefetchScalarGridSpec(
            num_scalar_prefetch=len(scalars), grid=(1,), in_specs=[ANY] * (1 + len(parts)), out_specs=outs, scratch_shapes=scratch),
        out_shape=shapes,
        input_output_aliases={} if final else {len(scalars): 0},
        compiler_params=params(),
        name="entity_last" if final else "entity_pass",
    )(*scalars, table, *parts)


def load_relation_terms(part, pad, counts, parts, terms, sems):
    shared = parts[0]
    stage = 8 * part * WORDS
    size = part // TILE * packed_rows(TILE, ROW_SLOT)
    copies = []
    for j in range(8):
        copies.append(pltpu.make_async_copy(shared.at[pl.ds(j * size, size)], terms.at[pl.ds(stage + j * size, size)], sems.at[j]))
    more = pltpu.make_async_copy(parts[1], terms.at[pl.ds(8 * part * WORDS, parts[1].shape[0])], sems.at[8])
    for c in copies:
        c.start()
    for c in copies:
        c.wait()
    tiles = part // TILE

    def body(i, carry):
        slot = i // tiles
        t = lax.rem(i, tiles)

        @pl.when(slot // 4 * part + t * TILE < counts[lax.rem(slot, 4)])
        def _():
            v, _ = get_packed(terms, stage + slot * size + t * packed_rows(TILE, ROW_SLOT), TILE, pad, ROW_SLOT)
            for c in range(WORDS):
                terms[pl.ds((slot * part + t * TILE) * WORDS + c, TILE, stride=WORDS), :] = v[c]

        return carry

    lax.fori_loop(0, 8 * tiles, body, 0)

    @pl.when(counts[4] > 0)
    def _():
        more.start()
        more.wait()


def relation_kernel(cfg, *refs):
    dim, lr, part, n_parts = cfg
    usrc, udst, uoff, counts, xsrc, xoff, table = refs[:7]
    parts = refs[7:7 + n_parts]
    out, xr, terms, acc, ring, rows, sems, load_sems, store_sems = refs[7 + n_parts:]
    blocks = table.shape[0] // (BLOCK * WORDS)
    acc[...] = jnp.zeros_like(acc)
    start_sweep(table, ring, load_sems)
    load_relation_terms(part, dim // 2 - LANES, counts, parts, terms, sems)

    def store(b):
        slot = lax.rem(b, SLOTS)
        at = block_rows(b)
        return pltpu.make_async_copy(ring.at[block_rows(slot)], out.at[at], store_sems.at[slot])

    def body(b, ref):
        sum_terms(usrc, udst, uoff[b], uoff[b + 1], terms, acc)
        update_words(ref, acc, dim, lr)
        copy_rows(xsrc, lambda k: k * WORDS, xoff[b], xoff[b + 1], ref, rows)

    sweep(table, ring, load_sems, store, blocks, body)
    copy = pltpu.make_async_copy(rows, xr, sems.at[0])
    copy.start()
    copy.wait()


def relation_last_kernel(cfg, *refs):
    dim, lr, part, n_parts = cfg
    usrc, udst, uoff, counts, src = refs[:5]
    parts = refs[5:5 + n_parts]
    dst, terms, acc, sems = refs[5 + n_parts:]
    step = pl.program_id(0)

    @pl.when(step == 0)
    def _():
        acc[...] = jnp.zeros_like(acc)
        load_relation_terms(part, dim // 2 - LANES, counts, parts, terms, sems)

    group = src.shape[0] // (BLOCK * WORDS)
    for j in range(group):
        b = step * group + j
        sum_terms(usrc, udst, uoff[b], uoff[b + 1], terms, acc)
        update_columns(src.at[block_rows(j)], acc, dst, None, dim, lr, j * BLOCK)


def relation_pass(table, edges, part, dim, lr, upd, parts, ext):
    count = 8 * part * WORDS + sum(p.shape[0] for p in parts[1:])
    scalars = [*upd, *ext]
    return pl.pallas_call(
        functools.partial(relation_kernel, (dim, lr, part, len(parts))),
        grid_spec=pltpu.PrefetchScalarGridSpec(
            num_scalar_prefetch=len(scalars), grid=(1,), in_specs=[ANY] * (1 + len(parts)), out_specs=[ANY, ANY],
            scratch_shapes=[
                pltpu.VMEM((count, LANES), F32),
                pltpu.VMEM((BLOCK * WORDS, LANES), F32),
                pltpu.VMEM((SLOTS * BLOCK * WORDS, LANES), F32),
                pltpu.VMEM((4 * BLOCK * WORDS, LANES), F32),
                pltpu.SemaphoreType.DMA((9,)),
                pltpu.SemaphoreType.DMA((SLOTS,)),
                pltpu.SemaphoreType.DMA((SLOTS,)),
            ]),
        out_shape=[jax.ShapeDtypeStruct(table.shape, F32), jax.ShapeDtypeStruct((edges * WORDS, LANES), F32)],
        input_output_aliases={len(scalars): 0},
        compiler_params=params(),
        name="relation_pass",
    )(*scalars, table, *parts)


def relation_last(table, n_rel, part, dim, lr, upd, parts):
    blocks = table.shape[0] // (BLOCK * WORDS)
    group = 3 if blocks % 3 == 0 else 1
    count = 8 * part * WORDS + sum(p.shape[0] for p in parts[1:])
    return pl.pallas_call(
        functools.partial(relation_last_kernel, (dim, lr, part, len(parts))),
        grid_spec=pltpu.PrefetchScalarGridSpec(
            num_scalar_prefetch=len(upd), grid=(blocks // group,),
            in_specs=[pl.BlockSpec((BLOCK * group * WORDS, LANES), lambda b, *_: (b, 0))] + [ANY] * len(parts),
            out_specs=pl.BlockSpec((dim, BLOCK * group), lambda b, *_: (0, b)),
            scratch_shapes=[
                pltpu.VMEM((count, LANES), F32),
                pltpu.VMEM((BLOCK * WORDS, LANES), F32),
                pltpu.SemaphoreType.DMA((9,)),
            ]),
        out_shape=jax.ShapeDtypeStruct((dim, n_rel), F32),
        compiler_params=params(),
        name="relation_last",
    )(*upd, table, *parts)


def edge_rows(ref, keep, keep_data):
    v = [ref[pl.ds(c, TILE, stride=WORDS), :] for c in range(WORDS)]
    return [jnp.where(keep_data if c % 2 else keep, v[c], 0.0) for c in range(WORDS)]


def edge_masks(start, n, pad):
    row = lax.broadcasted_iota(jnp.int32, (TILE, LANES), 0) + start
    lane = lax.broadcasted_iota(jnp.int32, (TILE, LANES), 1)
    keep = row < n
    return lane, keep, keep & (lane < pad)


def fetch_negatives(near, neg_in, nb, pad, sem):
    copy = pltpu.make_async_copy(near.at[pl.ds(near.shape[0] - neg_in.shape[0], neg_in.shape[0])], neg_in, sem)
    copy.start()
    copy.wait()
    for c, v in enumerate(get_packed(neg_in, 0, nb.shape[0], pad, ROW_SLOT)[0]):
        nb[:, LANES * c:LANES * (c + 1)] = v.astype(BF16)


def score_kernel(half, info, xh, xr, tb, near, qb_out, ds_out, gn, loss, neg_in, nb, gacc, sem):
    step = pl.program_id(0)
    pad = half - LANES
    n = info[0]
    start = step * TILE

    @pl.when(step == 0)
    def _():
        gacc[...] = jnp.zeros_like(gacc)
        loss[0, 0] = 0.0
        fetch_negatives(near, neg_in, nb, pad, sem)

    @pl.when(start < n)
    def _():
        lane, keep, keep_data = edge_masks(start, n, pad)
        h = edge_rows(xh, keep, keep_data)
        r = edge_rows(xr, keep, keep_data)
        q = [h[0] * r[0] - h[2] * r[2], h[1] * r[1] - h[3] * r[3], h[0] * r[2] + h[2] * r[0], h[1] * r[3] + h[3] * r[1]]
        qc = [v.astype(BF16) for v in q]
        query = jnp.concatenate(qc, axis=1)
        wide = [v.astype(F32) for v in qc]
        tail = [jnp.where(keep, v, 0.0) for v in get_packed(tb, 0, TILE, pad, ROW_SLOT)[0]]
        prod = [wide[c] * tail[c] for c in range(WORDS)]
        pos = jnp.sum((prod[0] + prod[1]) + (prod[2] + prod[3]), axis=1, keepdims=True)
        score = lax.dot_general(query, nb[...], (((1,), (1,)), ((), ())), preferred_element_type=F32)
        top = jnp.maximum(jnp.max(score, axis=1, keepdims=True), pos)
        pos_exp = jnp.exp(pos - top)
        neg_exp = jnp.exp(score - top)
        total = pos_exp + jnp.sum(neg_exp, axis=1, keepdims=True)
        weight = jnp.where(keep[:, :1], 1.0, 0.0)
        loss[0, 0] += jnp.sum(weight * ((top + jnp.log(total)) - pos))
        inverse = 1.0 / total
        dp = weight * (pos_exp * inverse - 1.0)
        ds = ((weight * inverse) * neg_exp).astype(BF16)
        ds_out[...] = ds
        gacc[...] += lax.dot_general(ds, query, (((0,), (0,)), ((), ())), preferred_element_type=F32)
        hi = dp.astype(BF16).astype(F32)
        mid = (dp - hi).astype(BF16).astype(F32)
        low = (dp - hi) - mid
        q3 = jnp.where(lane == pad, hi, jnp.where(lane == pad + 1, mid, jnp.where(lane == pad + 2, low, wide[3])))
        put_packed(qb_out, 0, [*wide[:3], q3], pad, QUERY_SLOT)

    @pl.when(step == pl.num_programs(0) - 1)
    def _():
        put_packed(gn, 0, [gacc[:, LANES * c:LANES * (c + 1)] for c in range(WORDS)], pad, ROW_SLOT)


def dp_of(last, pad):
    return (last[:, pad:pad + 1] + last[:, pad + 1:pad + 2]) + last[:, pad + 2:pad + 3]


def gradient_kernel(cfg, spot, info, xh, xr, tb, near, qb, ds, gh, ua, ub, neg_in, nb, gr, uniq, held, sem):
    cap, edges, half = cfg
    step = pl.program_id(0)
    pad = half - LANES
    n = info[0]
    start = step * TILE

    @pl.when(step == 0)
    def _():
        fetch_negatives(near, neg_in, nb, pad, sem)

    @pl.when(start < n)
    def _():
        _, keep, keep_data = edge_masks(start, n, pad)
        h = edge_rows(xh, keep, keep_data)
        r = edge_rows(xr, keep, keep_data)
        tail = [jnp.where(keep, v, 0.0) for v in get_packed(tb, 0, TILE, pad, ROW_SLOT)[0]]
        dp = dp_of(get_packed(qb, 0, TILE, pad, QUERY_SLOT)[1], pad)
        gq = lax.dot_general(ds[...], nb[...], (((1,), (0,)), ((), ())), preferred_element_type=F32)
        g = [dp * tail[c] + gq[:, LANES * c:LANES * (c + 1)] for c in range(WORDS)]
        out = [g[0] * r[0] + g[2] * r[2], g[1] * r[1] + g[3] * r[3], g[2] * r[0] - g[0] * r[2], g[3] * r[1] - g[1] * r[3]]
        rel_g = [g[0] * h[0] + g[2] * h[2], g[1] * h[1] + g[3] * h[3], g[2] * h[0] - g[0] * h[2], g[3] * h[1] - g[1] * h[3]]
        for c in range(WORDS):
            gh[pl.ds(c, TILE, stride=WORDS), :] = out[c]
            gr[pl.ds(c, TILE, stride=WORDS), :] = rel_g[c]

        def body(k, carry):
            prev, acc = carry
            at = spot[k]
            acc = jnp.where(at == prev, acc, 0.0) + gr[words_of(k - start), :]
            uniq[word(at), :] = acc
            return at, acc

        prev = jnp.where(step > 0, spot[jnp.maximum(start - 1, 0)], -1)
        _, acc = unrolled_loop(start, jnp.minimum(start + TILE, n), UNROLL, body, (prev, held[:WORDS, :]))
        held[:WORDS, :] = acc

    @pl.when(step == pl.num_programs(0) - 1)
    def _():
        more = pltpu.make_async_copy(uniq.at[pl.ds(cap * WORDS, (edges - cap) * WORDS)], ub, sem)
        more.start()
        part = cap // 2

        def body(t, carry):
            r0 = info[1] * part + t * TILE
            v = [uniq[pl.ds(r0 * WORDS + c, TILE, stride=WORDS), :] for c in range(WORDS)]
            put_packed(ua, t * packed_rows(TILE, ROW_SLOT), v, pad, ROW_SLOT)
            return carry

        lax.fori_loop(0, part // TILE, body, 0)
        more.wait()


def bucket_specs(negs):
    word_spec = pl.BlockSpec((TILE * WORDS, LANES), lambda t, *_: (t, 0))
    tail_spec = pl.BlockSpec((packed_rows(TILE, ROW_SLOT), LANES), lambda t, *_: (t, 0))
    query_spec = pl.BlockSpec((packed_rows(TILE, QUERY_SLOT), LANES), lambda t, *_: (t, 0))
    return word_spec, tail_spec, query_spec, pl.BlockSpec((TILE, negs), lambda t, *_: (t, 0))


def scores(info, xh, xr, near, edges, negs, half):
    word_spec, tail_spec, query_spec, prob_spec = bucket_specs(negs)
    neg_rows = packed_rows(negs, ROW_SLOT)
    return pl.pallas_call(
        functools.partial(score_kernel, half),
        grid_spec=pltpu.PrefetchScalarGridSpec(
            num_scalar_prefetch=1,
            grid=(edges // TILE,),
            in_specs=[word_spec, word_spec, tail_spec, ANY],
            out_specs=[query_spec, prob_spec, whole((neg_rows, LANES)),
                       pl.BlockSpec((1, 1), lambda *_: (0, 0), memory_space=pltpu.SMEM)],
            scratch_shapes=[
                pltpu.VMEM((neg_rows, LANES), BF16),
                pltpu.VMEM((negs, WIDE), BF16),
                pltpu.VMEM((negs, WIDE), F32),
                pltpu.SemaphoreType.DMA(()),
            ]),
        out_shape=[
            jax.ShapeDtypeStruct((edges // TILE * packed_rows(TILE, QUERY_SLOT), LANES), BF16),
            jax.ShapeDtypeStruct((edges, negs), BF16),
            jax.ShapeDtypeStruct((neg_rows, LANES), F32),
            jax.ShapeDtypeStruct((1, 1), F32),
        ],
        compiler_params=params(),
        name="scores",
    )(info, xh, xr, near, near)


def gradients(spot, info, xh, xr, near, qb, ds, negs, cap, half):
    edges = spot.shape[0]
    word_spec, tail_spec, query_spec, prob_spec = bucket_specs(negs)
    shared_rows = cap // 2 // TILE * packed_rows(TILE, ROW_SLOT)
    return pl.pallas_call(
        functools.partial(gradient_kernel, (cap, edges, half)),
        grid_spec=pltpu.PrefetchScalarGridSpec(
            num_scalar_prefetch=2,
            grid=(edges // TILE,),
            in_specs=[word_spec, word_spec, tail_spec, ANY, query_spec, prob_spec],
            out_specs=[word_spec, whole((shared_rows, LANES)), ANY],
            scratch_shapes=[
                pltpu.VMEM((packed_rows(negs, ROW_SLOT), LANES), BF16),
                pltpu.VMEM((negs, WIDE), BF16),
                pltpu.VMEM((TILE * WORDS, LANES), F32),
                pltpu.VMEM((edges * WORDS, LANES), F32),
                pltpu.VMEM((8, LANES), F32),
                pltpu.SemaphoreType.DMA(()),
            ]),
        out_shape=[
            jax.ShapeDtypeStruct((edges * WORDS, LANES), F32),
            jax.ShapeDtypeStruct((shared_rows, LANES), F32),
            jax.ShapeDtypeStruct(((edges - cap) * WORDS, LANES), F32),
        ],
        compiler_params=params(),
        name="gradients",
    )(spot, info, xh, xr, near, near, qb, ds)


def running_count(flags):
    lead = flags.shape[:-1]
    n = flags.shape[-1] // LANES
    x = flags.reshape(*lead, n, LANES).astype(F32)
    tri = jnp.triu(jnp.ones((LANES, LANES), F32))
    inner = jnp.einsum('...k,kl->...l', x, tri, precision=lax.Precision.HIGHEST)
    before = jnp.einsum('...k,kl->...l', inner[..., -1], jnp.triu(jnp.ones((n, n), F32), 1), precision=lax.Precision.HIGHEST)
    return (inner + before[..., None]).astype(jnp.int32).reshape(flags.shape)


def blank(shape, dtype):
    return pl.pallas_call(lambda out: None, out_shape=jax.ShapeDtypeStruct(shape, dtype), out_specs=ANY, name="blank")()


def halves(x, rep, count):
    size = x.shape[0] // 2 // count
    return [lax.dynamic_slice_in_dim(x, (rep * count + j) * size, size) for j in range(count)]


def offsets(keys, bounds):
    return jnp.sum(keys[:, None, :] < bounds[None, :, None], axis=2, dtype=jnp.int32)


def solution(mesh):
    groups = mesh.shape['ent']
    data_reps = mesh.shape['data']
    row_spec = P(('sweep', 'ent'), None)
    edge_spec = P(('sweep', 'ent'), None, 'data')

    def device_fn(ent_table, ent_state, rel_table, head_idx, tail_idx, rel_idx, edge_mask, neg_idx):
        part_rows, dim = ent_table.shape
        half = dim // 2
        n_rel = rel_table.shape[0]
        rounds = head_idx.shape[1]
        edges = head_idx.shape[2] * data_reps
        negs = neg_idx.shape[2]
        sizes = (edges, edges, negs)
        cap = edges // 2
        lr = LR_SCALE * dim ** -0.25
        me = lax.axis_index('ent')
        rep = lax.axis_index('data')

        rel_words = relation_words(rel_table.T)

        big = (NO_KEY >> 13) - 1
        order = jnp.where(edge_mask[0] > 0, rel_idx[0], big)
        packed = head_idx[0] * part_rows + tail_idx[0]
        both = lax.all_gather(jnp.stack([order, packed]), 'data', axis=2, tiled=True)
        spot = jnp.arange(edges, dtype=jnp.int32)
        order, packed = lax.sort((both[0] * edges + spot, both[1]), dimension=1, num_keys=1)
        rel_s = order // edges
        head_s = packed // part_rows
        tail_s = packed % part_rows
        live = rel_s < n_rel
        kept = jnp.sum(live, axis=1, dtype=jnp.int32)
        info = jnp.concatenate([jnp.where(live, rel_s, n_rel), jnp.where(live, tail_s, part_rows), neg_idx[0]], axis=1)
        every = lax.all_gather(info, 'ent', axis=0)
        every, fetch_from = lax.optimization_barrier((every, rel_words))
        xr = relation_fetch(fetch_from, edges, rel_s[0] * WORDS, kept[:1])

        far = jnp.stack([lax.dynamic_index_in_dim(every, (me - s) % groups, 0, False)[s, edges:] for s in range(rounds)])
        ids = jnp.concatenate([jnp.where(live, head_s, part_rows), far], axis=1)
        keys = jnp.where(ids < part_rows, (ids << SHIFT) + jnp.arange(sum(sizes), dtype=jnp.int32), NO_KEY)
        ent_key = lax.sort(keys, dimension=1, is_stable=False)
        ent_off = offsets(ent_key, jnp.arange(part_rows // BLOCK + 1, dtype=jnp.int32) * (BLOCK << SHIFT))
        ent_src = (ent_key & POS_MASK) * WORDS
        ent_dst = ((ent_key >> SHIFT) % BLOCK) * WORDS

        rels = every[:, :, :edges]
        prev = jnp.concatenate([jnp.full((groups, rounds, 1), -1, jnp.int32), rels[:, :, :-1]], axis=2)
        fresh = (rels != prev) & (rels < n_rel)
        slot = running_count(fresh) - 1
        over = jnp.max(slot[:, :, -1], axis=0) >= cap
        counts = jnp.concatenate([slot[:, :, -1] + 1, jnp.max(slot[:, :, -1] // cap, axis=0)[None]], axis=0).T
        own_spot = lax.dynamic_index_in_dim(slot, me, 0, False) * WORDS
        source = jnp.arange(groups, dtype=jnp.int32)[:, None, None]
        part = cap // data_reps
        first = (slot // part * groups + source) * part + slot % part
        slot = jnp.where(slot < cap, first, groups * cap + source * (edges - cap) + slot - cap)
        keys = jnp.where(fresh, (rels << SHIFT) + slot, NO_KEY).transpose(1, 0, 2).reshape(rounds, groups * edges)
        keys, ent_key = lax.optimization_barrier((keys, ent_key))
        rel_key = lax.sort(keys, dimension=1, is_stable=False)
        rel_key, own_spot = lax.optimization_barrier((rel_key, own_spot))
        bounds = jnp.arange(pl.cdiv(n_rel, BLOCK) + 1, dtype=jnp.int32) * BLOCK
        rel_off = offsets(rel_key, bounds << SHIFT)
        rel_src = (rel_key & POS_MASK) * WORDS
        rel_dst = ((rel_key >> SHIFT) % BLOCK) * WORDS
        own_off = offsets(jnp.where(live, rel_s, NO_KEY), bounds)
        own_src = (rel_s % BLOCK) * WORDS
        info = jnp.stack([kept, jnp.full((rounds,), rep, jnp.int32)], axis=1)

        ent_args = (sizes, dim, lr)
        rel_args = (part, dim, lr)
        ent_words, xh, xt = entity_first(ent_table.T, ent_state, sizes, (ent_dst[0], ent_src[0], ent_off[0]))
        place = rep[None].astype(jnp.int32)
        swap = [(i, 1 - i) for i in range(data_reps)]
        losses = []
        for s in range(rounds):
            tn = xt if s == 0 else lax.ppermute(xt, 'ent', [(i, (i - s) % groups) for i in range(groups)])
            own_qb, ds, gn, loss = scores(info[s], xh, xr, tn, edges, negs, half)
            losses.append(loss[0, 0] / edges)
            qb, gn = (own_qb,), (gn,)
            back = [(i, (i + s) % groups) for i in range(groups)]
            trade = s == groups // 2
            if trade:
                pieces = [lax.ppermute(v, 'ent', back) for v in (*halves(own_qb, rep, 2), *halves(gn[0], rep, 1))]
                pieces[0], own_qb = lax.optimization_barrier((pieces[0], own_qb))
            gh, ua, ub = gradients(own_spot[s], info[s], xh, xr, tn, own_qb, ds, negs, cap, half)
            if s > 0:
                if trade:
                    traded = [lax.ppermute(pieces[0], 'data', swap)]
                    for v in pieces[1:]:
                        v, gh = lax.optimization_barrier((v, gh))
                        traded.append(lax.ppermute(v, 'data', swap))
                    qb = (*pieces[:2], *traded[:2])
                    gn = (pieces[2], traded[2])
                else:
                    qb = (lax.ppermute(qb[0], 'ent', back),)
                    gn = (lax.ppermute(gn[0], 'ent', back),)
                qb, gn, ua = lax.optimization_barrier((qb, gn, ua))
            shared = lax.all_gather(ua, ('data', 'ent'), axis=0, tiled=True)

            final = s == rounds - 1
            ent_upd = (ent_src[s], ent_dst[s], ent_off[s])
            rel_upd = (rel_src[s], rel_dst[s], rel_off[s], counts[s])

            def relations(table, *parts, s=s, final=final, rel_upd=rel_upd):
                if final:
                    return (relation_last(table, n_rel, *rel_args, rel_upd, parts),)
                return relation_pass(table, edges, *rel_args, rel_upd, parts, (own_src[s + 1], own_off[s + 1]))

            def overflow(ub):
                return lax.all_gather(ub, 'ent', axis=0, tiled=True)

            def nothing(ub):
                return blank((groups * ub.shape[0], LANES), F32)

            more = lax.cond(over[s], overflow, nothing, ub)
            if final:
                ent_cols, state = entity_pass(ent_words, *ent_args, place, ent_upd, gh, qb, gn)
                (rel_cols,) = relations(rel_words, shared, more)
            else:
                ent_words, xh, xt = entity_pass(ent_words, *ent_args, place, ent_upd, gh, qb, gn, (ent_dst[s + 1], ent_src[s + 1], ent_off[s + 1]))
                rel_words, xr = relations(rel_words, shared, more)
        return ent_cols.T, state.reshape(part_rows), rel_cols.T, jnp.stack(losses)[None, :]

    return jax.shard_map(device_fn, mesh=mesh, in_specs=(row_spec, P(('sweep', 'ent')), P('sweep', None), edge_spec, edge_spec, edge_spec, edge_spec, P(('sweep', 'ent'), None, None)), out_specs=(row_spec, P(('sweep', 'ent')), P('sweep', None), row_spec), check_vma=False)
```

```python
import functools

import jax
import jax.numpy as jnp
from jax import lax
from jax.experimental import pallas as pl
from jax.experimental.pallas import tpu as pltpu
from jax.sharding import PartitionSpec as P

LR_SCALE = 0.2
EPSILON = 1e-8

LANES = 128
WORDS = 4
SHIFT = 14
POS_MASK = (1 << SHIFT) - 1
NO_KEY = 2**31 - 1
BLOCK = 1024
SUB = 128
SLOTS = 4
FIRST = 2
UNROLL = (16, 4)
ROW_SLOT = 16
QUERY_SLOT = 32
WIDE = WORDS * LANES
TILE = 512
CHUNK = 256
VMEM_LIMIT = 63 * 2**20
F32 = jnp.float32
BF16 = jnp.bfloat16
ANY = pl.BlockSpec(memory_space=pl.ANY)


def words_of(start):
    return pl.ds(pl.multiple_of(start * WORDS, WORDS), WORDS)


def word(start):
    return pl.ds(pl.multiple_of(start, WORDS), WORDS)


def block_rows(slot):
    return pl.ds(pl.multiple_of(slot * BLOCK * WORDS, BLOCK * WORDS), BLOCK * WORDS)


def unrolled_loop(lo, hi, unroll, body, carry):
    for width in (*unroll, 1):
        full = (hi - lo) // width

        def several(t, c, lo=lo, width=width):
            for j in range(width):
                c = body(lo + t * width + j, c)
            return c

        carry = lax.fori_loop(0, full, several, carry)
        lo = lo + full * width
    return carry


def packed_rows(n, slot):
    return 3 * n + n * slot // LANES


def pack(v, pad, slot):
    n = v[0].shape[0]
    gap = LANES - pad
    lane = lax.broadcasted_iota(jnp.int32, (n, LANES), 1)
    mixed = jnp.where(lane < pad, v[1], pltpu.roll(v[3], pad, 1))
    groups = LANES // slot
    size = n // groups
    thin = lane[:size]
    rest = jnp.zeros((size, LANES), F32)
    for a in range(groups):
        moved = pltpu.roll(v[3][a * size:(a + 1) * size], (slot * a - gap) % LANES, 1)
        rest = jnp.where((thin >= slot * a) & (thin < slot * (a + 1)), moved, rest)
    return v[0], v[2], mixed, rest


def unpack(first, third, mixed, rest, pad, slot):
    n = first.shape[0]
    gap = LANES - pad
    lane = lax.broadcasted_iota(jnp.int32, (n, LANES), 1)
    tail = jnp.concatenate([pltpu.roll(rest, (gap - slot * a) % LANES, 1) for a in range(LANES // slot)], axis=0)
    last = jnp.where(lane < gap, pltpu.roll(mixed, LANES - pad, 1), tail)
    return [first, jnp.where(lane < pad, mixed, 0.0), third, jnp.where(lane < pad, last, 0.0)], last


def put_packed(ref, base, v, pad, slot):
    n = v[0].shape[0]
    for c, part in enumerate(pack(v, pad, slot)):
        ref[pl.ds(pl.multiple_of(base + c * n, 16), part.shape[0]), :] = part.astype(ref.dtype)


def get_packed(ref, base, n, pad, slot):
    at = [pl.ds(pl.multiple_of(base + c * n, 16), n if c < 3 else n * slot // LANES) for c in range(4)]
    return unpack(*[ref[i, :].astype(F32) for i in at], pad, slot)


def params(**kw):
    return pltpu.CompilerParams(dimension_semantics=("arbitrary",), vmem_limit_bytes=VMEM_LIMIT, **kw)


def whole(shape):
    return pl.BlockSpec(shape, lambda *_: (0,) * len(shape), pipeline_mode=pl.Buffered(1))


def convert_block(src, state, dst, half, first=0):
    pad = half - LANES
    sub8 = lax.broadcasted_iota(jnp.int32, (8, LANES), 0)
    for r0 in range(0, BLOCK, SUB):
        cols = slice(first + r0, first + r0 + SUB)
        if state is not None:
            low = jnp.where(sub8 == 7, jnp.broadcast_to(state[:, cols], (8, LANES)), 0.0)
        else:
            low = jnp.zeros((8, LANES), F32)
        gap = jnp.zeros((LANES - pad - 8, LANES), F32)
        none = jnp.zeros((8, LANES), F32)
        w = [
            src[:LANES, cols],
            jnp.concatenate([src[LANES:half, cols], gap, none], axis=0),
            src[half:half + LANES, cols],
            jnp.concatenate([src[half + LANES:, cols], gap, low], axis=0),
        ]
        for c in range(WORDS):
            dst[pl.ds(r0 * WORDS + c, SUB, stride=WORDS), :] = w[c].T


def relation_words_kernel(half, src, dst):
    for j in range(dst.shape[0] // (BLOCK * WORDS)):
        convert_block(src, None, dst.at[block_rows(j)], half, j * BLOCK)


def entity_first_kernel(sizes, half, xsrc, xdst, xoff, src, state, dst, xh, xt, rows, sems):
    step = pl.program_id(0)
    for j in range(FIRST):
        part = dst.at[block_rows(j)]
        convert_block(src, state, part, half, j * BLOCK)
        b = step * FIRST + j
        copy_rows(xsrc, lambda k: xdst[k], xoff[b], xoff[b + 1], part, rows)

    @pl.when(step == pl.num_programs(0) - 1)
    def _():
        store_entity_rows(sizes, half, rows, xh, xt, sems.at[0])


def relation_words(table_t):
    dim, rows = table_t.shape
    blocks = pl.cdiv(rows, BLOCK)
    group = 3 if blocks % 3 == 0 else 1
    return pl.pallas_call(
        functools.partial(relation_words_kernel, dim // 2),
        grid=(blocks // group,),
        in_specs=[pl.BlockSpec((dim, BLOCK * group), lambda b: (0, b))],
        out_specs=pl.BlockSpec((BLOCK * group * WORDS, LANES), lambda b: (b, 0)),
        out_shape=jax.ShapeDtypeStruct((blocks * BLOCK * WORDS, LANES), F32),
        compiler_params=params(),
        name="relation_words",
    )(table_t)


def entity_first(table_t, state, sizes, ext):
    dim, rows = table_t.shape
    heads, tails, negs = sizes
    steps = rows // (BLOCK * FIRST)
    near = near_rows(tails, negs)
    return pl.pallas_call(
        functools.partial(entity_first_kernel, sizes, dim // 2),
        grid_spec=pltpu.PrefetchScalarGridSpec(
            num_scalar_prefetch=3, grid=(steps,),
            in_specs=[pl.BlockSpec((dim, BLOCK * FIRST), lambda b, *_: (0, b)),
                      pl.BlockSpec((None, 1, BLOCK * FIRST), lambda b, *_: (b, 0, 0))],
            out_specs=[pl.BlockSpec((BLOCK * FIRST * WORDS, LANES), lambda b, *_: (b, 0)), ANY, whole((near, LANES))],
            scratch_shapes=[pltpu.VMEM((sum(sizes) * WORDS, LANES), F32), pltpu.SemaphoreType.DMA((1,))]),
        out_shape=[jax.ShapeDtypeStruct((rows * WORDS, LANES), F32), jax.ShapeDtypeStruct((heads * WORDS, LANES), F32),
                   jax.ShapeDtypeStruct((near, LANES), BF16)],
        compiler_params=params(),
        name="entity_first",
    )(*ext, table_t, state.reshape(steps, 1, BLOCK * FIRST))


def block_load(table, ring, load_sems, b):
    slot = lax.rem(b, SLOTS)
    return pltpu.make_async_copy(table.at[block_rows(b)], ring.at[block_rows(slot)], load_sems.at[slot])


def start_sweep(table, ring, load_sems):
    for b in range(2):
        block_load(table, ring, load_sems, b).start()


def sweep(table, ring, load_sems, store, blocks, body):
    load = functools.partial(block_load, table, ring, load_sems)

    def turn(b, carry):
        load(b).wait()

        @pl.when(b >= 2)
        def _():
            store(b - 2).wait()

        @pl.when(b + 2 < blocks)
        def _():
            load(b + 2).start()

        body(b, ring.at[block_rows(lax.rem(b, SLOTS))])
        store(b).start()
        return carry

    lax.fori_loop(0, blocks, turn, 0)
    store(blocks - 2).wait()
    store(blocks - 1).wait()


def apply_step(w, g, lane, dim, lr):
    total = (g[0] * g[0] + g[1] * g[1]) + (g[2] * g[2] + g[3] * g[3])
    last = lane == LANES - 1
    state = jnp.sum(total * (1.0 / dim) + jnp.where(last, w[3], 0.0), axis=1, keepdims=True)
    scale = lr * lax.rsqrt(state + EPSILON)
    new = [w[c] - g[c] * scale for c in range(WORDS)]
    return [*new[:3], jnp.where(last, state, new[3])]


def sum_terms(src, dst, lo, hi, terms, acc):
    def body(k, carry):
        prev, total = carry
        at = dst[k]
        total = jnp.where(at == prev, total, 0.0) + terms[word(src[k]), :]
        acc[word(at), :] = total
        return at, total

    unrolled_loop(lo, hi, UNROLL, body, (jnp.int32(-1), jnp.zeros((WORDS, LANES), F32)))


def take_sums(acc, at):
    sums = [acc[i, :] for i in at]
    for i in at:
        acc[i, :] = jnp.zeros((SUB, LANES), F32)
    return sums


def update_words(ref, acc, dim, lr):
    lane = lax.broadcasted_iota(jnp.int32, (SUB, LANES), 1)
    for r0 in range(0, BLOCK, SUB):
        at = [pl.ds(r0 * WORDS + c, SUB, stride=WORDS) for c in range(WORDS)]
        w = apply_step([ref[i, :] for i in at], take_sums(acc, at), lane, dim, lr)
        for c in range(WORDS):
            ref[at[c], :] = w[c]


def update_columns(ref, acc, dst, state_out, dim, lr, first=0):
    half = dim // 2
    pad = half - LANES
    lane = lax.broadcasted_iota(jnp.int32, (SUB, LANES), 1)
    for r0 in range(0, BLOCK, SUB):
        at = [pl.ds(r0 * WORDS + c, SUB, stride=WORDS) for c in range(WORDS)]
        w = apply_step([ref[i, :] for i in at], take_sums(acc, at), lane, dim, lr)
        cols = slice(first + r0, first + r0 + SUB)
        dst[:LANES, cols] = w[0].T
        dst[LANES:half, cols] = w[1].T[:pad]
        dst[half:half + LANES, cols] = w[2].T
        w3 = w[3].T
        dst[half + LANES:, cols] = w3[:pad]
        if state_out is not None:
            state_out[:, cols] = w3[LANES - 1:]


def place_parts(rep, parts, dst, sems, first):
    size = parts[0].shape[0]
    side = len(parts) // 2
    copies = []
    for n, part in enumerate(parts):
        at = 0 if side == 0 else (rep * side + n if n < side else (1 - rep) * side + n - side) * size
        copies.append(pltpu.make_async_copy(part, dst.at[pl.ds(pl.multiple_of(at, 16) if side else 0, size)], sems.at[first + n]))
    return copies


def load_entity_terms(sizes, half, rep, gh, qb, gn, terms, queries, neg_terms, sems, then):
    heads, tails, negs = sizes
    pad = half - LANES
    head_copy = pltpu.make_async_copy(gh, terms.at[pl.ds(0, heads * WORDS)], sems.at[0])
    query_copies = place_parts(rep, qb, queries, sems, 1)
    neg_copies = place_parts(rep, gn, neg_terms, sems, 1 + len(qb))
    for c in (*query_copies, *neg_copies, head_copy):
        c.start()
    then()
    for c in query_copies:
        c.wait()

    def body(t, carry):
        q, last = get_packed(queries, t * packed_rows(TILE, QUERY_SLOT), TILE, pad, QUERY_SLOT)
        dp = dp_of(last, pad)
        for c in range(WORDS):
            terms[pl.ds((heads + t * TILE) * WORDS + c, TILE, stride=WORDS), :] = dp * q[c]
        return carry

    lax.fori_loop(0, tails // TILE, body, 0)
    for c in neg_copies:
        c.wait()
    for c, v in enumerate(get_packed(neg_terms, 0, negs, pad, ROW_SLOT)[0]):
        terms[pl.ds((heads + tails) * WORDS + c, negs, stride=WORDS), :] = v
    head_copy.wait()


def store_entity_rows(sizes, half, rows, xh, xt, sem):
    heads, tails, negs = sizes
    pad = half - LANES
    copy = pltpu.make_async_copy(rows.at[pl.ds(0, heads * WORDS)], xh, sem)
    copy.start()

    def move(r0, n, base):
        v = [rows[pl.ds((heads + r0) * WORDS + c, n, stride=WORDS), :] for c in range(WORDS)]
        put_packed(xt, base, v, pad, ROW_SLOT)

    def body(t, carry):
        move(t * TILE, TILE, t * packed_rows(TILE, ROW_SLOT))
        return carry

    lax.fori_loop(0, tails // TILE, body, 0)
    move(tails, negs, tails // TILE * packed_rows(TILE, ROW_SLOT))
    copy.wait()


def near_rows(tails, negs):
    return tails // TILE * packed_rows(TILE, ROW_SLOT) + packed_rows(negs, ROW_SLOT)


def fetch_rows(row, spot, count, table, rows, sem):
    def body(k, carry):
        pltpu.make_async_copy(table.at[word(row[k])], rows.at[word(spot(k))], sem).start()
        return carry

    unrolled_loop(0, count, UNROLL, body, 0)
    size = pl.multiple_of(count * WORDS, WORDS)
    pltpu.make_async_copy(table.at[pl.ds(0, size)], rows.at[pl.ds(0, size)], sem).wait()


def relation_fetch_kernel(row, count, table, xr, rows, sems):
    fetch_rows(row, lambda k: k * WORDS, count[0], table, rows, sems.at[0])
    copy = pltpu.make_async_copy(rows, xr, sems.at[1])
    copy.start()
    copy.wait()


def entity_kernel(cfg, *refs):
    sizes, dim, lr, final, n_qb, n_gn = cfg
    it = iter(refs)
    place, usrc, udst, uoff = next(it), next(it), next(it), next(it)
    xsrc, xdst, xoff = (None, None, None) if final else (next(it), next(it), next(it))
    table, gh = next(it), next(it)
    qb = [next(it) for _ in range(n_qb)]
    gn = [next(it) for _ in range(n_gn)]
    out = next(it)
    if final:
        state_out = next(it)
    else:
        xh, xt = next(it), next(it)
    terms, queries, neg_terms, acc, ring = next(it), next(it), next(it), next(it), next(it)
    rows = None if final else next(it)
    cols = next(it) if final else None
    sems, load_sems, store_sems = next(it), next(it), next(it)
    blocks = table.shape[0] // (BLOCK * WORDS)
    acc[...] = jnp.zeros_like(acc)
    load_entity_terms(sizes, dim // 2, place[0], gh, qb, gn, terms, queries, neg_terms, sems, lambda: start_sweep(table, ring, load_sems))

    def store(b):
        if final:
            slot = lax.rem(b, 2)
            at = pl.ds(pl.multiple_of(b * BLOCK, BLOCK), BLOCK)
            return pltpu.make_async_copy(cols.at[slot], out.at[:, at], store_sems.at[slot])
        slot = lax.rem(b, SLOTS)
        at = block_rows(b)
        return pltpu.make_async_copy(ring.at[block_rows(slot)], out.at[at], store_sems.at[slot])

    def body(b, ref):
        sum_terms(usrc, udst, uoff[b], uoff[b + 1], terms, acc)
        if final:
            update_columns(ref, acc, cols.at[lax.rem(b, 2)], state_out.at[b], dim, lr)
        else:
            update_words(ref, acc, dim, lr)
            copy_rows(xsrc, lambda k: xdst[k], xoff[b], xoff[b + 1], ref, rows)

    sweep(table, ring, load_sems, store, blocks, body)
    if not final:
        store_entity_rows(sizes, dim // 2, rows, xh, xt, sems.at[0])


def copy_rows(src, dst, lo, hi, ref, rows):
    def body(k, carry):
        rows[word(dst(k)), :] = ref[word(src[k]), :]
        return carry

    unrolled_loop(lo, hi, UNROLL, body, 0)


def relation_fetch(table, edges, row, count):
    return pl.pallas_call(
        relation_fetch_kernel,
        grid_spec=pltpu.PrefetchScalarGridSpec(
            num_scalar_prefetch=2, grid=(1,), in_specs=[ANY], out_specs=ANY,
            scratch_shapes=[pltpu.VMEM((edges * WORDS, LANES), F32), pltpu.SemaphoreType.DMA((2,))]),
        out_shape=jax.ShapeDtypeStruct((edges * WORDS, LANES), F32),
        compiler_params=params(),
        name="relation_fetch",
    )(row, count, table)


def entity_pass(table, sizes, dim, lr, place, upd, gh, qb, gn, ext=None):
    heads, tails, negs = sizes
    final = ext is None
    blocks = table.shape[0] // (BLOCK * WORDS)
    total = sum(sizes) * WORDS
    scalars = [place, *upd, *(() if final else ext)]
    parts = (gh, *qb, *gn)
    scratch = [
        pltpu.VMEM((total, LANES), F32),
        pltpu.VMEM((sum(p.shape[0] for p in qb), LANES), BF16),
        pltpu.VMEM((sum(p.shape[0] for p in gn), LANES), F32),
        pltpu.VMEM((BLOCK * WORDS, LANES), F32),
        pltpu.VMEM((SLOTS * BLOCK * WORDS, LANES), F32),
    ]
    if final:
        outs = [ANY, whole((blocks, 1, BLOCK))]
        shapes = [jax.ShapeDtypeStruct((dim, blocks * BLOCK), F32), jax.ShapeDtypeStruct((blocks, 1, BLOCK), F32)]
        scratch.append(pltpu.VMEM((2, dim, BLOCK), F32))
    else:
        outs = [ANY, ANY, whole((near_rows(tails, negs), LANES))]
        shapes = [jax.ShapeDtypeStruct(table.shape, F32), jax.ShapeDtypeStruct((heads * WORDS, LANES), F32),
                  jax.ShapeDtypeStruct((near_rows(tails, negs), LANES), BF16)]
        scratch.append(pltpu.VMEM((total, LANES), F32))
    scratch += [pltpu.SemaphoreType.DMA((len(parts),)), pltpu.SemaphoreType.DMA((SLOTS,)), pltpu.SemaphoreType.DMA((SLOTS,))]
    return pl.pallas_call(
        functools.partial(entity_kernel, (sizes, dim, lr, final, len(qb), len(gn))),
        grid_spec=pltpu.PrefetchScalarGridSpec(
            num_scalar_prefetch=len(scalars), grid=(1,), in_specs=[ANY] * (1 + len(parts)), out_specs=outs, scratch_shapes=scratch),
        out_shape=shapes,
        input_output_aliases={} if final else {len(scalars): 0},
        compiler_params=params(),
        name="entity_last" if final else "entity_pass",
    )(*scalars, table, *parts)


def load_relation_terms(part, pad, counts, parts, terms, sems):
    shared = parts[0]
    stage = 8 * part * WORDS
    size = part // TILE * packed_rows(TILE, ROW_SLOT)
    copies = []
    for j in range(8):
        copies.append(pltpu.make_async_copy(shared.at[pl.ds(j * size, size)], terms.at[pl.ds(stage + j * size, size)], sems.at[j]))
    more = pltpu.make_async_copy(parts[1], terms.at[pl.ds(8 * part * WORDS, parts[1].shape[0])], sems.at[8])
    for c in copies:
        c.start()
    for c in copies:
        c.wait()
    tiles = part // TILE

    def body(i, carry):
        slot = i // tiles
        t = lax.rem(i, tiles)

        @pl.when(slot // 4 * part + t * TILE < counts[lax.rem(slot, 4)])
        def _():
            v, _ = get_packed(terms, stage + slot * size + t * packed_rows(TILE, ROW_SLOT), TILE, pad, ROW_SLOT)
            for c in range(WORDS):
                terms[pl.ds((slot * part + t * TILE) * WORDS + c, TILE, stride=WORDS), :] = v[c]

        return carry

    lax.fori_loop(0, 8 * tiles, body, 0)

    @pl.when(counts[4] > 0)
    def _():
        more.start()
        more.wait()


def relation_kernel(cfg, *refs):
    dim, lr, part, n_parts = cfg
    usrc, udst, uoff, counts, xsrc, xoff, table = refs[:7]
    parts = refs[7:7 + n_parts]
    out, xr, terms, acc, ring, rows, sems, load_sems, store_sems = refs[7 + n_parts:]
    blocks = table.shape[0] // (BLOCK * WORDS)
    acc[...] = jnp.zeros_like(acc)
    start_sweep(table, ring, load_sems)
    load_relation_terms(part, dim // 2 - LANES, counts, parts, terms, sems)

    def store(b):
        slot = lax.rem(b, SLOTS)
        at = block_rows(b)
        return pltpu.make_async_copy(ring.at[block_rows(slot)], out.at[at], store_sems.at[slot])

    def body(b, ref):
        sum_terms(usrc, udst, uoff[b], uoff[b + 1], terms, acc)
        update_words(ref, acc, dim, lr)
        copy_rows(xsrc, lambda k: k * WORDS, xoff[b], xoff[b + 1], ref, rows)

    sweep(table, ring, load_sems, store, blocks, body)
    copy = pltpu.make_async_copy(rows, xr, sems.at[0])
    copy.start()
    copy.wait()


def relation_last_kernel(cfg, *refs):
    dim, lr, part, n_parts = cfg
    usrc, udst, uoff, counts, src = refs[:5]
    parts = refs[5:5 + n_parts]
    dst, terms, acc, sems = refs[5 + n_parts:]
    step = pl.program_id(0)

    @pl.when(step == 0)
    def _():
        acc[...] = jnp.zeros_like(acc)
        load_relation_terms(part, dim // 2 - LANES, counts, parts, terms, sems)

    group = src.shape[0] // (BLOCK * WORDS)
    for j in range(group):
        b = step * group + j
        sum_terms(usrc, udst, uoff[b], uoff[b + 1], terms, acc)
        update_columns(src.at[block_rows(j)], acc, dst, None, dim, lr, j * BLOCK)


def relation_pass(table, edges, part, dim, lr, upd, parts, ext):
    count = 8 * part * WORDS + sum(p.shape[0] for p in parts[1:])
    scalars = [*upd, *ext]
    return pl.pallas_call(
        functools.partial(relation_kernel, (dim, lr, part, len(parts))),
        grid_spec=pltpu.PrefetchScalarGridSpec(
            num_scalar_prefetch=len(scalars), grid=(1,), in_specs=[ANY] * (1 + len(parts)), out_specs=[ANY, ANY],
            scratch_shapes=[
                pltpu.VMEM((count, LANES), F32),
                pltpu.VMEM((BLOCK * WORDS, LANES), F32),
                pltpu.VMEM((SLOTS * BLOCK * WORDS, LANES), F32),
                pltpu.VMEM((4 * BLOCK * WORDS, LANES), F32),
                pltpu.SemaphoreType.DMA((9,)),
                pltpu.SemaphoreType.DMA((SLOTS,)),
                pltpu.SemaphoreType.DMA((SLOTS,)),
            ]),
        out_shape=[jax.ShapeDtypeStruct(table.shape, F32), jax.ShapeDtypeStruct((edges * WORDS, LANES), F32)],
        input_output_aliases={len(scalars): 0},
        compiler_params=params(),
        name="relation_pass",
    )(*scalars, table, *parts)


def relation_last(table, n_rel, part, dim, lr, upd, parts):
    blocks = table.shape[0] // (BLOCK * WORDS)
    group = 3 if blocks % 3 == 0 else 1
    count = 8 * part * WORDS + sum(p.shape[0] for p in parts[1:])
    return pl.pallas_call(
        functools.partial(relation_last_kernel, (dim, lr, part, len(parts))),
        grid_spec=pltpu.PrefetchScalarGridSpec(
            num_scalar_prefetch=len(upd), grid=(blocks // group,),
            in_specs=[pl.BlockSpec((BLOCK * group * WORDS, LANES), lambda b, *_: (b, 0))] + [ANY] * len(parts),
            out_specs=pl.BlockSpec((dim, BLOCK * group), lambda b, *_: (0, b)),
            scratch_shapes=[
                pltpu.VMEM((count, LANES), F32),
                pltpu.VMEM((BLOCK * WORDS, LANES), F32),
                pltpu.SemaphoreType.DMA((9,)),
            ]),
        out_shape=jax.ShapeDtypeStruct((dim, n_rel), F32),
        compiler_params=params(),
        name="relation_last",
    )(*upd, table, *parts)


def edge_rows(ref, keep, keep_data):
    v = [ref[pl.ds(c, TILE, stride=WORDS), :] for c in range(WORDS)]
    return [jnp.where(keep_data if c % 2 else keep, v[c], 0.0) for c in range(WORDS)]


def edge_masks(start, n, pad):
    row = lax.broadcasted_iota(jnp.int32, (TILE, LANES), 0) + start
    lane = lax.broadcasted_iota(jnp.int32, (TILE, LANES), 1)
    keep = row < n
    return lane, keep, keep & (lane < pad)


def fetch_negatives(near, neg_in, nb, pad, sem):
    copy = pltpu.make_async_copy(near.at[pl.ds(near.shape[0] - neg_in.shape[0], neg_in.shape[0])], neg_in, sem)
    copy.start()
    copy.wait()
    for c, v in enumerate(get_packed(neg_in, 0, nb.shape[0], pad, ROW_SLOT)[0]):
        nb[:, LANES * c:LANES * (c + 1)] = v.astype(BF16)


def pick_tail(tails, buf, step, rep):
    if len(tails) == 1:
        return tails[0]
    quarter = pl.num_programs(0) // 4
    side = step // quarter - 2
    for ref, chosen in zip(tails, (side < 0, side == rep, (side >= 0) & (side != rep))):
        @pl.when(chosen)
        def _(ref=ref):
            buf[...] = ref[...]

    return buf


def score_kernel(cfg, info, xh, xr, *refs):
    half, n_tails = cfg
    tails, (near, qb_out, ds_out, gn, loss, tail_buf, neg_in, nb, gacc, sem) = refs[:n_tails], refs[n_tails:]
    step = pl.program_id(0)
    pad = half - LANES
    n = info[0]
    start = step * TILE

    @pl.when(step == 0)
    def _():
        gacc[...] = jnp.zeros_like(gacc)
        loss[0, 0] = 0.0
        fetch_negatives(near, neg_in, nb, pad, sem)

    @pl.when(start < n)
    def _():
        tb = pick_tail(tails, tail_buf, step, info[1])
        lane, keep, keep_data = edge_masks(start, n, pad)
        h = edge_rows(xh, keep, keep_data)
        r = edge_rows(xr, keep, keep_data)
        q = [h[0] * r[0] - h[2] * r[2], h[1] * r[1] - h[3] * r[3], h[0] * r[2] + h[2] * r[0], h[1] * r[3] + h[3] * r[1]]
        qc = [v.astype(BF16) for v in q]
        query = jnp.concatenate(qc, axis=1)
        wide = [v.astype(F32) for v in qc]
        tail = [jnp.where(keep, v, 0.0) for v in get_packed(tb, 0, TILE, pad, ROW_SLOT)[0]]
        prod = [wide[c] * tail[c] for c in range(WORDS)]
        pos = jnp.sum((prod[0] + prod[1]) + (prod[2] + prod[3]), axis=1, keepdims=True)
        score = lax.dot_general(query, nb[...], (((1,), (1,)), ((), ())), preferred_element_type=F32)
        top = jnp.maximum(jnp.max(score, axis=1, keepdims=True), pos)
        pos_exp = jnp.exp(pos - top)
        neg_exp = jnp.exp(score - top)
        total = pos_exp + jnp.sum(neg_exp, axis=1, keepdims=True)
        weight = jnp.where(keep[:, :1], 1.0, 0.0)
        loss[0, 0] += jnp.sum(weight * ((top + jnp.log(total)) - pos))
        inverse = 1.0 / total
        dp = weight * (pos_exp * inverse - 1.0)
        ds = ((weight * inverse) * neg_exp).astype(BF16)
        ds_out[...] = ds
        gacc[...] += lax.dot_general(ds, query, (((0,), (0,)), ((), ())), preferred_element_type=F32)
        hi = dp.astype(BF16).astype(F32)
        mid = (dp - hi).astype(BF16).astype(F32)
        low = (dp - hi) - mid
        q3 = jnp.where(lane == pad, hi, jnp.where(lane == pad + 1, mid, jnp.where(lane == pad + 2, low, wide[3])))
        put_packed(qb_out, 0, [*wide[:3], q3], pad, QUERY_SLOT)

    @pl.when(step == pl.num_programs(0) - 1)
    def _():
        put_packed(gn, 0, [gacc[:, LANES * c:LANES * (c + 1)] for c in range(WORDS)], pad, ROW_SLOT)


def dp_of(last, pad):
    return (last[:, pad:pad + 1] + last[:, pad + 1:pad + 2]) + last[:, pad + 2:pad + 3]


def gradient_kernel(cfg, spot, info, xh, xr, *refs):
    cap, edges, half, n_tails = cfg
    tails, (near, qb, ds, gh, ua, ub, tail_buf, neg_in, nb, gr, uniq, held, sem) = refs[:n_tails], refs[n_tails:]
    step = pl.program_id(0)
    pad = half - LANES
    n = info[0]
    start = step * TILE

    @pl.when(step == 0)
    def _():
        fetch_negatives(near, neg_in, nb, pad, sem)

    @pl.when(start < n)
    def _():
        tb = pick_tail(tails, tail_buf, step, info[1])
        _, keep, keep_data = edge_masks(start, n, pad)
        h = edge_rows(xh, keep, keep_data)
        r = edge_rows(xr, keep, keep_data)
        tail = [jnp.where(keep, v, 0.0) for v in get_packed(tb, 0, TILE, pad, ROW_SLOT)[0]]
        dp = dp_of(get_packed(qb, 0, TILE, pad, QUERY_SLOT)[1], pad)
        gq = lax.dot_general(ds[...], nb[...], (((1,), (0,)), ((), ())), preferred_element_type=F32)
        g = [dp * tail[c] + gq[:, LANES * c:LANES * (c + 1)] for c in range(WORDS)]
        out = [g[0] * r[0] + g[2] * r[2], g[1] * r[1] + g[3] * r[3], g[2] * r[0] - g[0] * r[2], g[3] * r[1] - g[1] * r[3]]
        rel_g = [g[0] * h[0] + g[2] * h[2], g[1] * h[1] + g[3] * h[3], g[2] * h[0] - g[0] * h[2], g[3] * h[1] - g[1] * h[3]]
        for c in range(WORDS):
            gh[pl.ds(c, TILE, stride=WORDS), :] = out[c]
            gr[pl.ds(c, TILE, stride=WORDS), :] = rel_g[c]

        def body(k, carry):
            prev, acc = carry
            at = spot[k]
            acc = jnp.where(at == prev, acc, 0.0) + gr[words_of(k - start), :]
            uniq[word(at), :] = acc
            return at, acc

        prev = jnp.where(step > 0, spot[jnp.maximum(start - 1, 0)], -1)
        _, acc = unrolled_loop(start, jnp.minimum(start + TILE, n), UNROLL, body, (prev, held[:WORDS, :]))
        held[:WORDS, :] = acc

    @pl.when(step == pl.num_programs(0) - 1)
    def _():
        more = pltpu.make_async_copy(uniq.at[pl.ds(cap * WORDS, (edges - cap) * WORDS)], ub, sem)
        more.start()
        part = cap // 2

        def body(t, carry):
            r0 = info[1] * part + t * TILE
            v = [uniq[pl.ds(r0 * WORDS + c, TILE, stride=WORDS), :] for c in range(WORDS)]
            put_packed(ua, t * packed_rows(TILE, ROW_SLOT), v, pad, ROW_SLOT)
            return carry

        lax.fori_loop(0, part // TILE, body, 0)
        more.wait()


def bucket_specs(negs, n_tails, tiles):
    word_spec = pl.BlockSpec((TILE * WORDS, LANES), lambda t, *_: (t, 0))
    tail_block = (packed_rows(TILE, ROW_SLOT), LANES)
    quarter = tiles // 4
    if n_tails == 1:
        tail_specs = [pl.BlockSpec(tail_block, lambda t, *_: (t, 0))]
    else:
        tail_specs = [
            pl.BlockSpec(tail_block, lambda t, *_: (jnp.minimum(t, 2 * quarter - 1), 0)),
            pl.BlockSpec(tail_block, lambda t, *s: (jnp.clip(t - (2 + s[-1][1]) * quarter, 0, quarter - 1), 0)),
            pl.BlockSpec(tail_block, lambda t, *s: (jnp.clip(t - (3 - s[-1][1]) * quarter, 0, quarter - 1), 0)),
        ]
    query_spec = pl.BlockSpec((packed_rows(TILE, QUERY_SLOT), LANES), lambda t, *_: (t, 0))
    return word_spec, tail_specs, query_spec, pl.BlockSpec((TILE, negs), lambda t, *_: (t, 0)), pltpu.VMEM(tail_block, BF16)


def scores(info, xh, xr, near, edges, negs, half):
    tails, near_negs = near
    word_spec, tail_specs, query_spec, prob_spec, tail_buf = bucket_specs(negs, len(tails), edges // TILE)
    neg_rows = packed_rows(negs, ROW_SLOT)
    return pl.pallas_call(
        functools.partial(score_kernel, (half, len(tails))),
        grid_spec=pltpu.PrefetchScalarGridSpec(
            num_scalar_prefetch=1,
            grid=(edges // TILE,),
            in_specs=[word_spec, word_spec, *tail_specs, ANY],
            out_specs=[query_spec, prob_spec, whole((neg_rows, LANES)),
                       pl.BlockSpec((1, 1), lambda *_: (0, 0), memory_space=pltpu.SMEM)],
            scratch_shapes=[
                tail_buf,
                pltpu.VMEM((neg_rows, LANES), BF16),
                pltpu.VMEM((negs, WIDE), BF16),
                pltpu.VMEM((negs, WIDE), F32),
                pltpu.SemaphoreType.DMA(()),
            ]),
        out_shape=[
            jax.ShapeDtypeStruct((edges // TILE * packed_rows(TILE, QUERY_SLOT), LANES), BF16),
            jax.ShapeDtypeStruct((edges, negs), BF16),
            jax.ShapeDtypeStruct((neg_rows, LANES), F32),
            jax.ShapeDtypeStruct((1, 1), F32),
        ],
        compiler_params=params(),
        name="scores",
    )(info, xh, xr, *tails, near_negs)


def gradients(spot, info, xh, xr, near, qb, ds, negs, cap, half):
    edges = spot.shape[0]
    tails, near_negs = near
    word_spec, tail_specs, query_spec, prob_spec, tail_buf = bucket_specs(negs, len(tails), edges // TILE)
    shared_rows = cap // 2 // TILE * packed_rows(TILE, ROW_SLOT)
    return pl.pallas_call(
        functools.partial(gradient_kernel, (cap, edges, half, len(tails))),
        grid_spec=pltpu.PrefetchScalarGridSpec(
            num_scalar_prefetch=2,
            grid=(edges // TILE,),
            in_specs=[word_spec, word_spec, *tail_specs, ANY, query_spec, prob_spec],
            out_specs=[word_spec, whole((shared_rows, LANES)), ANY],
            scratch_shapes=[
                tail_buf,
                pltpu.VMEM((packed_rows(negs, ROW_SLOT), LANES), BF16),
                pltpu.VMEM((negs, WIDE), BF16),
                pltpu.VMEM((TILE * WORDS, LANES), F32),
                pltpu.VMEM((edges * WORDS, LANES), F32),
                pltpu.VMEM((8, LANES), F32),
                pltpu.SemaphoreType.DMA(()),
            ]),
        out_shape=[
            jax.ShapeDtypeStruct((edges * WORDS, LANES), F32),
            jax.ShapeDtypeStruct((shared_rows, LANES), F32),
            jax.ShapeDtypeStruct(((edges - cap) * WORDS, LANES), F32),
        ],
        compiler_params=params(),
        name="gradients",
    )(spot, info, xh, xr, *tails, near_negs, qb, ds)


def running_count(flags):
    lead = flags.shape[:-1]
    n = flags.shape[-1] // LANES
    x = flags.reshape(*lead, n, LANES).astype(F32)
    tri = jnp.triu(jnp.ones((LANES, LANES), F32))
    inner = jnp.einsum('...k,kl->...l', x, tri, precision=lax.Precision.HIGHEST)
    before = jnp.einsum('...k,kl->...l', inner[..., -1], jnp.triu(jnp.ones((n, n), F32), 1), precision=lax.Precision.HIGHEST)
    return (inner + before[..., None]).astype(jnp.int32).reshape(flags.shape)


def blank(shape, dtype):
    return pl.pallas_call(lambda out: None, out_shape=jax.ShapeDtypeStruct(shape, dtype), out_specs=ANY, name="blank")()


def halves(x, rep, count):
    size = x.shape[0] // 2 // count
    return [lax.dynamic_slice_in_dim(x, (rep * count + j) * size, size) for j in range(count)]


def offsets(keys, bounds):
    return jnp.sum(keys[:, None, :] < bounds[None, :, None], axis=2, dtype=jnp.int32)


def solution(mesh):
    groups = mesh.shape['ent']
    data_reps = mesh.shape['data']
    row_spec = P(('sweep', 'ent'), None)
    edge_spec = P(('sweep', 'ent'), None, 'data')

    def device_fn(ent_table, ent_state, rel_table, head_idx, tail_idx, rel_idx, edge_mask, neg_idx):
        part_rows, dim = ent_table.shape
        half = dim // 2
        n_rel = rel_table.shape[0]
        rounds = head_idx.shape[1]
        edges = head_idx.shape[2] * data_reps
        negs = neg_idx.shape[2]
        sizes = (edges, edges, negs)
        cap = edges // 2
        lr = LR_SCALE * dim ** -0.25
        me = lax.axis_index('ent')
        rep = lax.axis_index('data')

        rel_words = relation_words(rel_table.T)

        big = (NO_KEY >> 13) - 1
        order = jnp.where(edge_mask[0] > 0, rel_idx[0], big)
        packed = head_idx[0] * part_rows + tail_idx[0]
        both = lax.all_gather(jnp.stack([order, packed]), 'data', axis=2, tiled=True)
        spot = jnp.arange(edges, dtype=jnp.int32)
        order, packed = lax.sort((both[0] * edges + spot, both[1]), dimension=1, num_keys=1)
        rel_s = order // edges
        head_s = packed // part_rows
        tail_s = packed % part_rows
        live = rel_s < n_rel
        kept = jnp.sum(live, axis=1, dtype=jnp.int32)
        info = jnp.concatenate([jnp.where(live, rel_s, n_rel), jnp.where(live, tail_s, part_rows), neg_idx[0]], axis=1)
        every = lax.all_gather(info, 'ent', axis=0)
        every, fetch_from = lax.optimization_barrier((every, rel_words))
        xr = relation_fetch(fetch_from, edges, rel_s[0] * WORDS, kept[:1])

        far = jnp.stack([lax.dynamic_index_in_dim(every, (me - s) % groups, 0, False)[s, edges:] for s in range(rounds)])
        ids = jnp.concatenate([jnp.where(live, head_s, part_rows), far], axis=1)
        keys = jnp.where(ids < part_rows, (ids << SHIFT) + jnp.arange(sum(sizes), dtype=jnp.int32), NO_KEY)
        ent_key = lax.sort(keys, dimension=1, is_stable=False)
        ent_off = offsets(ent_key, jnp.arange(part_rows // BLOCK + 1, dtype=jnp.int32) * (BLOCK << SHIFT))
        ent_src = (ent_key & POS_MASK) * WORDS
        ent_dst = ((ent_key >> SHIFT) % BLOCK) * WORDS

        rels = every[:, :, :edges]
        prev = jnp.concatenate([jnp.full((groups, rounds, 1), -1, jnp.int32), rels[:, :, :-1]], axis=2)
        fresh = (rels != prev) & (rels < n_rel)
        slot = running_count(fresh) - 1
        over = jnp.max(slot[:, :, -1], axis=0) >= cap
        counts = jnp.concatenate([slot[:, :, -1] + 1, jnp.max(slot[:, :, -1] // cap, axis=0)[None]], axis=0).T
        own_spot = lax.dynamic_index_in_dim(slot, me, 0, False) * WORDS
        source = jnp.arange(groups, dtype=jnp.int32)[:, None, None]
        part = cap // data_reps
        first = (slot // part * groups + source) * part + slot % part
        slot = jnp.where(slot < cap, first, groups * cap + source * (edges - cap) + slot - cap)
        keys = jnp.where(fresh, (rels << SHIFT) + slot, NO_KEY).transpose(1, 0, 2).reshape(rounds, groups * edges)
        keys, ent_key = lax.optimization_barrier((keys, ent_key))
        rel_key = lax.sort(keys, dimension=1, is_stable=False)
        rel_key, own_spot = lax.optimization_barrier((rel_key, own_spot))
        bounds = jnp.arange(pl.cdiv(n_rel, BLOCK) + 1, dtype=jnp.int32) * BLOCK
        rel_off = offsets(rel_key, bounds << SHIFT)
        rel_src = (rel_key & POS_MASK) * WORDS
        rel_dst = ((rel_key >> SHIFT) % BLOCK) * WORDS
        own_off = offsets(jnp.where(live, rel_s, NO_KEY), bounds)
        own_src = (rel_s % BLOCK) * WORDS
        info = jnp.stack([kept, jnp.full((rounds,), rep, jnp.int32)], axis=1)

        ent_args = (sizes, dim, lr)
        rel_args = (part, dim, lr)
        ent_words, xh, xt = entity_first(ent_table.T, ent_state, sizes, (ent_dst[0], ent_src[0], ent_off[0]))
        place = rep[None].astype(jnp.int32)
        swap = [(i, 1 - i) for i in range(data_reps)]
        losses = []
        for s in range(rounds):
            forth = [(i, (i - s) % groups) for i in range(groups)]
            if s == 0:
                tn = ((xt,), xt)
            elif s == groups // 2:
                tail_rows = edges // TILE * packed_rows(TILE, ROW_SLOT)
                lead = tail_rows // 2
                part_size = lead // data_reps
                early = lax.ppermute(lax.dynamic_slice_in_dim(xt, lead + rep * part_size, part_size), 'ent', forth)
                rest = [lax.ppermute(v, 'ent', forth) for v in (xt[:lead], xt[tail_rows:])]
                late, xr = lax.optimization_barrier((early, xr))
                late = lax.ppermute(late, 'data', swap)
                tn = ((rest[0], early, late), rest[1])
            else:
                xt = lax.ppermute(xt, 'ent', forth)
                tn = ((xt,), xt)
            own_qb, ds, gn, loss = scores(info[s], xh, xr, tn, edges, negs, half)
            losses.append(loss[0, 0] / edges)
            qb, gn = (own_qb,), (gn,)
            back = [(i, (i + s) % groups) for i in range(groups)]
            trade = s == groups // 2
            if trade:
                pieces = [lax.ppermute(v, 'ent', back) for v in (*halves(own_qb, rep, 2), *halves(gn[0], rep, 1))]
                pieces[0], own_qb = lax.optimization_barrier((pieces[0], own_qb))
            gh, ua, ub = gradients(own_spot[s], info[s], xh, xr, tn, own_qb, ds, negs, cap, half)
            if s > 0:
                if trade:
                    traded = [lax.ppermute(pieces[0], 'data', swap)]
                    for v in pieces[1:]:
                        v, gh = lax.optimization_barrier((v, gh))
                        traded.append(lax.ppermute(v, 'data', swap))
                    qb = (*pieces[:2], *traded[:2])
                    gn = (pieces[2], traded[2])
                else:
                    qb = (lax.ppermute(qb[0], 'ent', back),)
                    gn = (lax.ppermute(gn[0], 'ent', back),)
                qb, gn, ua = lax.optimization_barrier((qb, gn, ua))
            shared = lax.all_gather(ua, ('data', 'ent'), axis=0, tiled=True)

            final = s == rounds - 1
            ent_upd = (ent_src[s], ent_dst[s], ent_off[s])
            rel_upd = (rel_src[s], rel_dst[s], rel_off[s], counts[s])

            def relations(table, *parts, s=s, final=final, rel_upd=rel_upd):
                if final:
                    return (relation_last(table, n_rel, *rel_args, rel_upd, parts),)
                return relation_pass(table, edges, *rel_args, rel_upd, parts, (own_src[s + 1], own_off[s + 1]))

            def overflow(ub):
                return lax.all_gather(ub, 'ent', axis=0, tiled=True)

            def nothing(ub):
                return blank((groups * ub.shape[0], LANES), F32)

            more = lax.cond(over[s], overflow, nothing, ub)
            if final:
                ent_cols, state = entity_pass(ent_words, *ent_args, place, ent_upd, gh, qb, gn)
                (rel_cols,) = relations(rel_words, shared, more)
            else:
                ent_words, xh, xt = entity_pass(ent_words, *ent_args, place, ent_upd, gh, qb, gn, (ent_dst[s + 1], ent_src[s + 1], ent_off[s + 1]))
                rel_words, xr = relations(rel_words, shared, more)
        return ent_cols.T, state.reshape(part_rows), rel_cols.T, jnp.stack(losses)[None, :]

    return jax.shard_map(device_fn, mesh=mesh, in_specs=(row_spec, P(('sweep', 'ent')), P('sweep', None), edge_spec, edge_spec, edge_spec, edge_spec, P(('sweep', 'ent'), None, None)), out_specs=(row_spec, P(('sweep', 'ent')), P('sweep', None), row_spec), check_vma=False)
```

```python
import functools

import jax
import jax.numpy as jnp
from jax import lax
from jax.experimental import pallas as pl
from jax.experimental.pallas import tpu as pltpu
from jax.sharding import PartitionSpec as P

LR_SCALE = 0.2
EPSILON = 1e-8

LANES = 128
WORDS = 4
SHIFT = 14
POS_MASK = (1 << SHIFT) - 1
NO_KEY = 2**31 - 1
BLOCK = 1024
SUB = 128
SLOTS = 4
FIRST = 2
UNROLL = (16, 4)
ROW_SLOT = 16
QUERY_SLOT = 32
WIDE = WORDS * LANES
TILE = 512
CHUNK = 256
VMEM_LIMIT = 63 * 2**20
F32 = jnp.float32
BF16 = jnp.bfloat16
ANY = pl.BlockSpec(memory_space=pl.ANY)


def words_of(start):
    return pl.ds(pl.multiple_of(start * WORDS, WORDS), WORDS)


def word(start):
    return pl.ds(pl.multiple_of(start, WORDS), WORDS)


def block_rows(slot):
    return pl.ds(pl.multiple_of(slot * BLOCK * WORDS, BLOCK * WORDS), BLOCK * WORDS)


def unrolled_loop(lo, hi, unroll, body, carry):
    for width in (*unroll, 1):
        full = (hi - lo) // width

        def several(t, c, lo=lo, width=width):
            for j in range(width):
                c = body(lo + t * width + j, c)
            return c

        carry = lax.fori_loop(0, full, several, carry)
        lo = lo + full * width
    return carry


def packed_rows(n, slot):
    return 3 * n + n * slot // LANES


def pack(v, pad, slot):
    n = v[0].shape[0]
    gap = LANES - pad
    lane = lax.broadcasted_iota(jnp.int32, (n, LANES), 1)
    mixed = jnp.where(lane < pad, v[1], pltpu.roll(v[3], pad, 1))
    groups = LANES // slot
    size = n // groups
    thin = lane[:size]
    rest = jnp.zeros((size, LANES), F32)
    for a in range(groups):
        moved = pltpu.roll(v[3][a * size:(a + 1) * size], (slot * a - gap) % LANES, 1)
        rest = jnp.where((thin >= slot * a) & (thin < slot * (a + 1)), moved, rest)
    return v[0], v[2], mixed, rest


def unpack(first, third, mixed, rest, pad, slot):
    n = first.shape[0]
    gap = LANES - pad
    lane = lax.broadcasted_iota(jnp.int32, (n, LANES), 1)
    tail = jnp.concatenate([pltpu.roll(rest, (gap - slot * a) % LANES, 1) for a in range(LANES // slot)], axis=0)
    last = jnp.where(lane < gap, pltpu.roll(mixed, LANES - pad, 1), tail)
    return [first, jnp.where(lane < pad, mixed, 0.0), third, jnp.where(lane < pad, last, 0.0)], last


def put_packed(ref, base, v, pad, slot):
    n = v[0].shape[0]
    for c, part in enumerate(pack(v, pad, slot)):
        ref[pl.ds(pl.multiple_of(base + c * n, 16), part.shape[0]), :] = part.astype(ref.dtype)


def get_packed(ref, base, n, pad, slot):
    at = [pl.ds(pl.multiple_of(base + c * n, 16), n if c < 3 else n * slot // LANES) for c in range(4)]
    return unpack(*[ref[i, :].astype(F32) for i in at], pad, slot)


def params(**kw):
    return pltpu.CompilerParams(dimension_semantics=("arbitrary",), vmem_limit_bytes=VMEM_LIMIT, **kw)


def whole(shape):
    return pl.BlockSpec(shape, lambda *_: (0,) * len(shape), pipeline_mode=pl.Buffered(1))


def convert_block(src, state, dst, half, first=0):
    pad = half - LANES
    sub8 = lax.broadcasted_iota(jnp.int32, (8, LANES), 0)
    for r0 in range(0, BLOCK, SUB):
        cols = slice(first + r0, first + r0 + SUB)
        if state is not None:
            low = jnp.where(sub8 == 7, jnp.broadcast_to(state[:, cols], (8, LANES)), 0.0)
        else:
            low = jnp.zeros((8, LANES), F32)
        gap = jnp.zeros((LANES - pad - 8, LANES), F32)
        none = jnp.zeros((8, LANES), F32)
        w = [
            src[:LANES, cols],
            jnp.concatenate([src[LANES:half, cols], gap, none], axis=0),
            src[half:half + LANES, cols],
            jnp.concatenate([src[half + LANES:, cols], gap, low], axis=0),
        ]
        for c in range(WORDS):
            dst[pl.ds(r0 * WORDS + c, SUB, stride=WORDS), :] = w[c].T


def relation_words_kernel(half, src, dst):
    for j in range(dst.shape[0] // (BLOCK * WORDS)):
        convert_block(src, None, dst.at[block_rows(j)], half, j * BLOCK)


def entity_first_kernel(sizes, half, xsrc, xdst, xoff, src, state, dst, xh, xt, rows, sems):
    step = pl.program_id(0)
    for j in range(FIRST):
        part = dst.at[block_rows(j)]
        convert_block(src, state, part, half, j * BLOCK)
        b = step * FIRST + j
        copy_rows(xsrc, lambda k: xdst[k], xoff[b], xoff[b + 1], part, rows)

    @pl.when(step == pl.num_programs(0) - 1)
    def _():
        store_entity_rows(sizes, half, rows, xh, xt, sems.at[0])


def relation_words(table_t):
    dim, rows = table_t.shape
    blocks = pl.cdiv(rows, BLOCK)
    group = 3 if blocks % 3 == 0 else 1
    return pl.pallas_call(
        functools.partial(relation_words_kernel, dim // 2),
        grid=(blocks // group,),
        in_specs=[pl.BlockSpec((dim, BLOCK * group), lambda b: (0, b))],
        out_specs=pl.BlockSpec((BLOCK * group * WORDS, LANES), lambda b: (b, 0)),
        out_shape=jax.ShapeDtypeStruct((blocks * BLOCK * WORDS, LANES), F32),
        compiler_params=params(),
        name="relation_words",
    )(table_t)


def entity_first(table_t, state, sizes, ext):
    dim, rows = table_t.shape
    heads, tails, negs = sizes
    steps = rows // (BLOCK * FIRST)
    near = near_rows(tails, negs)
    return pl.pallas_call(
        functools.partial(entity_first_kernel, sizes, dim // 2),
        grid_spec=pltpu.PrefetchScalarGridSpec(
            num_scalar_prefetch=3, grid=(steps,),
            in_specs=[pl.BlockSpec((dim, BLOCK * FIRST), lambda b, *_: (0, b)),
                      pl.BlockSpec((None, 1, BLOCK * FIRST), lambda b, *_: (b, 0, 0))],
            out_specs=[pl.BlockSpec((BLOCK * FIRST * WORDS, LANES), lambda b, *_: (b, 0)), ANY, whole((near, LANES))],
            scratch_shapes=[pltpu.VMEM((sum(sizes) * WORDS, LANES), F32), pltpu.SemaphoreType.DMA((1,))]),
        out_shape=[jax.ShapeDtypeStruct((rows * WORDS, LANES), F32), jax.ShapeDtypeStruct((heads * WORDS, LANES), F32),
                   jax.ShapeDtypeStruct((near, LANES), BF16)],
        compiler_params=params(),
        name="entity_first",
    )(*ext, table_t, state.reshape(steps, 1, BLOCK * FIRST))


def block_load(table, ring, load_sems, b):
    slot = lax.rem(b, SLOTS)
    return pltpu.make_async_copy(table.at[block_rows(b)], ring.at[block_rows(slot)], load_sems.at[slot])


def start_sweep(table, ring, load_sems):
    for b in range(2):
        block_load(table, ring, load_sems, b).start()


def sweep(table, ring, load_sems, store, blocks, body):
    load = functools.partial(block_load, table, ring, load_sems)

    def turn(b, carry):
        load(b).wait()

        @pl.when(b >= 2)
        def _():
            store(b - 2).wait()

        @pl.when(b + 2 < blocks)
        def _():
            load(b + 2).start()

        body(b, ring.at[block_rows(lax.rem(b, SLOTS))])
        store(b).start()
        return carry

    lax.fori_loop(0, blocks, turn, 0)
    store(blocks - 2).wait()
    store(blocks - 1).wait()


def apply_step(w, g, lane, dim, lr):
    total = (g[0] * g[0] + g[1] * g[1]) + (g[2] * g[2] + g[3] * g[3])
    last = lane == LANES - 1
    state = jnp.sum(total * (1.0 / dim) + jnp.where(last, w[3], 0.0), axis=1, keepdims=True)
    scale = lr * lax.rsqrt(state + EPSILON)
    new = [w[c] - g[c] * scale for c in range(WORDS)]
    return [*new[:3], jnp.where(last, state, new[3])]


def sum_terms(src, dst, lo, hi, terms, acc):
    def body(k, carry):
        prev, total = carry
        at = dst[k]
        total = jnp.where(at == prev, total, 0.0) + terms[word(src[k]), :]
        acc[word(at), :] = total
        return at, total

    unrolled_loop(lo, hi, UNROLL, body, (jnp.int32(-1), jnp.zeros((WORDS, LANES), F32)))


def take_sums(acc, at):
    sums = [acc[i, :] for i in at]
    for i in at:
        acc[i, :] = jnp.zeros((SUB, LANES), F32)
    return sums


def update_words(ref, acc, dim, lr):
    lane = lax.broadcasted_iota(jnp.int32, (SUB, LANES), 1)
    for r0 in range(0, BLOCK, SUB):
        at = [pl.ds(r0 * WORDS + c, SUB, stride=WORDS) for c in range(WORDS)]
        w = apply_step([ref[i, :] for i in at], take_sums(acc, at), lane, dim, lr)
        for c in range(WORDS):
            ref[at[c], :] = w[c]


def update_columns(ref, acc, dst, state_out, dim, lr, first=0):
    half = dim // 2
    pad = half - LANES
    lane = lax.broadcasted_iota(jnp.int32, (SUB, LANES), 1)
    for r0 in range(0, BLOCK, SUB):
        at = [pl.ds(r0 * WORDS + c, SUB, stride=WORDS) for c in range(WORDS)]
        w = apply_step([ref[i, :] for i in at], take_sums(acc, at), lane, dim, lr)
        cols = slice(first + r0, first + r0 + SUB)
        dst[:LANES, cols] = w[0].T
        dst[LANES:half, cols] = w[1].T[:pad]
        dst[half:half + LANES, cols] = w[2].T
        w3 = w[3].T
        dst[half + LANES:, cols] = w3[:pad]
        if state_out is not None:
            state_out[:, cols] = w3[LANES - 1:]


def place_parts(rep, parts, dst, sems, first):
    size = parts[0].shape[0]
    side = len(parts) // 2
    copies = []
    for n, part in enumerate(parts):
        at = 0 if side == 0 else (rep * side + n if n < side else (1 - rep) * side + n - side) * size
        copies.append(pltpu.make_async_copy(part, dst.at[pl.ds(pl.multiple_of(at, 16) if side else 0, size)], sems.at[first + n]))
    return copies


def load_entity_terms(sizes, half, rep, gh, qb, gn, terms, queries, neg_terms, sems, then):
    heads, tails, negs = sizes
    pad = half - LANES
    head_copy = pltpu.make_async_copy(gh, terms.at[pl.ds(0, heads * WORDS)], sems.at[0])
    query_copies = place_parts(rep, qb, queries, sems, 1)
    neg_copies = place_parts(rep, gn, neg_terms, sems, 1 + len(qb))
    for c in (*query_copies, *neg_copies, head_copy):
        c.start()
    then()
    for c in query_copies:
        c.wait()

    def body(t, carry):
        q, last = get_packed(queries, t * packed_rows(TILE, QUERY_SLOT), TILE, pad, QUERY_SLOT)
        dp = dp_of(last, pad)
        for c in range(WORDS):
            terms[pl.ds((heads + t * TILE) * WORDS + c, TILE, stride=WORDS), :] = dp * q[c]
        return carry

    lax.fori_loop(0, tails // TILE, body, 0)
    for c in neg_copies:
        c.wait()
    for c, v in enumerate(get_packed(neg_terms, 0, negs, pad, ROW_SLOT)[0]):
        terms[pl.ds((heads + tails) * WORDS + c, negs, stride=WORDS), :] = v
    head_copy.wait()


def store_entity_rows(sizes, half, rows, xh, xt, sem):
    heads, tails, negs = sizes
    pad = half - LANES
    copy = pltpu.make_async_copy(rows.at[pl.ds(0, heads * WORDS)], xh, sem)
    copy.start()

    def move(r0, n, base):
        v = [rows[pl.ds((heads + r0) * WORDS + c, n, stride=WORDS), :] for c in range(WORDS)]
        put_packed(xt, base, v, pad, ROW_SLOT)

    def body(t, carry):
        move(t * TILE, TILE, t * packed_rows(TILE, ROW_SLOT))
        return carry

    lax.fori_loop(0, tails // TILE, body, 0)
    move(tails, negs, tails // TILE * packed_rows(TILE, ROW_SLOT))
    copy.wait()


def near_rows(tails, negs):
    return tails // TILE * packed_rows(TILE, ROW_SLOT) + packed_rows(negs, ROW_SLOT)


def fetch_rows(row, spot, count, table, rows, sem):
    def body(k, carry):
        pltpu.make_async_copy(table.at[word(row[k])], rows.at[word(spot(k))], sem).start()
        return carry

    unrolled_loop(0, count, UNROLL, body, 0)
    size = pl.multiple_of(count * WORDS, WORDS)
    pltpu.make_async_copy(table.at[pl.ds(0, size)], rows.at[pl.ds(0, size)], sem).wait()


def relation_fetch_kernel(row, count, table, xr, rows, sems):
    fetch_rows(row, lambda k: k * WORDS, count[0], table, rows, sems.at[0])
    copy = pltpu.make_async_copy(rows, xr, sems.at[1])
    copy.start()
    copy.wait()


def entity_kernel(cfg, *refs):
    sizes, dim, lr, final, n_qb, n_gn = cfg
    it = iter(refs)
    place, usrc, udst, uoff = next(it), next(it), next(it), next(it)
    xsrc, xdst, xoff = (None, None, None) if final else (next(it), next(it), next(it))
    table, gh = next(it), next(it)
    qb = [next(it) for _ in range(n_qb)]
    gn = [next(it) for _ in range(n_gn)]
    out = next(it)
    if final:
        state_out = next(it)
    else:
        xh, xt = next(it), next(it)
    terms, queries, neg_terms, acc, ring = next(it), next(it), next(it), next(it), next(it)
    rows = None if final else next(it)
    cols = next(it) if final else None
    sems, load_sems, store_sems = next(it), next(it), next(it)
    blocks = table.shape[0] // (BLOCK * WORDS)
    acc[...] = jnp.zeros_like(acc)
    load_entity_terms(sizes, dim // 2, place[0], gh, qb, gn, terms, queries, neg_terms, sems, lambda: start_sweep(table, ring, load_sems))

    def store(b):
        if final:
            slot = lax.rem(b, 2)
            at = pl.ds(pl.multiple_of(b * BLOCK, BLOCK), BLOCK)
            return pltpu.make_async_copy(cols.at[slot], out.at[:, at], store_sems.at[slot])
        slot = lax.rem(b, SLOTS)
        at = block_rows(b)
        return pltpu.make_async_copy(ring.at[block_rows(slot)], out.at[at], store_sems.at[slot])

    def body(b, ref):
        sum_terms(usrc, udst, uoff[b], uoff[b + 1], terms, acc)
        if final:
            update_columns(ref, acc, cols.at[lax.rem(b, 2)], state_out.at[b], dim, lr)
        else:
            update_words(ref, acc, dim, lr)
            copy_rows(xsrc, lambda k: xdst[k], xoff[b], xoff[b + 1], ref, rows)

    sweep(table, ring, load_sems, store, blocks, body)
    if not final:
        store_entity_rows(sizes, dim // 2, rows, xh, xt, sems.at[0])


def copy_rows(src, dst, lo, hi, ref, rows):
    def body(k, carry):
        rows[word(dst(k)), :] = ref[word(src[k]), :]
        return carry

    unrolled_loop(lo, hi, UNROLL, body, 0)


def relation_fetch(table, edges, row, count):
    return pl.pallas_call(
        relation_fetch_kernel,
        grid_spec=pltpu.PrefetchScalarGridSpec(
            num_scalar_prefetch=2, grid=(1,), in_specs=[ANY], out_specs=ANY,
            scratch_shapes=[pltpu.VMEM((edges * WORDS, LANES), F32), pltpu.SemaphoreType.DMA((2,))]),
        out_shape=jax.ShapeDtypeStruct((edges * WORDS, LANES), F32),
        compiler_params=params(),
        name="relation_fetch",
    )(row, count, table)


def entity_pass(table, sizes, dim, lr, place, upd, gh, qb, gn, ext=None):
    heads, tails, negs = sizes
    final = ext is None
    blocks = table.shape[0] // (BLOCK * WORDS)
    total = sum(sizes) * WORDS
    scalars = [place, *upd, *(() if final else ext)]
    parts = (gh, *qb, *gn)
    scratch = [
        pltpu.VMEM((total, LANES), F32),
        pltpu.VMEM((sum(p.shape[0] for p in qb), LANES), BF16),
        pltpu.VMEM((sum(p.shape[0] for p in gn), LANES), F32),
        pltpu.VMEM((BLOCK * WORDS, LANES), F32),
        pltpu.VMEM((SLOTS * BLOCK * WORDS, LANES), F32),
    ]
    if final:
        outs = [ANY, whole((blocks, 1, BLOCK))]
        shapes = [jax.ShapeDtypeStruct((dim, blocks * BLOCK), F32), jax.ShapeDtypeStruct((blocks, 1, BLOCK), F32)]
        scratch.append(pltpu.VMEM((2, dim, BLOCK), F32))
    else:
        outs = [ANY, ANY, whole((near_rows(tails, negs), LANES))]
        shapes = [jax.ShapeDtypeStruct(table.shape, F32), jax.ShapeDtypeStruct((heads * WORDS, LANES), F32),
                  jax.ShapeDtypeStruct((near_rows(tails, negs), LANES), BF16)]
        scratch.append(pltpu.VMEM((total, LANES), F32))
    scratch += [pltpu.SemaphoreType.DMA((len(parts),)), pltpu.SemaphoreType.DMA((SLOTS,)), pltpu.SemaphoreType.DMA((SLOTS,))]
    return pl.pallas_call(
        functools.partial(entity_kernel, (sizes, dim, lr, final, len(qb), len(gn))),
        grid_spec=pltpu.PrefetchScalarGridSpec(
            num_scalar_prefetch=len(scalars), grid=(1,), in_specs=[ANY] * (1 + len(parts)), out_specs=outs, scratch_shapes=scratch),
        out_shape=shapes,
        input_output_aliases={} if final else {len(scalars): 0},
        compiler_params=params(),
        name="entity_last" if final else "entity_pass",
    )(*scalars, table, *parts)


def load_relation_terms(part, pad, counts, parts, terms, sems):
    shared = parts[0]
    stage = 8 * part * WORDS
    size = part // TILE * packed_rows(TILE, ROW_SLOT)
    copies = []
    for j in range(8):
        copies.append(pltpu.make_async_copy(shared.at[pl.ds(j * size, size)], terms.at[pl.ds(stage + j * size, size)], sems.at[j]))
    more = pltpu.make_async_copy(parts[1], terms.at[pl.ds(8 * part * WORDS, parts[1].shape[0])], sems.at[8])
    for c in copies:
        c.start()
    for c in copies:
        c.wait()
    tiles = part // TILE

    def body(i, carry):
        slot = i // tiles
        t = lax.rem(i, tiles)

        @pl.when(slot // 4 * part + t * TILE < counts[lax.rem(slot, 4)])
        def _():
            v, _ = get_packed(terms, stage + slot * size + t * packed_rows(TILE, ROW_SLOT), TILE, pad, ROW_SLOT)
            for c in range(WORDS):
                terms[pl.ds((slot * part + t * TILE) * WORDS + c, TILE, stride=WORDS), :] = v[c]

        return carry

    lax.fori_loop(0, 8 * tiles, body, 0)

    @pl.when(counts[4] > 0)
    def _():
        more.start()
        more.wait()


def relation_kernel(cfg, *refs):
    dim, lr, part, n_parts = cfg
    usrc, udst, uoff, counts, xsrc, xoff, table = refs[:7]
    parts = refs[7:7 + n_parts]
    out, xr, terms, acc, ring, rows, sems, load_sems, store_sems = refs[7 + n_parts:]
    blocks = table.shape[0] // (BLOCK * WORDS)
    acc[...] = jnp.zeros_like(acc)
    start_sweep(table, ring, load_sems)
    load_relation_terms(part, dim // 2 - LANES, counts, parts, terms, sems)

    def store(b):
        slot = lax.rem(b, SLOTS)
        at = block_rows(b)
        return pltpu.make_async_copy(ring.at[block_rows(slot)], out.at[at], store_sems.at[slot])

    def body(b, ref):
        sum_terms(usrc, udst, uoff[b], uoff[b + 1], terms, acc)
        update_words(ref, acc, dim, lr)
        copy_rows(xsrc, lambda k: k * WORDS, xoff[b], xoff[b + 1], ref, rows)

    sweep(table, ring, load_sems, store, blocks, body)
    copy = pltpu.make_async_copy(rows, xr, sems.at[0])
    copy.start()
    copy.wait()


def relation_last_kernel(cfg, *refs):
    dim, lr, part, n_parts = cfg
    usrc, udst, uoff, counts, src = refs[:5]
    parts = refs[5:5 + n_parts]
    dst, terms, acc, sems = refs[5 + n_parts:]
    step = pl.program_id(0)

    @pl.when(step == 0)
    def _():
        acc[...] = jnp.zeros_like(acc)
        load_relation_terms(part, dim // 2 - LANES, counts, parts, terms, sems)

    group = src.shape[0] // (BLOCK * WORDS)
    for j in range(group):
        b = step * group + j
        sum_terms(usrc, udst, uoff[b], uoff[b + 1], terms, acc)
        update_columns(src.at[block_rows(j)], acc, dst, None, dim, lr, j * BLOCK)


def relation_pass(table, edges, part, dim, lr, upd, parts, ext):
    count = 8 * part * WORDS + sum(p.shape[0] for p in parts[1:])
    scalars = [*upd, *ext]
    return pl.pallas_call(
        functools.partial(relation_kernel, (dim, lr, part, len(parts))),
        grid_spec=pltpu.PrefetchScalarGridSpec(
            num_scalar_prefetch=len(scalars), grid=(1,), in_specs=[ANY] * (1 + len(parts)), out_specs=[ANY, ANY],
            scratch_shapes=[
                pltpu.VMEM((count, LANES), F32),
                pltpu.VMEM((BLOCK * WORDS, LANES), F32),
                pltpu.VMEM((SLOTS * BLOCK * WORDS, LANES), F32),
                pltpu.VMEM((4 * BLOCK * WORDS, LANES), F32),
                pltpu.SemaphoreType.DMA((9,)),
                pltpu.SemaphoreType.DMA((SLOTS,)),
                pltpu.SemaphoreType.DMA((SLOTS,)),
            ]),
        out_shape=[jax.ShapeDtypeStruct(table.shape, F32), jax.ShapeDtypeStruct((edges * WORDS, LANES), F32)],
        input_output_aliases={len(scalars): 0},
        compiler_params=params(),
        name="relation_pass",
    )(*scalars, table, *parts)


def relation_last(table, n_rel, part, dim, lr, upd, parts):
    blocks = table.shape[0] // (BLOCK * WORDS)
    group = 3 if blocks % 3 == 0 else 1
    count = 8 * part * WORDS + sum(p.shape[0] for p in parts[1:])
    return pl.pallas_call(
        functools.partial(relation_last_kernel, (dim, lr, part, len(parts))),
        grid_spec=pltpu.PrefetchScalarGridSpec(
            num_scalar_prefetch=len(upd), grid=(blocks // group,),
            in_specs=[pl.BlockSpec((BLOCK * group * WORDS, LANES), lambda b, *_: (b, 0))] + [ANY] * len(parts),
            out_specs=pl.BlockSpec((dim, BLOCK * group), lambda b, *_: (0, b)),
            scratch_shapes=[
                pltpu.VMEM((count, LANES), F32),
                pltpu.VMEM((BLOCK * WORDS, LANES), F32),
                pltpu.SemaphoreType.DMA((9,)),
            ]),
        out_shape=jax.ShapeDtypeStruct((dim, n_rel), F32),
        compiler_params=params(),
        name="relation_last",
    )(*upd, table, *parts)


def edge_rows(ref, keep, keep_data):
    v = [ref[pl.ds(c, TILE, stride=WORDS), :] for c in range(WORDS)]
    return [jnp.where(keep_data if c % 2 else keep, v[c], 0.0) for c in range(WORDS)]


def edge_masks(start, n, pad):
    row = lax.broadcasted_iota(jnp.int32, (TILE, LANES), 0) + start
    lane = lax.broadcasted_iota(jnp.int32, (TILE, LANES), 1)
    keep = row < n
    return lane, keep, keep & (lane < pad)


def fetch_negatives(near, neg_in, nb, pad, sem):
    copy = pltpu.make_async_copy(near.at[pl.ds(near.shape[0] - neg_in.shape[0], neg_in.shape[0])], neg_in, sem)
    copy.start()
    copy.wait()
    for c, v in enumerate(get_packed(neg_in, 0, nb.shape[0], pad, ROW_SLOT)[0]):
        nb[:, LANES * c:LANES * (c + 1)] = v.astype(BF16)


def pick_tail(tails, buf, step, rep):
    if len(tails) == 1:
        return tails[0]
    quarter = pl.num_programs(0) // 4
    side = step // quarter - 2
    for ref, chosen in zip(tails, (side < 0, side == rep, (side >= 0) & (side != rep))):
        @pl.when(chosen)
        def _(ref=ref):
            buf[...] = ref[...]

    return buf


def score_kernel(cfg, info, xh, xr, *refs):
    half, n_tails = cfg
    tails, (near, qb_out, ds_out, gn, loss, tail_buf, neg_in, nb, gacc, sem) = refs[:n_tails], refs[n_tails:]
    step = pl.program_id(0)
    pad = half - LANES
    n = info[0]
    start = step * TILE

    @pl.when(step == 0)
    def _():
        gacc[...] = jnp.zeros_like(gacc)
        loss[0, 0] = 0.0
        fetch_negatives(near, neg_in, nb, pad, sem)

    @pl.when(start < n)
    def _():
        tb = pick_tail(tails, tail_buf, step, info[1])
        lane, keep, keep_data = edge_masks(start, n, pad)
        h = edge_rows(xh, keep, keep_data)
        r = edge_rows(xr, keep, keep_data)
        q = [h[0] * r[0] - h[2] * r[2], h[1] * r[1] - h[3] * r[3], h[0] * r[2] + h[2] * r[0], h[1] * r[3] + h[3] * r[1]]
        qc = [v.astype(BF16) for v in q]
        query = jnp.concatenate(qc, axis=1)
        wide = [v.astype(F32) for v in qc]
        tail = [jnp.where(keep, v, 0.0) for v in get_packed(tb, 0, TILE, pad, ROW_SLOT)[0]]
        prod = [wide[c] * tail[c] for c in range(WORDS)]
        pos = jnp.sum((prod[0] + prod[1]) + (prod[2] + prod[3]), axis=1, keepdims=True)
        score = lax.dot_general(query, nb[...], (((1,), (1,)), ((), ())), preferred_element_type=F32)
        top = jnp.maximum(jnp.max(score, axis=1, keepdims=True), pos)
        pos_exp = jnp.exp(pos - top)
        neg_exp = jnp.exp(score - top)
        total = pos_exp + jnp.sum(neg_exp, axis=1, keepdims=True)
        weight = jnp.where(keep[:, :1], 1.0, 0.0)
        loss[0, 0] += jnp.sum(weight * ((top + jnp.log(total)) - pos))
        inverse = 1.0 / total
        dp = weight * (pos_exp * inverse - 1.0)
        ds = ((weight * inverse) * neg_exp).astype(BF16)
        ds_out[...] = ds
        gacc[...] += lax.dot_general(ds, query, (((0,), (0,)), ((), ())), preferred_element_type=F32)
        hi = dp.astype(BF16).astype(F32)
        mid = (dp - hi).astype(BF16).astype(F32)
        low = (dp - hi) - mid
        q3 = jnp.where(lane == pad, hi, jnp.where(lane == pad + 1, mid, jnp.where(lane == pad + 2, low, wide[3])))
        put_packed(qb_out, 0, [*wide[:3], q3], pad, QUERY_SLOT)

    @pl.when(step == pl.num_programs(0) - 1)
    def _():
        put_packed(gn, 0, [gacc[:, LANES * c:LANES * (c + 1)] for c in range(WORDS)], pad, ROW_SLOT)


def dp_of(last, pad):
    return (last[:, pad:pad + 1] + last[:, pad + 1:pad + 2]) + last[:, pad + 2:pad + 3]


def gradient_kernel(cfg, spot, info, xh, xr, *refs):
    cap, edges, half, n_tails = cfg
    tails, (near, qb, ds, gh, ua, ub, tail_buf, neg_in, nb, gr, uniq, held, sem) = refs[:n_tails], refs[n_tails:]
    step = pl.program_id(0)
    pad = half - LANES
    n = info[0]
    start = step * TILE

    @pl.when(step == 0)
    def _():
        fetch_negatives(near, neg_in, nb, pad, sem)

    @pl.when(start < n)
    def _():
        tb = pick_tail(tails, tail_buf, step, info[1])
        _, keep, keep_data = edge_masks(start, n, pad)
        h = edge_rows(xh, keep, keep_data)
        r = edge_rows(xr, keep, keep_data)
        tail = [jnp.where(keep, v, 0.0) for v in get_packed(tb, 0, TILE, pad, ROW_SLOT)[0]]
        dp = dp_of(get_packed(qb, 0, TILE, pad, QUERY_SLOT)[1], pad)
        gq = lax.dot_general(ds[...], nb[...], (((1,), (0,)), ((), ())), preferred_element_type=F32)
        g = [dp * tail[c] + gq[:, LANES * c:LANES * (c + 1)] for c in range(WORDS)]
        out = [g[0] * r[0] + g[2] * r[2], g[1] * r[1] + g[3] * r[3], g[2] * r[0] - g[0] * r[2], g[3] * r[1] - g[1] * r[3]]
        rel_g = [g[0] * h[0] + g[2] * h[2], g[1] * h[1] + g[3] * h[3], g[2] * h[0] - g[0] * h[2], g[3] * h[1] - g[1] * h[3]]
        for c in range(WORDS):
            gh[pl.ds(c, TILE, stride=WORDS), :] = out[c]
            gr[pl.ds(c, TILE, stride=WORDS), :] = rel_g[c]

        def body(k, carry):
            prev, acc = carry
            at = spot[k]
            acc = jnp.where(at == prev, acc, 0.0) + gr[words_of(k - start), :]
            uniq[word(at), :] = acc
            return at, acc

        prev = jnp.where(step > 0, spot[jnp.maximum(start - 1, 0)], -1)
        _, acc = unrolled_loop(start, jnp.minimum(start + TILE, n), UNROLL, body, (prev, held[:WORDS, :]))
        held[:WORDS, :] = acc

    @pl.when(step == pl.num_programs(0) - 1)
    def _():
        more = pltpu.make_async_copy(uniq.at[pl.ds(cap * WORDS, (edges - cap) * WORDS)], ub, sem)
        more.start()
        part = cap // 2

        def body(t, carry):
            r0 = info[1] * part + t * TILE
            v = [uniq[pl.ds(r0 * WORDS + c, TILE, stride=WORDS), :] for c in range(WORDS)]
            put_packed(ua, t * packed_rows(TILE, ROW_SLOT), v, pad, ROW_SLOT)
            return carry

        lax.fori_loop(0, part // TILE, body, 0)
        more.wait()


def bucket_specs(negs, n_tails, tiles):
    word_spec = pl.BlockSpec((TILE * WORDS, LANES), lambda t, *_: (t, 0))
    tail_block = (packed_rows(TILE, ROW_SLOT), LANES)
    quarter = tiles // 4
    if n_tails == 1:
        tail_specs = [pl.BlockSpec(tail_block, lambda t, *_: (t, 0))]
    else:
        tail_specs = [
            pl.BlockSpec(tail_block, lambda t, *_: (jnp.minimum(t, 2 * quarter - 1), 0)),
            pl.BlockSpec(tail_block, lambda t, *s: (jnp.clip(t - (2 + s[-1][1]) * quarter, 0, quarter - 1), 0)),
            pl.BlockSpec(tail_block, lambda t, *s: (jnp.clip(t - (3 - s[-1][1]) * quarter, 0, quarter - 1), 0)),
        ]
    query_spec = pl.BlockSpec((packed_rows(TILE, QUERY_SLOT), LANES), lambda t, *_: (t, 0))
    return word_spec, tail_specs, query_spec, pl.BlockSpec((TILE, negs), lambda t, *_: (t, 0)), pltpu.VMEM(tail_block, BF16)


def scores(info, xh, xr, near, edges, negs, half):
    tails, near_negs = near
    word_spec, tail_specs, query_spec, prob_spec, tail_buf = bucket_specs(negs, len(tails), edges // TILE)
    neg_rows = packed_rows(negs, ROW_SLOT)
    return pl.pallas_call(
        functools.partial(score_kernel, (half, len(tails))),
        grid_spec=pltpu.PrefetchScalarGridSpec(
            num_scalar_prefetch=1,
            grid=(edges // TILE,),
            in_specs=[word_spec, word_spec, *tail_specs, ANY],
            out_specs=[query_spec, prob_spec, whole((neg_rows, LANES)),
                       pl.BlockSpec((1, 1), lambda *_: (0, 0), memory_space=pltpu.SMEM)],
            scratch_shapes=[
                tail_buf,
                pltpu.VMEM((neg_rows, LANES), BF16),
                pltpu.VMEM((negs, WIDE), BF16),
                pltpu.VMEM((negs, WIDE), F32),
                pltpu.SemaphoreType.DMA(()),
            ]),
        out_shape=[
            jax.ShapeDtypeStruct((edges // TILE * packed_rows(TILE, QUERY_SLOT), LANES), BF16),
            jax.ShapeDtypeStruct((edges, negs), BF16),
            jax.ShapeDtypeStruct((neg_rows, LANES), F32),
            jax.ShapeDtypeStruct((1, 1), F32),
        ],
        compiler_params=params(),
        name="scores",
    )(info, xh, xr, *tails, near_negs)


def gradients(spot, info, xh, xr, near, qb, ds, negs, cap, half):
    edges = spot.shape[0]
    tails, near_negs = near
    word_spec, tail_specs, query_spec, prob_spec, tail_buf = bucket_specs(negs, len(tails), edges // TILE)
    shared_rows = cap // 2 // TILE * packed_rows(TILE, ROW_SLOT)
    return pl.pallas_call(
        functools.partial(gradient_kernel, (cap, edges, half, len(tails))),
        grid_spec=pltpu.PrefetchScalarGridSpec(
            num_scalar_prefetch=2,
            grid=(edges // TILE,),
            in_specs=[word_spec, word_spec, *tail_specs, ANY, query_spec, prob_spec],
            out_specs=[word_spec, whole((shared_rows, LANES)), ANY],
            scratch_shapes=[
                tail_buf,
                pltpu.VMEM((packed_rows(negs, ROW_SLOT), LANES), BF16),
                pltpu.VMEM((negs, WIDE), BF16),
                pltpu.VMEM((TILE * WORDS, LANES), F32),
                pltpu.VMEM((edges * WORDS, LANES), F32),
                pltpu.VMEM((8, LANES), F32),
                pltpu.SemaphoreType.DMA(()),
            ]),
        out_shape=[
            jax.ShapeDtypeStruct((edges * WORDS, LANES), F32),
            jax.ShapeDtypeStruct((shared_rows, LANES), F32),
            jax.ShapeDtypeStruct(((edges - cap) * WORDS, LANES), F32),
        ],
        compiler_params=params(),
        name="gradients",
    )(spot, info, xh, xr, *tails, near_negs, qb, ds)


def running_count(flags):
    lead = flags.shape[:-1]
    n = flags.shape[-1] // LANES
    x = flags.reshape(*lead, n, LANES).astype(F32)
    tri = jnp.triu(jnp.ones((LANES, LANES), F32))
    inner = jnp.einsum('...k,kl->...l', x, tri, precision=lax.Precision.HIGHEST)
    before = jnp.einsum('...k,kl->...l', inner[..., -1], jnp.triu(jnp.ones((n, n), F32), 1), precision=lax.Precision.HIGHEST)
    return (inner + before[..., None]).astype(jnp.int32).reshape(flags.shape)


def blank(shape, dtype):
    return pl.pallas_call(lambda out: None, out_shape=jax.ShapeDtypeStruct(shape, dtype), out_specs=ANY, name="blank")()


def halves(x, rep, count):
    size = x.shape[0] // 2 // count
    return [lax.dynamic_slice_in_dim(x, (rep * count + j) * size, size) for j in range(count)]


def offsets(keys, bounds):
    return jnp.sum(keys[:, None, :] < bounds[None, :, None], axis=2, dtype=jnp.int32)


def solution(mesh):
    groups = mesh.shape['ent']
    data_reps = mesh.shape['data']
    row_spec = P(('sweep', 'ent'), None)
    edge_spec = P(('sweep', 'ent'), None, 'data')

    def device_fn(ent_table, ent_state, rel_table, head_idx, tail_idx, rel_idx, edge_mask, neg_idx):
        part_rows, dim = ent_table.shape
        half = dim // 2
        n_rel = rel_table.shape[0]
        rounds = head_idx.shape[1]
        edges = head_idx.shape[2] * data_reps
        negs = neg_idx.shape[2]
        sizes = (edges, edges, negs)
        cap = edges // 2
        lr = LR_SCALE * dim ** -0.25
        me = lax.axis_index('ent')
        rep = lax.axis_index('data')

        rel_words = relation_words(rel_table.T)

        big = (NO_KEY >> 13) - 1
        order = jnp.where(edge_mask[0] > 0, rel_idx[0], big)
        packed = head_idx[0] * part_rows + tail_idx[0]
        both = lax.all_gather(jnp.stack([order, packed]), 'data', axis=2, tiled=True)
        spot = jnp.arange(edges, dtype=jnp.int32)
        order, packed = lax.sort((both[0] * edges + spot, both[1]), dimension=1, num_keys=1)
        rel_s = order // edges
        head_s = packed // part_rows
        tail_s = packed % part_rows
        live = rel_s < n_rel
        kept = jnp.sum(live, axis=1, dtype=jnp.int32)
        info = jnp.concatenate([jnp.where(live, rel_s, n_rel), jnp.where(live, tail_s, part_rows), neg_idx[0]], axis=1)
        every = lax.all_gather(info, 'ent', axis=0)
        every, fetch_from = lax.optimization_barrier((every, rel_words))
        xr = relation_fetch(fetch_from, edges, rel_s[0] * WORDS, kept[:1])

        far = jnp.stack([lax.dynamic_index_in_dim(every, (me - s) % groups, 0, False)[s, edges:] for s in range(rounds)])
        ids = jnp.concatenate([jnp.where(live, head_s, part_rows), far], axis=1)
        keys = jnp.where(ids < part_rows, (ids << SHIFT) + jnp.arange(sum(sizes), dtype=jnp.int32), NO_KEY)
        ent_key = lax.sort(keys, dimension=1, is_stable=False)
        ent_off = offsets(ent_key, jnp.arange(part_rows // BLOCK + 1, dtype=jnp.int32) * (BLOCK << SHIFT))
        ent_src = (ent_key & POS_MASK) * WORDS
        ent_dst = ((ent_key >> SHIFT) % BLOCK) * WORDS

        rels = every[:, :, :edges]
        prev = jnp.concatenate([jnp.full((groups, rounds, 1), -1, jnp.int32), rels[:, :, :-1]], axis=2)
        fresh = (rels != prev) & (rels < n_rel)
        slot = running_count(fresh) - 1
        over = jnp.max(slot[:, :, -1], axis=0) >= cap
        counts = jnp.concatenate([slot[:, :, -1] + 1, jnp.max(slot[:, :, -1] // cap, axis=0)[None]], axis=0).T
        own_spot = lax.dynamic_index_in_dim(slot, me, 0, False) * WORDS
        source = jnp.arange(groups, dtype=jnp.int32)[:, None, None]
        part = cap // data_reps
        first = (slot // part * groups + source) * part + slot % part
        slot = jnp.where(slot < cap, first, groups * cap + source * (edges - cap) + slot - cap)
        keys = jnp.where(fresh, (rels << SHIFT) + slot, NO_KEY).transpose(1, 0, 2).reshape(rounds, groups * edges)
        keys, ent_key = lax.optimization_barrier((keys, ent_key))
        rel_key = lax.sort(keys, dimension=1, is_stable=False)
        rel_key, own_spot = lax.optimization_barrier((rel_key, own_spot))
        bounds = jnp.arange(pl.cdiv(n_rel, BLOCK) + 1, dtype=jnp.int32) * BLOCK
        rel_off = offsets(rel_key, bounds << SHIFT)
        rel_src = (rel_key & POS_MASK) * WORDS
        rel_dst = ((rel_key >> SHIFT) % BLOCK) * WORDS
        own_off = offsets(jnp.where(live, rel_s, NO_KEY), bounds)
        own_src = (rel_s % BLOCK) * WORDS
        info = jnp.stack([kept, jnp.full((rounds,), rep, jnp.int32)], axis=1)

        ent_args = (sizes, dim, lr)
        rel_args = (part, dim, lr)
        ent_words, xh, xt = entity_first(ent_table.T, ent_state, sizes, (ent_dst[0], ent_src[0], ent_off[0]))
        place = rep[None].astype(jnp.int32)
        swap = [(i, 1 - i) for i in range(data_reps)]
        losses = []
        for s in range(rounds):
            forth = [(i, (i - s) % groups) for i in range(groups)]
            if s == 0:
                tn = ((xt,), xt)
            elif s == groups // 2:
                tail_rows = edges // TILE * packed_rows(TILE, ROW_SLOT)
                lead = tail_rows // 2
                part_size = lead // data_reps
                early = lax.ppermute(lax.dynamic_slice_in_dim(xt, lead + rep * part_size, part_size), 'ent', forth)
                rest = [lax.ppermute(v, 'ent', forth) for v in (xt[:lead], xt[tail_rows:])]
                late, xr = lax.optimization_barrier((early, xr))
                late = lax.ppermute(late, 'data', swap)
                tn = ((rest[0], early, late), rest[1])
            else:
                xt = lax.ppermute(xt, 'ent', forth)
                tn = ((xt,), xt)
            own_qb, ds, gn, loss = scores(info[s], xh, xr, tn, edges, negs, half)
            losses.append(loss[0, 0] / edges)
            qb, gn = (own_qb,), (gn,)
            back = [(i, (i + s) % groups) for i in range(groups)]
            trade = s == groups // 2
            if trade:
                pieces = [lax.ppermute(v, 'ent', back) for v in halves(own_qb, rep, 2)]
            gh, ua, ub = gradients(own_spot[s], info[s], xh, xr, tn, own_qb, ds, negs, cap, half)
            if s > 0:
                if trade:
                    last, gh = lax.optimization_barrier((gn[0], gh))
                    gn = (lax.ppermute(last, 'ent', back),)
                    traded = []
                    for v in pieces:
                        v, gh = lax.optimization_barrier((v, gh))
                        traded.append(lax.ppermute(v, 'data', swap))
                    qb = (*pieces, *traded)
                else:
                    qb = (lax.ppermute(qb[0], 'ent', back),)
                    gn = (lax.ppermute(gn[0], 'ent', back),)
                qb, gn, ua = lax.optimization_barrier((qb, gn, ua))
            shared = lax.all_gather(ua, ('data', 'ent'), axis=0, tiled=True)

            final = s == rounds - 1
            ent_upd = (ent_src[s], ent_dst[s], ent_off[s])
            rel_upd = (rel_src[s], rel_dst[s], rel_off[s], counts[s])

            def relations(table, *parts, s=s, final=final, rel_upd=rel_upd):
                if final:
                    return (relation_last(table, n_rel, *rel_args, rel_upd, parts),)
                return relation_pass(table, edges, *rel_args, rel_upd, parts, (own_src[s + 1], own_off[s + 1]))

            def overflow(ub):
                return lax.all_gather(ub, 'ent', axis=0, tiled=True)

            def nothing(ub):
                return blank((groups * ub.shape[0], LANES), F32)

            more = lax.cond(over[s], overflow, nothing, ub)
            if final:
                ent_cols, state = entity_pass(ent_words, *ent_args, place, ent_upd, gh, qb, gn)
                (rel_cols,) = relations(rel_words, shared, more)
            else:
                ent_words, xh, xt = entity_pass(ent_words, *ent_args, place, ent_upd, gh, qb, gn, (ent_dst[s + 1], ent_src[s + 1], ent_off[s + 1]))
                rel_words, xr = relations(rel_words, shared, more)
        return ent_cols.T, state.reshape(part_rows), rel_cols.T, jnp.stack(losses)[None, :]

    return jax.shard_map(device_fn, mesh=mesh, in_specs=(row_spec, P(('sweep', 'ent')), P('sweep', None), edge_spec, edge_spec, edge_spec, edge_spec, P(('sweep', 'ent'), None, None)), out_specs=(row_spec, P(('sweep', 'ent')), P('sweep', None), row_spec), check_vma=False)
```
